8 devices in a mesh: dp: 2 (over z, y), tp: 4 (over x, core).
Axes of the slice: x: 2, y: 2, z: 1, core: 2. Of those that a mesh axis runs over, the one named last changes fastest.
Arguments:
- tok_hidden: bfloat16 [256, 2048], P('dp'), parts along dimension 0
- seq_lens: int32 [256], P('dp'), parts along dimension 0
- k_cache: bfloat16 [256, 512, 4, 128], P('dp', None, 'tp'), parts along dimension 0
- v_cache: bfloat16 [256, 512, 4, 128], P('dp', None, 'tp'), parts along dimension 0
- next_tok: int32 [256], P('dp'), parts along dimension 0
- g_attn: bfloat16 [2048], replicated
- w_q: bfloat16 [2048, 2048], P(None, 'tp')
- b_q: bfloat16 [2048], P('tp')
- w_k: bfloat16 [2048, 512], P(None, 'tp')
- b_k: bfloat16 [512], P('tp')
- w_v: bfloat16 [2048, 512], P(None, 'tp')
- b_v: bfloat16 [512], P('tp')
- w_o: bfloat16 [2048, 2048], P('tp')
- g_mlp: bfloat16 [2048], replicated
- w_gate: bfloat16 [2048, 11008], P(None, 'tp')
- w_up: bfloat16 [2048, 11008], P(None, 'tp')
- w_down: bfloat16 [11008, 2048], P('tp')
- g_final: bfloat16 [2048], replicated
- w_head: bfloat16 [151936, 2048], P('tp')
Outputs:
- output 1: bfloat16 [256, 2048], P('dp'), parts along dimension 0
- output 2: bfloat16 [256, 512, 4, 128], P('dp', None, 'tp'), parts along dimension 0
- output 3: bfloat16 [256, 512, 4, 128], P('dp', None, 'tp'), parts along dimension 0
- output 4: float32 [256], P('dp'), parts along dimension 0
- output 5: float32 [256], P('dp'), parts along dimension 0
There are 2 independent parts. The reference program is written for one: setup_inputs(seed, part) draws one part's arguments, and reference() takes and returns one part's arrays. A program takes and returns all parts, laid end to end along the dimension named above; an argument that names none is the same for every part.
All inputs are finite; a program needn't handle non-finite values.
Results may differ from the reference program's by a relative error of at most 0.0126882.
Values are sent between devices in bfloat16 or wider.
A program may use at most 1 GiB of HBM per device.

```python
import math
import jax
import jax.numpy as jnp
from jax import lax

BATCH = 128
LMAX = 512
D = 2048
HEADS = 16
KV_HEADS = 2
HEAD = 128
FF = 11008
VOCAB = 151936
KV_SLOTS = 4
THETA = 1000000
EPS = 1e-6
COPIES = KV_SLOTS // KV_HEADS
GROUP = HEADS // KV_SLOTS


def rms_norm(values, gain_vec):
    vals_f32 = values.astype(jnp.float32)
    inv_rms = lax.rsqrt(jnp.mean(vals_f32 * vals_f32, axis=-1, keepdims=True) + EPS)
    return (vals_f32 * inv_rms * gain_vec.astype(jnp.float32)).astype(jnp.bfloat16)


def rotary(values, positions):
    half_dim = values.shape[-1] // 2
    inv_freq = jnp.power(float(THETA), jnp.arange(half_dim, dtype=jnp.float32) * (-2.0 / values.shape[-1]))
    angles = positions.astype(jnp.float32)[:, None] * inv_freq[None, :]
    cos_part = jnp.cos(angles)[:, None, :]
    sin_part = jnp.sin(angles)[:, None, :]
    first_half = values[..., :half_dim]
    second_half = values[..., half_dim:]
    return jnp.concatenate([first_half * cos_part - second_half * sin_part, second_half * cos_part + first_half * sin_part], axis=-1)


def draw_lengths(len_key):
    exp_key, off_key, pick_key = jax.random.split(len_key, 3)
    log_max = int(math.log2(LMAX))
    exponent = jax.random.randint(exp_key, (BATCH,), 0, log_max)
    base_len = jnp.left_shift(jnp.ones((BATCH,), jnp.int32), exponent)
    offset = jax.random.randint(off_key, (BATCH,), 0, LMAX) % base_len
    longest = jax.random.randint(pick_key, (), 0, BATCH)
    return jnp.where(jnp.arange(BATCH) == longest, LMAX - 1, base_len + offset).astype(jnp.int32)


def gaussian(rand_key, arr_shape, spread):
    return jax.random.normal(rand_key, arr_shape, jnp.float32) * spread


def setup_inputs(seed: int = 0, part: int = 0) -> dict:
    shared_keys = jax.random.split(jax.random.key(seed), 16)
    part_keys = jax.random.split(jax.random.fold_in(jax.random.key(seed + 1), part), 8)
    k_scale = math.sqrt(max(math.log(LMAX / 8.0), 1.0) / 1.25)
    k_base = gaussian(part_keys[2], (BATCH, LMAX, KV_HEADS, HEAD), k_scale)
    v_base = gaussian(part_keys[3], (BATCH, LMAX, KV_HEADS, HEAD), 1.0)
    w_k = gaussian(shared_keys[3], (D, KV_HEADS, HEAD), D ** -0.5)
    b_k = gaussian(shared_keys[4], (KV_HEADS, HEAD), 0.5)
    w_v = gaussian(shared_keys[5], (D, KV_HEADS, HEAD), D ** -0.5)
    b_v = gaussian(shared_keys[6], (KV_HEADS, HEAD), 0.5)
    return {
        'tok_hidden': gaussian(part_keys[0], (BATCH, D), 1.0).astype(jnp.bfloat16),
        'seq_lens': draw_lengths(part_keys[1]),
        'k_cache': jnp.repeat(k_base, COPIES, axis=2).astype(jnp.bfloat16),
        'v_cache': jnp.repeat(v_base, COPIES, axis=2).astype(jnp.bfloat16),
        'next_tok': jax.random.randint(part_keys[4], (BATCH,), 0, VOCAB),
        'g_attn': (1.0 + gaussian(shared_keys[0], (D,), 0.2)).astype(jnp.bfloat16),
        'w_q': gaussian(shared_keys[1], (D, HEADS * HEAD), D ** -0.5).astype(jnp.bfloat16),
        'b_q': gaussian(shared_keys[2], (HEADS * HEAD,), 0.5).astype(jnp.bfloat16),
        'w_k': jnp.repeat(w_k, COPIES, axis=1).reshape(D, KV_SLOTS * HEAD).astype(jnp.bfloat16),
        'b_k': jnp.repeat(b_k, COPIES, axis=0).reshape(KV_SLOTS * HEAD).astype(jnp.bfloat16),
        'w_v': jnp.repeat(w_v, COPIES, axis=1).reshape(D, KV_SLOTS * HEAD).astype(jnp.bfloat16),
        'b_v': jnp.repeat(b_v, COPIES, axis=0).reshape(KV_SLOTS * HEAD).astype(jnp.bfloat16),
        'w_o': gaussian(shared_keys[7], (HEADS * HEAD, D), (HEADS * HEAD) ** -0.5).astype(jnp.bfloat16),
        'g_mlp': (1.0 + gaussian(shared_keys[8], (D,), 0.2)).astype(jnp.bfloat16),
        'w_gate': gaussian(shared_keys[9], (D, FF), D ** -0.5).astype(jnp.bfloat16),
        'w_up': gaussian(shared_keys[10], (D, FF), D ** -0.5).astype(jnp.bfloat16),
        'w_down': gaussian(shared_keys[11], (FF, D), FF ** -0.5).astype(jnp.bfloat16),
        'g_final': (3.0 + gaussian(shared_keys[12], (D,), 0.5)).astype(jnp.bfloat16),
        'w_head': gaussian(shared_keys[13], (VOCAB, D), D ** -0.5).astype(jnp.bfloat16),
    }


def reference(tok_hidden, seq_lens, k_cache, v_cache, next_tok, g_attn, w_q, b_q, w_k, b_k, w_v, b_v, w_o, g_mlp, w_gate, w_up, w_down, g_final, w_head):
    normed = rms_norm(tok_hidden, g_attn)
    q_proj = jnp.dot(normed, w_q, preferred_element_type=jnp.float32) + b_q.astype(jnp.float32)
    k_proj = jnp.dot(normed, w_k, preferred_element_type=jnp.float32) + b_k.astype(jnp.float32)
    v_proj = jnp.dot(normed, w_v, preferred_element_type=jnp.float32) + b_v.astype(jnp.float32)
    q_rot = rotary(q_proj.reshape(BATCH, HEADS, HEAD), seq_lens).astype(jnp.bfloat16)
    k_new = rotary(k_proj.reshape(BATCH, KV_SLOTS, HEAD), seq_lens).astype(jnp.bfloat16)
    v_new = v_proj.reshape(BATCH, KV_SLOTS, HEAD).astype(jnp.bfloat16)
    slot_ids = jnp.arange(LMAX)
    write_mask = (slot_ids[None, :] == seq_lens[:, None])[:, :, None, None]
    k_all = jnp.where(write_mask, k_new[:, None], k_cache)
    v_all = jnp.where(write_mask, v_new[:, None], v_cache)

    def one_row(row_args):
        q_row, k_row, v_row, length = row_args
        q_grp = q_row.reshape(KV_SLOTS, GROUP, HEAD).astype(jnp.float32)
        scores = jnp.einsum('kgd,lkd->kgl', q_grp, k_row.astype(jnp.float32)) * (HEAD ** -0.5)
        scores = jnp.where((slot_ids <= length)[None, None, :], scores, -jnp.inf)
        attn_probs = jax.nn.softmax(scores, axis=-1).astype(jnp.bfloat16).astype(jnp.float32)
        attn_vals = jnp.einsum('kgl,lkd->kgd', attn_probs, v_row.astype(jnp.float32))
        return attn_vals.reshape(HEADS * HEAD).astype(jnp.bfloat16)

    attn_out = lax.map(one_row, (q_rot, k_all, v_all, seq_lens))
    attn_proj = jnp.dot(attn_out, w_o, preferred_element_type=jnp.float32)
    residual = (tok_hidden.astype(jnp.float32) + attn_proj).astype(jnp.bfloat16)
    mlp_in = rms_norm(residual, g_mlp)
    gate_proj = jnp.dot(mlp_in, w_gate, preferred_element_type=jnp.float32)
    up_proj = jnp.dot(mlp_in, w_up, preferred_element_type=jnp.float32)
    hidden = (jax.nn.silu(gate_proj) * up_proj).astype(jnp.bfloat16)
    down_proj = jnp.dot(hidden, w_down, preferred_element_type=jnp.float32)
    y_out = (residual.astype(jnp.float32) + down_proj).astype(jnp.bfloat16)
    final_norm = rms_norm(y_out, g_final)
    logits = lax.dot_general(final_norm, w_head, (((1,), (1,)), ((), ())), preferred_element_type=jnp.float32)
    norm_lse = jax.nn.logsumexp(logits, axis=-1)
    vocab_ids = jnp.arange(VOCAB)
    target = jnp.sum(jnp.where(vocab_ids[None, :] == next_tok[:, None], logits, 0.0), axis=-1)
    tok_logp = target - norm_lse
    return (y_out, k_all, v_all, tok_logp, norm_lse)
```

```python
import jax
import jax.numpy as jnp
from jax import lax
from jax.experimental import pallas as pl
from jax.experimental.pallas import tpu as pltpu
from jax.sharding import PartitionSpec as P

THETA = 1000000.0
EPS = 1e-6
MESH = pl.DeviceIdType.MESH
F32 = jnp.float32
BF16 = jnp.bfloat16
VMEM_BYTES = 67043328

ROWS = 128
WIDTH = 2048
HEAD = 128
SLOTS = 512
GROUP = 32
CHUNK = 256
NCH = 8
HALF = 4
TILE = 768
RING = 18


def dot(a, b):
    return lax.dot_general(a, b, (((1,), (0,)), ((), ())), preferred_element_type=F32)


def dot_t(a, b):
    return lax.dot_general(a, b, (((1,), (1,)), ((), ())), preferred_element_type=F32)


def attn_kernel(lens_ref, x_ref, g_ref, cos_ref, sin_ref, lanelen_ref, bq_ref, bk_ref, bv_ref,
                wq_hbm, wk_hbm, wv_hbm, wo_hbm, k_hbm, v_hbm,
                part_ref, ko_hbm, vo_hbm,
                kbuf, vbuf, wq, wk, wv, wo, q_s, k_s, v_s, qg_s, qt_s, sc_s, pt_s, o_s, at_s,
                wsem, ksem, vsem, kosem, vosem):
    groups = ROWS // GROUP
    part = GROUP // 4
    for i, (src, dst) in enumerate(((wq_hbm, wq), (wk_hbm, wk), (wv_hbm, wv))):
        pltpu.make_async_copy(src, dst, wsem.at[i]).start()

    def start_in(g, hbm, buf, sem):
        for i in range(4):
            rows = pl.ds(g * GROUP + i * part, part)
            pltpu.make_async_copy(hbm.at[rows], buf.at[rows], sem.at[g]).start()

    for g in range(groups):
        start_in(g, k_hbm, kbuf, ksem)
        start_in(g, v_hbm, vbuf, vsem)
        if g == 0:
            pltpu.make_async_copy(wo_hbm, wo, wsem.at[3]).start()

    x = x_ref[...].astype(F32)
    inv = lax.rsqrt(jnp.mean(x * x, axis=-1, keepdims=True) + EPS)
    normed = (x * inv * g_ref[...].astype(F32)).astype(BF16)
    cos = cos_ref[...]
    sin = sin_ref[...]
    for i, (src, dst) in enumerate(((wq_hbm, wq), (wk_hbm, wk), (wv_hbm, wv))):
        pltpu.make_async_copy(src, dst, wsem.at[i]).wait()

    def rope(u):
        return u * cos + pltpu.roll(u, HEAD // 2, 1) * sin

    k_s[...] = rope(dot(normed, wk[...]) + bk_ref[...].astype(F32))
    v_s[...] = dot(normed, wv[...]) + bv_ref[...].astype(F32)
    for h in range(4):
        cols = slice(h * HEAD, (h + 1) * HEAD)
        q_s[h] = rope(dot(normed, wq[:, cols]) + bq_ref[:, cols].astype(F32))

    lane_seq = lax.broadcasted_iota(jnp.int32, (HEAD, 128), 1) // 4
    slot_id = lax.broadcasted_iota(jnp.int32, (SLOTS, 128), 0)
    row16 = lax.broadcasted_iota(jnp.int32, (16, HEAD), 0)
    row_seq = lax.broadcasted_iota(jnp.int32, (16, HEAD), 0) // 4

    def one_group(g, _):
        rows = pl.ds(pl.multiple_of(g * GROUP, GROUP), GROUP)
        pltpu.make_async_copy(k_hbm.at[rows], kbuf.at[rows], ksem.at[g]).wait()

        def put(new_s, buf):
            def one(i, _):
                b = g * GROUP + i
                length = lens_ref[b]
                base = pl.multiple_of((length // 16) * 16, 16)
                old = buf[b, pl.ds(base, 16), :]
                new = jnp.broadcast_to(new_s[pl.ds(b, 1), :].astype(BF16), (16, HEAD))
                buf[b, pl.ds(base, 16), :] = jnp.where(row16 == length - base, new, old)
                return 0
            lax.fori_loop(0, GROUP, one, 0, unroll=4)

        put(k_s, kbuf)
        for h in range(4):
            qg_s[pl.ds(h, GROUP, stride=4), :] = q_s[h, rows, :]
        qt_s[...] = qg_s[...].T.astype(BF16)
        qt = qt_s[...]
        zero = jnp.zeros_like(qt)
        acc = None
        for p in range(GROUP // 2):
            b = g * GROUP + 2 * p
            lhs = jnp.concatenate([kbuf[b], kbuf[b + 1]], axis=1)
            rhs = jnp.concatenate([jnp.where(lane_seq == 2 * p, qt, zero), jnp.where(lane_seq == 2 * p + 1, qt, zero)], axis=0)
            term = dot(lhs, rhs)
            acc = term if acc is None else acc + term
        sc_s[...] = acc
        pltpu.make_async_copy(kbuf.at[rows], ko_hbm.at[rows], kosem.at[g]).start()
        live = slot_id <= lanelen_ref[pl.ds(g, 1), :]
        scores = jnp.where(live, sc_s[...] * (HEAD ** -0.5), -jnp.inf)
        top = jnp.max(scores, axis=0, keepdims=True)
        exps = jnp.exp(scores - top)
        sc_s[...] = exps
        recip = 1.0 / jnp.sum(exps, axis=0, keepdims=True)
        for i in range(4):
            blk = sc_s[i * 128:(i + 1) * 128, :] * recip
            pt_s[:, i * 128:(i + 1) * 128] = blk.T.astype(BF16)

        pltpu.make_async_copy(v_hbm.at[rows], vbuf.at[rows], vsem.at[g]).wait()
        put(v_s, vbuf)
        for j in range(GROUP // 4):
            b = g * GROUP + 4 * j
            rhs = jnp.concatenate([vbuf[b + i] for i in range(4)], axis=1)
            out = dot(pt_s[16 * j:16 * j + 16, :], rhs)
            o = jnp.zeros((16, HEAD), F32)
            for i in range(4):
                o = jnp.where(row_seq == i, out[:, i * HEAD:(i + 1) * HEAD], o)
            o_s[16 * j:16 * j + 16, :] = o
        pltpu.make_async_copy(vbuf.at[rows], vo_hbm.at[rows], vosem.at[g]).start()
        for h in range(4):
            at_s[rows, h * HEAD:(h + 1) * HEAD] = o_s[pl.ds(h, GROUP, stride=4), :].astype(BF16)
        return 0

    lax.fori_loop(0, groups, one_group, 0)

    pltpu.make_async_copy(wo_hbm, wo, wsem.at[3]).wait()
    attn = at_s[...]
    for c in range(NCH):
        part_ref[c] = dot(attn, wo[:, c * CHUNK:(c + 1) * CHUNK]).astype(BF16)
    for g in range(groups):
        rows = pl.ds(g * GROUP, GROUP)
        pltpu.make_async_copy(kbuf.at[rows], ko_hbm.at[rows], kosem.at[g]).wait()
        pltpu.make_async_copy(vbuf.at[rows], vo_hbm.at[rows], vosem.at[g]).wait()


def tail_kernel(ff, vocab_loc,
                part_ref, x_ref, gm_ref, gf_ref, tok_ref, wg_hbm, wu_hbm, wd_hbm, wh_hbm,
                y_ref, logp_ref, lse_ref,
                wbuf, r1, s1, r2, a_s, m_s, hid, p2, r1b, s2, r2b, y_s, f_s, tok2, st_s, st_r,
                wsem, s_d1, r_d1, s_x1, r_x1, s_a, r_a, s_d2, r_d2, s_x2, r_x2,
                s_y, r_y, s_o, r_o, s_f, r_f, s_t, r_t, s_st, r_st):
    dp = lax.axis_index('dp')
    tp = lax.axis_index('tp')
    core = lax.rem(tp, 2)
    dev = dp * 4 + tp
    partner = (dp, tp + 1 - 2 * core)
    xnext = (dp, lax.rem(tp + 2, 4))
    ynext = (1 - dp, tp)
    mine = core * HALF
    other = (1 - core) * HALF

    mlp_tiles = [(i * TILE, min(TILE, ff - i * TILE)) for i in range(-(-ff // TILE))]
    n_mlp = len(mlp_tiles)
    tail_pad = -(-mlp_tiles[-1][1] // CHUNK) * CHUNK
    vocab_half = vocab_loc // 2
    n_full = vocab_half // TILE
    n_tail = vocab_half - n_full * TILE
    n_head = n_full + (1 if n_tail else 0)
    head0 = 3 * n_mlp
    vbase = dp * vocab_half

    def mlp_copy(i):
        if i < 2 * n_mlp:
            src, (r, n) = (wg_hbm, wu_hbm)[i % 2], mlp_tiles[i // 2]
        else:
            src, (r, n) = wd_hbm, mlp_tiles[i - 2 * n_mlp]
        slot = i % RING
        return pltpu.make_async_copy(src.at[pl.ds(r, n)], wbuf.at[slot, pl.ds(0, n)], wsem.at[slot])

    def head_copy(i, n=TILE):
        slot = lax.rem(head0 + i, RING)
        start = pl.multiple_of(vbase + i * TILE, 16)
        return pltpu.make_async_copy(wh_hbm.at[pl.ds(start, n)], wbuf.at[slot, pl.ds(0, n)], wsem.at[slot])

    def start_item(i):
        if i < head0:
            mlp_copy(i).start()
        elif i - head0 < n_full:
            head_copy(i - head0).start()
        elif i - head0 < n_head:
            head_copy(i - head0, n_tail).start()

    for i in range(RING):
        start_item(i)

    barrier = pltpu.get_barrier_semaphore()
    for d in range(2):
        for t in range(4):
            @pl.when(d * 4 + t != dev)
            def _():
                pl.semaphore_signal(barrier, inc=1, device_id=(d, t), device_id_type=MESH)
    last_n = mlp_tiles[-1][1]
    if tail_pad > last_n:
        for i in (2 * n_mlp - 2, 2 * n_mlp - 1, 3 * n_mlp - 1):
            wbuf[i % RING, last_n:tail_pad, :] = jnp.zeros((tail_pad - last_n, WIDTH), BF16)
    pl.semaphore_wait(barrier, 7)

    def remote(src, dst, ssem, rsem, who):
        return pltpu.make_async_remote_copy(src_ref=src, dst_ref=dst, send_sem=ssem, recv_sem=rsem, device_id=who, device_id_type=MESH)

    tok_copy = remote(tok_ref, tok2, s_t, r_t, ynext)
    d1 = [remote(part_ref.at[other + j], r1.at[j], s_d1.at[j], r_d1.at[j], partner) for j in range(HALF)]
    x1 = [remote(s1.at[j], r2.at[j], s_x1.at[j], r_x1.at[j], xnext) for j in range(HALF)]
    ac = [remote(a_s.at[mine + j], a_s.at[mine + j], s_a.at[j], r_a.at[j], partner) for j in range(HALF)]
    d2 = [remote(p2.at[other + j], r1b.at[j], s_d2.at[j], r_d2.at[j], partner) for j in range(HALF)]
    x2 = [remote(s2.at[j], r2b.at[j], s_x2.at[j], r_x2.at[j], xnext) for j in range(HALF)]
    yo = [remote(y_s.at[0, mine + j], y_s.at[0, mine + j], s_o.at[j], r_o.at[j], partner) for j in range(HALF)]
    yy = [remote(y_s.at[0, mine + j], y_s.at[1, mine + j], s_y.at[j], r_y.at[j], ynext) for j in range(HALF)]
    yf = [remote(y_s.at[1, mine + j], y_s.at[1, mine + j], s_f.at[j], r_f.at[j], partner) for j in range(HALF)]

    def cols_of(c):
        return pl.ds(pl.multiple_of(c * CHUNK, CHUNK), CHUNK)

    for j in range(HALF):
        d1[j].start()
    tok_copy.start()
    for j in range(HALF):
        d1[j].wait_recv()
        s1[j] = (part_ref[mine + j].astype(F32) + r1[j].astype(F32)).astype(BF16)
        x1[j].start()
    for j in range(HALF):
        x1[j].wait_recv()
        total = s1[j].astype(F32) + r2[j].astype(F32)
        a_s[mine + j] = (x_ref[:, cols_of(mine + j)].astype(F32) + total).astype(BF16)
        ac[j].start()
    for j in range(HALF):
        ac[j].wait_recv()

    def inv_rms(src):
        total = jnp.zeros((ROWS, CHUNK), F32)
        for c in range(NCH):
            v = src[c].astype(F32)
            total = total + v * v
        return lax.rsqrt(jnp.sum(total, axis=-1, keepdims=True) * (1.0 / WIDTH) + EPS)

    inv = inv_rms(a_s)
    for c in range(NCH):
        cols = slice(c * CHUNK, (c + 1) * CHUNK)
        m_s[:, cols] = (a_s[c].astype(F32) * inv * gm_ref[:, cols].astype(F32)).astype(BF16)

    for i, (r, n) in enumerate(mlp_tiles):
        mlp_copy(2 * i).wait()
        mlp_copy(2 * i + 1).wait()
        gslot, uslot = (2 * i) % RING, (2 * i + 1) % RING
        pad = -(-n // CHUNK) * CHUNK
        for b in range(0, pad, CHUNK):
            gate = dot_t(m_s[...], wbuf[gslot, b:b + CHUNK, :])
            up = dot_t(m_s[...], wbuf[uslot, b:b + CHUNK, :])
            hid[:, r + b:r + b + CHUNK] = (gate * jax.nn.sigmoid(gate) * up).astype(BF16)
        start_item(2 * i + RING)
        start_item(2 * i + 1 + RING)

    for i in range(n_mlp):
        mlp_copy(2 * n_mlp + i).wait()

    def down(c):
        acc = None
        for i, (r, n) in enumerate(mlp_tiles):
            pad = -(-n // CHUNK) * CHUNK
            term = dot(hid[:, r:r + pad], wbuf[(2 * n_mlp + i) % RING, :pad, cols_of(c)])
            acc = term if acc is None else acc + term
        return acc.astype(BF16)

    def chip_sum(j):
        d2[j].wait_recv()
        s2[j] = (p2[mine + j].astype(F32) + r1b[j].astype(F32)).astype(BF16)
        x2[j].start()

    for j in range(HALF):
        p2[other + j] = down(other + j)
        d2[j].start()
        p2[mine + j] = down(mine + j)
        if j:
            chip_sum(j - 1)
    chip_sum(HALF - 1)
    for i in range(n_mlp):
        start_item(2 * n_mlp + i + RING)

    def forward(j):
        yy[j].wait_recv()
        yf[j].start()

    for j in range(HALF):
        x2[j].wait_recv()
        total = s2[j].astype(F32) + r2b[j].astype(F32)
        y_s[0, mine + j] = (a_s[mine + j].astype(F32) + total).astype(BF16)
        yy[j].start()
        yo[j].start()
        if j:
            forward(j - 1)
    forward(HALF - 1)
    for j in range(HALF):
        yo[j].wait_recv()
    for c in range(NCH):
        y_ref[:, c * CHUNK:(c + 1) * CHUNK] = y_s[0, c]

    def final_norm(grp):
        inv = inv_rms(y_s.at[grp])
        for c in range(NCH):
            cols = slice(c * CHUNK, (c + 1) * CHUNK)
            f_s[grp * ROWS:(grp + 1) * ROWS, cols] = (y_s[grp, c].astype(F32) * inv * gf_ref[:, cols].astype(F32)).astype(BF16)

    final_norm(0)
    for j in range(HALF):
        yf[j].wait_recv()
    final_norm(1)
    tok_copy.wait()

    tok = jnp.concatenate([tok_ref[...], tok2[...]], axis=1) - (tp * vocab_loc + vbase)
    row_id = lax.broadcasted_iota(jnp.int32, (8, 2 * ROWS), 0)

    def score(slot, first, n, state):
        top, tot, tgt = state
        for b in range(0, n, CHUNK):
            size = min(CHUNK, n - b)
            logits = dot_t(wbuf[slot, pl.ds(b, size), :], f_s[...])
            blocks = [logits[8 * i:8 * i + 8] for i in range(size // 8)]
            peak = blocks[0]
            for v in blocks[1:]:
                peak = jnp.maximum(peak, v)
            new = jnp.maximum(top, peak)
            part_sum = None
            for i, v in enumerate(blocks):
                e = jnp.exp(v - new)
                part_sum = e if part_sum is None else part_sum + e
                tgt = jnp.where(row_id + (first + b + 8 * i) == tok, v, tgt)
            tot = tot * jnp.exp(top - new) + part_sum
            top = new
        return top, tot, tgt

    def one_tile(i, state):
        slot = lax.rem(head0 + i, RING)
        head_copy(i).wait()
        state = score(slot, i * TILE, TILE, state)

        @pl.when(i + RING < n_full)
        def _():
            head_copy(i + RING).start()
        if n_tail:
            @pl.when(i + RING == n_full)
            def _():
                head_copy(n_full, n_tail).start()
        return state

    state = (jnp.full((8, 2 * ROWS), -1e30, F32), jnp.zeros((8, 2 * ROWS), F32), jnp.zeros((8, 2 * ROWS), F32))
    state = lax.fori_loop(0, n_full, one_tile, state)
    if n_tail:
        head_copy(n_full, n_tail).wait()
        state = score((head0 + n_full) % RING, n_full * TILE, n_tail, state)
    top, tot, tgt = state
    peak = jnp.max(top, axis=0, keepdims=True)
    tot = jnp.sum(tot * jnp.exp(top - peak), axis=0, keepdims=True)
    tgt = jnp.sum(tgt, axis=0, keepdims=True)
    pad = jnp.zeros((5, ROWS), F32)
    for g in range(2):
        cols = slice(g * ROWS, (g + 1) * ROWS)
        st_s[g] = jnp.concatenate([peak[:, cols], tot[:, cols], tgt[:, cols], pad], axis=0)

    sends = []
    for k in range(1, 8):
        who = lax.rem(dev + k, 8)
        whod, whot = who // 4, lax.rem(who, 4)
        grp = lax.rem(whod + dp, 2)
        sends.append(remote(st_s.at[grp], st_r.at[dev], s_st.at[k - 1], r_st.at[k - 1], (whod, whot)))
    for c in sends:
        c.start()
    st_r[dev] = st_s[0]
    for c in sends:
        c.wait()
    stats = [st_r[i] for i in range(8)]
    peak = stats[0][0:1]
    for s in stats[1:]:
        peak = jnp.maximum(peak, s[0:1])
    tot = jnp.zeros_like(peak)
    tgt = jnp.zeros_like(peak)
    for s in stats:
        tot = tot + s[1:2] * jnp.exp(s[0:1] - peak)
        tgt = tgt + s[2:3]
    lse = peak + jnp.log(tot)
    lse_ref[...] = lse
    logp_ref[...] = tgt - lse

    for group in (d1, x1, ac, d2, x2, yo, yy, yf):
        for c in group:
            c.wait_send()


def local_step(tok_hidden, seq_lens, k_cache, v_cache, next_tok, g_attn, w_q, b_q, w_k, b_k, w_v, b_v, w_o, g_mlp, w_gate, w_up, w_down, g_final, w_head):
    half = HEAD // 2
    inv_freq = jnp.power(THETA, jnp.arange(half, dtype=F32) * (-2.0 / HEAD))
    angles = seq_lens.astype(F32)[:, None] * inv_freq[None, :]
    cos, sin = jnp.cos(angles), jnp.sin(angles)
    cos_full = jnp.concatenate([cos, cos], axis=1)
    sin_full = jnp.concatenate([-sin, sin], axis=1)
    lane_len = jnp.repeat(seq_lens, 4).reshape(ROWS // GROUP, 128)
    vm = pl.BlockSpec(memory_space=pltpu.VMEM)
    sm = pl.BlockSpec(memory_space=pltpu.SMEM)
    hb = pl.BlockSpec(memory_space=pl.ANY)
    dma = pltpu.SemaphoreType.DMA
    cache = jax.ShapeDtypeStruct((ROWS, SLOTS, HEAD), BF16)
    part, k_all, v_all = pl.pallas_call(
        attn_kernel,
        out_shape=(jax.ShapeDtypeStruct((NCH, ROWS, CHUNK), BF16), cache, cache),
        in_specs=[sm] + [vm] * 8 + [hb] * 6,
        out_specs=(vm, hb, hb),
        scratch_shapes=[
            pltpu.VMEM((ROWS, SLOTS, HEAD), BF16), pltpu.VMEM((ROWS, SLOTS, HEAD), BF16),
            pltpu.VMEM((WIDTH, 512), BF16), pltpu.VMEM((WIDTH, HEAD), BF16), pltpu.VMEM((WIDTH, HEAD), BF16), pltpu.VMEM((512, WIDTH), BF16),
            pltpu.VMEM((4, ROWS, HEAD), F32), pltpu.VMEM((ROWS, HEAD), F32), pltpu.VMEM((ROWS, HEAD), F32),
            pltpu.VMEM((128, HEAD), F32), pltpu.VMEM((HEAD, 128), BF16), pltpu.VMEM((SLOTS, 128), F32), pltpu.VMEM((128, SLOTS), BF16),
            pltpu.VMEM((128, HEAD), F32), pltpu.VMEM((ROWS, 512), BF16),
            dma((4,)), dma((4,)), dma((4,)), dma((4,)), dma((4,)),
        ],
        compiler_params=pltpu.CompilerParams(vmem_limit_bytes=VMEM_BYTES),
        name="attention",
    )(seq_lens, tok_hidden, g_attn.reshape(1, WIDTH), cos_full, sin_full, lane_len, b_q.reshape(1, 512), b_k.reshape(1, HEAD), b_v.reshape(1, HEAD),
      w_q, w_k, w_v, w_o, k_cache.reshape(ROWS, SLOTS, HEAD), v_cache.reshape(ROWS, SLOTS, HEAD))

    ff = w_gate.shape[1]
    vocab_loc = w_head.shape[0]
    ff_pad = -(-ff // CHUNK) * CHUNK
    chunk4 = pltpu.VMEM((HALF, ROWS, CHUNK), BF16)
    chunk8 = pltpu.VMEM((NCH, ROWS, CHUNK), BF16)

    def kernel(*refs):
        tail_kernel(ff, vocab_loc, *refs)

    y_out, logp, lse = pl.pallas_call(
        kernel,
        out_shape=(jax.ShapeDtypeStruct((ROWS, WIDTH), BF16), jax.ShapeDtypeStruct((1, ROWS), F32), jax.ShapeDtypeStruct((1, ROWS), F32)),
        in_specs=[vm] * 5 + [hb] * 4,
        out_specs=(vm, vm, vm),
        scratch_shapes=[
            pltpu.VMEM((RING, TILE, WIDTH), BF16),
            chunk4, chunk4, chunk4, chunk8, pltpu.VMEM((ROWS, WIDTH), BF16), pltpu.VMEM((ROWS, ff_pad), BF16),
            chunk8, chunk4, chunk4, chunk4, pltpu.VMEM((2, NCH, ROWS, CHUNK), BF16), pltpu.VMEM((2 * ROWS, WIDTH), BF16),
            pltpu.VMEM((1, ROWS), jnp.int32), pltpu.VMEM((2, 8, ROWS), F32), pltpu.VMEM((8, 8, ROWS), F32),
            dma((RING,)),
        ] + [dma((HALF,))] * 16 + [dma, dma, dma((7,)), dma((7,))],
        compiler_params=pltpu.CompilerParams(vmem_limit_bytes=VMEM_BYTES, collective_id=0, has_side_effects=True),
        name="tail",
    )(part, tok_hidden, g_mlp.reshape(1, WIDTH), g_final.reshape(1, WIDTH), next_tok.reshape(1, ROWS), w_gate.T, w_up.T, w_down, w_head)
    shape = (ROWS, SLOTS, 1, HEAD)
    return y_out, k_all.reshape(shape), v_all.reshape(shape), logp.reshape(ROWS), lse.reshape(ROWS)


def solution(mesh):
    row_spec = P('dp', None)
    vec_spec = P('dp')
    cache_spec = P('dp', None, 'tp', None)
    col_spec = P(None, 'tp')
    part_spec = P('tp')
    whole_spec = P(None)
    in_specs = (row_spec, vec_spec, cache_spec, cache_spec, vec_spec, whole_spec, col_spec, part_spec, col_spec, part_spec, col_spec, part_spec, P('tp', None), whole_spec, col_spec, col_spec, P('tp', None), whole_spec, P('tp', None))
    out_specs = (row_spec, cache_spec, cache_spec, vec_spec, vec_spec)
    return jax.shard_map(local_step, mesh=mesh, in_specs=in_specs, out_specs=out_specs, check_vma=False)
```

```python
import jax
import numpy as np
import jax.numpy as jnp
from jax import lax
from jax.experimental import pallas as pl
from jax.experimental.pallas import tpu as pltpu
from jax.sharding import PartitionSpec as P

THETA = 1000000.0
EPS = 1e-6
MESH = pl.DeviceIdType.MESH
F32 = jnp.float32
BF16 = jnp.bfloat16
VMEM_BYTES = 67043328

ROWS = 128
WIDTH = 2048
HEAD = 128
SLOTS = 512
GROUP = 32
CHUNK = 256
NCH = 8
HALF = 4
TILE = 768
RING = 18


def dot(a, b):
    return lax.dot_general(a, b, (((1,), (0,)), ((), ())), preferred_element_type=F32)


def dot_t(a, b):
    return lax.dot_general(a, b, (((1,), (1,)), ((), ())), preferred_element_type=F32)


def attn_kernel(lens_ref, lenv_hbm, freq_hbm, x_hbm, g_hbm, bq_hbm, bk_hbm, bv_hbm,
                wq_hbm, wk_hbm, wv_hbm, wo_hbm, k_hbm, v_hbm,
                part_ref, ko_hbm, vo_hbm,
                lenv_ref, freq_ref, x_ref, g_ref, bq_ref, bk_ref, bv_ref,
                kbuf, vbuf, wq, wk, wv, wo, q_s, k_s, v_s, qg_s, qt_s, sc_s, pt_s, o_s, at_s, ll_s,
                wsem, ksem, vsem, kosem, vosem, insem):
    groups = ROWS // GROUP
    part = GROUP // 4
    small = [pltpu.make_async_copy(src, dst, insem.at[i]) for i, (src, dst) in enumerate((
        (x_hbm, x_ref), (lenv_hbm, lenv_ref), (freq_hbm, freq_ref), (g_hbm, g_ref), (bq_hbm, bq_ref), (bk_hbm, bk_ref), (bv_hbm, bv_ref)))]
    for c in small:
        c.start()
    for i, (src, dst) in enumerate(((wq_hbm, wq), (wk_hbm, wk), (wv_hbm, wv))):
        pltpu.make_async_copy(src, dst, wsem.at[i]).start()

    def start_in(g, hbm, buf, sem):
        for i in range(4):
            rows = pl.ds(g * GROUP + i * part, part)
            pltpu.make_async_copy(hbm.at[rows], buf.at[rows], sem.at[g]).start()

    for g in range(groups):
        start_in(g, k_hbm, kbuf, ksem)
        start_in(g, v_hbm, vbuf, vsem)
        if g == 0:
            pltpu.make_async_copy(wo_hbm, wo, wsem.at[3]).start()

    for c in small:
        c.wait()
    len_rows = jnp.broadcast_to(lenv_ref[...].astype(F32), (ROWS, ROWS)).T
    angles = len_rows * freq_ref[...]
    cos = jnp.cos(angles)
    sin = jnp.sin(angles) * jnp.where(lax.broadcasted_iota(jnp.int32, (ROWS, HEAD), 1) < HEAD // 2, -1.0, 1.0)
    seq_of = lax.broadcasted_iota(jnp.int32, (GROUP, 128), 1) // 4
    pick = lax.broadcasted_iota(jnp.int32, (GROUP, 128), 0) == seq_of
    for g in range(groups):
        ll_s[g:g + 1, :] = jnp.sum(jnp.where(pick, len_rows[g * GROUP:(g + 1) * GROUP], 0.0), axis=0, keepdims=True).astype(jnp.int32)

    x = x_ref[...].astype(F32)
    inv = lax.rsqrt(jnp.mean(x * x, axis=-1, keepdims=True) + EPS)
    normed = (x * inv * g_ref[...].astype(F32).reshape(1, WIDTH)).astype(BF16)
    for i, (src, dst) in enumerate(((wq_hbm, wq), (wk_hbm, wk), (wv_hbm, wv))):
        pltpu.make_async_copy(src, dst, wsem.at[i]).wait()

    def rope(u):
        return u * cos + pltpu.roll(u, HEAD // 2, 1) * sin

    k_s[...] = rope(dot(normed, wk[...]) + bk_ref[...].astype(F32).reshape(1, HEAD))
    v_s[...] = dot(normed, wv[...]) + bv_ref[...].astype(F32).reshape(1, HEAD)
    q_all = dot(normed, wq[...]) + bq_ref[...].astype(F32).reshape(1, 4 * HEAD)
    for h in range(4):
        q_s[h] = rope(q_all[:, h * HEAD:(h + 1) * HEAD])

    lane_seq = lax.broadcasted_iota(jnp.int32, (HEAD, 128), 1) // 4
    slot_id = lax.broadcasted_iota(jnp.int32, (SLOTS, 128), 0)
    row16 = lax.broadcasted_iota(jnp.int32, (16, HEAD), 0)
    row_seq = lax.broadcasted_iota(jnp.int32, (16, HEAD), 0) // 4

    def one_group(g, _):
        rows = pl.ds(pl.multiple_of(g * GROUP, GROUP), GROUP)
        pltpu.make_async_copy(k_hbm.at[rows], kbuf.at[rows], ksem.at[g]).wait()

        def put(new_s, buf):
            def one(i, _):
                b = g * GROUP + i
                length = lens_ref[b]
                base = pl.multiple_of((length // 16) * 16, 16)
                old = buf[b, pl.ds(base, 16), :]
                new = jnp.broadcast_to(new_s[pl.ds(b, 1), :].astype(BF16), (16, HEAD))
                buf[b, pl.ds(base, 16), :] = jnp.where(row16 == length - base, new, old)
                return 0
            lax.fori_loop(0, GROUP, one, 0, unroll=4)

        put(k_s, kbuf)
        for h in range(4):
            qg_s[pl.ds(h, GROUP, stride=4), :] = q_s[h, rows, :]
        qt_s[...] = qg_s[...].T.astype(BF16)
        qt = qt_s[...]
        zero = jnp.zeros_like(qt)
        top_half, low_half = None, None
        for p in range(GROUP // 2):
            b = g * GROUP + 2 * p
            rhs = jnp.concatenate([jnp.where(lane_seq == 2 * p, qt, zero), jnp.where(lane_seq == 2 * p + 1, qt, zero)], axis=0)
            t0 = dot(jnp.concatenate([kbuf[b, :SLOTS // 2], kbuf[b + 1, :SLOTS // 2]], axis=1), rhs)
            t1 = dot(jnp.concatenate([kbuf[b, SLOTS // 2:], kbuf[b + 1, SLOTS // 2:]], axis=1), rhs)
            top_half = t0 if top_half is None else top_half + t0
            low_half = t1 if low_half is None else low_half + t1
        sc_s[:SLOTS // 2] = top_half
        sc_s[SLOTS // 2:] = low_half
        pltpu.make_async_copy(kbuf.at[rows], ko_hbm.at[rows], kosem.at[g]).start()
        live = slot_id <= ll_s[pl.ds(g, 1), :]
        scores = jnp.where(live, sc_s[...] * (HEAD ** -0.5), -jnp.inf)
        top = jnp.max(scores, axis=0, keepdims=True)
        exps = jnp.exp(scores - top)
        sc_s[...] = exps
        recip = 1.0 / jnp.sum(exps, axis=0, keepdims=True)
        for i in range(4):
            blk = sc_s[i * 128:(i + 1) * 128, :] * recip
            pt_s[:, i * 128:(i + 1) * 128] = blk.T.astype(BF16)

        pltpu.make_async_copy(v_hbm.at[rows], vbuf.at[rows], vsem.at[g]).wait()
        put(v_s, vbuf)
        for j in range(GROUP // 4):
            b = g * GROUP + 4 * j
            probs = pt_s[16 * j:16 * j + 16, :]
            o = jnp.zeros((16, HEAD), F32)
            for i in range(0, 4, 2):
                out = dot(probs, jnp.concatenate([vbuf[b + i], vbuf[b + i + 1]], axis=1))
                o = jnp.where(row_seq == i, out[:, :HEAD], o)
                o = jnp.where(row_seq == i + 1, out[:, HEAD:], o)
            o_s[16 * j:16 * j + 16, :] = o
        pltpu.make_async_copy(vbuf.at[rows], vo_hbm.at[rows], vosem.at[g]).start()
        for h in range(4):
            at_s[rows, h * HEAD:(h + 1) * HEAD] = o_s[pl.ds(h, GROUP, stride=4), :].astype(BF16)
        return 0

    lax.fori_loop(0, groups, one_group, 0)

    pltpu.make_async_copy(wo_hbm, wo, wsem.at[3]).wait()
    attn = at_s[...]
    for c in range(NCH):
        part_ref[c] = dot(attn, wo[:, c * CHUNK:(c + 1) * CHUNK]).astype(BF16)
    for g in range(groups):
        rows = pl.ds(g * GROUP, GROUP)
        pltpu.make_async_copy(kbuf.at[rows], ko_hbm.at[rows], kosem.at[g]).wait()
        pltpu.make_async_copy(vbuf.at[rows], vo_hbm.at[rows], vosem.at[g]).wait()


def tail_kernel(ff, vocab_loc,
                part_hbm, x_hbm, gm_hbm, gf_hbm, tok_hbm, wg_hbm, wu_hbm, wd_hbm, wh_hbm,
                y_ref, logp_ref, lse_ref,
                part_ref, x_ref, gm_ref, gf_ref, tok_ref, wbuf, r1, s1, r2, a_s, m_s, hid, p2, r1b, s2, r2b, y_s, f_s, tok2, st_s, st_r,
                wsem, s_d1, r_d1, s_x1, r_x1, s_a, r_a, s_d2, r_d2, s_x2, r_x2,
                s_y, r_y, s_o, r_o, s_f, r_f, s_t, r_t, s_st, r_st, insem):
    dp = lax.axis_index('dp')
    tp = lax.axis_index('tp')
    core = lax.rem(tp, 2)
    dev = dp * 4 + tp
    partner = (dp, tp + 1 - 2 * core)
    xnext = (dp, lax.rem(tp + 2, 4))
    ynext = (1 - dp, tp)
    mine = core * HALF
    other = (1 - core) * HALF

    mlp_tiles = [(i * TILE, min(TILE, ff - i * TILE)) for i in range(-(-ff // TILE))]
    n_mlp = len(mlp_tiles)
    tail_pad = -(-mlp_tiles[-1][1] // CHUNK) * CHUNK
    vocab_half = vocab_loc // 2
    n_full = vocab_half // TILE
    n_tail = vocab_half - n_full * TILE
    n_head = n_full + (1 if n_tail else 0)
    head0 = 3 * n_mlp
    vbase = dp * vocab_half

    def mlp_copy(i):
        if i < 2 * n_mlp:
            src, (r, n) = (wg_hbm, wu_hbm)[i % 2], mlp_tiles[i // 2]
        else:
            src, (r, n) = wd_hbm, mlp_tiles[i - 2 * n_mlp]
        slot = i % RING
        return pltpu.make_async_copy(src.at[pl.ds(r, n)], wbuf.at[slot, pl.ds(0, n)], wsem.at[slot])

    def head_copy(i, n=TILE):
        slot = lax.rem(head0 + i, RING)
        start = pl.multiple_of(vbase + i * TILE, 16)
        return pltpu.make_async_copy(wh_hbm.at[pl.ds(start, n)], wbuf.at[slot, pl.ds(0, n)], wsem.at[slot])

    def start_item(i):
        if i < head0:
            mlp_copy(i).start()
        elif i - head0 < n_full:
            head_copy(i - head0).start()
        elif i - head0 < n_head:
            head_copy(i - head0, n_tail).start()

    small = [pltpu.make_async_copy(src, dst, insem.at[i]) for i, (src, dst) in enumerate((
        (part_hbm, part_ref), (x_hbm, x_ref), (gm_hbm, gm_ref), (gf_hbm, gf_ref), (tok_hbm, tok_ref)))]
    for c in small:
        c.start()
    for i in range(RING):
        start_item(i)

    barrier = pltpu.get_barrier_semaphore()
    for d in range(2):
        for t in range(4):
            @pl.when(d * 4 + t != dev)
            def _():
                pl.semaphore_signal(barrier, inc=1, device_id=(d, t), device_id_type=MESH)
    last_n = mlp_tiles[-1][1]
    if tail_pad > last_n:
        for i in (2 * n_mlp - 2, 2 * n_mlp - 1, 3 * n_mlp - 1):
            wbuf[i % RING, last_n:tail_pad, :] = jnp.zeros((tail_pad - last_n, WIDTH), BF16)
    for c in small:
        c.wait()
    pl.semaphore_wait(barrier, 7)

    def remote(src, dst, ssem, rsem, who):
        return pltpu.make_async_remote_copy(src_ref=src, dst_ref=dst, send_sem=ssem, recv_sem=rsem, device_id=who, device_id_type=MESH)

    tok_copy = remote(tok_ref, tok2, s_t, r_t, ynext)
    d1 = [remote(part_ref.at[other + j], r1.at[j], s_d1.at[j], r_d1.at[j], partner) for j in range(HALF)]
    x1 = [remote(s1.at[j], r2.at[j], s_x1.at[j], r_x1.at[j], xnext) for j in range(HALF)]
    ac = [remote(a_s.at[mine + j], a_s.at[mine + j], s_a.at[j], r_a.at[j], partner) for j in range(HALF)]
    d2 = [remote(p2.at[other + j], r1b.at[j], s_d2.at[j], r_d2.at[j], partner) for j in range(HALF)]
    x2 = [remote(s2.at[j], r2b.at[j], s_x2.at[j], r_x2.at[j], xnext) for j in range(HALF)]
    yo = [remote(y_s.at[0, mine + j], y_s.at[0, mine + j], s_o.at[j], r_o.at[j], partner) for j in range(HALF)]
    yy = [remote(y_s.at[0, mine + j], y_s.at[1, mine + j], s_y.at[j], r_y.at[j], ynext) for j in range(HALF)]
    yf = [remote(y_s.at[1, mine + j], y_s.at[1, mine + j], s_f.at[j], r_f.at[j], partner) for j in range(HALF)]

    def cols_of(c):
        return pl.ds(pl.multiple_of(c * CHUNK, CHUNK), CHUNK)

    for j in range(HALF):
        d1[j].start()
    tok_copy.start()
    for j in range(HALF):
        d1[j].wait_recv()
        s1[j] = (part_ref[mine + j].astype(F32) + r1[j].astype(F32)).astype(BF16)
        x1[j].start()
    for j in range(HALF):
        x1[j].wait_recv()
        total = s1[j].astype(F32) + r2[j].astype(F32)
        a_s[mine + j] = (x_ref[:, cols_of(mine + j)].astype(F32) + total).astype(BF16)
        ac[j].start()
    for j in range(HALF):
        ac[j].wait_recv()

    def inv_rms(src):
        total = jnp.zeros((ROWS, CHUNK), F32)
        for c in range(NCH):
            v = src[c].astype(F32)
            total = total + v * v
        return lax.rsqrt(jnp.sum(total, axis=-1, keepdims=True) * (1.0 / WIDTH) + EPS)

    inv = inv_rms(a_s)
    gm = gm_ref[...].astype(F32).reshape(1, WIDTH)
    for c in range(NCH):
        cols = slice(c * CHUNK, (c + 1) * CHUNK)
        m_s[:, cols] = (a_s[c].astype(F32) * inv * gm[:, cols]).astype(BF16)

    for i, (r, n) in enumerate(mlp_tiles):
        mlp_copy(2 * i).wait()
        mlp_copy(2 * i + 1).wait()
        gslot, uslot = (2 * i) % RING, (2 * i + 1) % RING
        pad = -(-n // CHUNK) * CHUNK
        for b in range(0, pad, CHUNK):
            gate = dot_t(m_s[...], wbuf[gslot, b:b + CHUNK, :])
            up = dot_t(m_s[...], wbuf[uslot, b:b + CHUNK, :])
            hid[:, r + b:r + b + CHUNK] = (gate * jax.nn.sigmoid(gate) * up).astype(BF16)
        start_item(2 * i + RING)
        start_item(2 * i + 1 + RING)

    for i in range(n_mlp):
        mlp_copy(2 * n_mlp + i).wait()

    def down(c):
        acc = None
        for i, (r, n) in enumerate(mlp_tiles):
            pad = -(-n // CHUNK) * CHUNK
            term = dot(hid[:, r:r + pad], wbuf[(2 * n_mlp + i) % RING, :pad, cols_of(c)])
            acc = term if acc is None else acc + term
        return acc.astype(BF16)

    def chip_sum(j):
        d2[j].wait_recv()
        s2[j] = (p2[mine + j].astype(F32) + r1b[j].astype(F32)).astype(BF16)
        x2[j].start()

    for j in range(HALF):
        theirs, ours = down(other + j), down(mine + j)
        p2[other + j] = theirs
        p2[mine + j] = ours
        d2[j].start()
        if j:
            chip_sum(j - 1)
    chip_sum(HALF - 1)
    for i in range(n_mlp):
        start_item(2 * n_mlp + i + RING)

    def forward(j):
        yy[j].wait_recv()
        yf[j].start()

    for j in range(HALF):
        x2[j].wait_recv()
        total = s2[j].astype(F32) + r2b[j].astype(F32)
        y_s[0, mine + j] = (a_s[mine + j].astype(F32) + total).astype(BF16)
        yy[j].start()
        yo[j].start()
        if j:
            forward(j - 1)
    forward(HALF - 1)
    for j in range(HALF):
        yo[j].wait_recv()
    for c in range(NCH):
        y_ref[:, c * CHUNK:(c + 1) * CHUNK] = y_s[0, c]

    gf = gf_ref[...].astype(F32).reshape(1, WIDTH)

    def final_norm(grp):
        inv = inv_rms(y_s.at[grp])
        for c in range(NCH):
            cols = slice(c * CHUNK, (c + 1) * CHUNK)
            f_s[grp * ROWS:(grp + 1) * ROWS, cols] = (y_s[grp, c].astype(F32) * inv * gf[:, cols]).astype(BF16)

    final_norm(0)
    for j in range(HALF):
        yf[j].wait_recv()
    final_norm(1)
    tok_copy.wait()

    tok = jnp.concatenate([tok_ref[...], tok2[...]], axis=1) - (tp * vocab_loc + vbase)
    row_id = lax.broadcasted_iota(jnp.int32, (8, 2 * ROWS), 0)

    def score(slot, first, n, state):
        top, tot, tgt = state
        cut = -(-n // 32) * 16
        for b, size in ((0, cut), (cut, n - cut)):
            logits = dot_t(wbuf[slot, pl.ds(b, size), :], f_s[...])
            blocks = [logits[8 * i:8 * i + 8] for i in range(size // 8)]
            peak = blocks[0]
            for v in blocks[1:]:
                peak = jnp.maximum(peak, v)
            new = jnp.maximum(top, peak)
            part_sum = None
            for i, v in enumerate(blocks):
                e = jnp.exp(v - new)
                part_sum = e if part_sum is None else part_sum + e
                tgt = jnp.where(row_id + (first + b + 8 * i) == tok, v, tgt)
            tot = tot * jnp.exp(top - new) + part_sum
            top = new
        return top, tot, tgt

    def one_tile(i, state):
        slot = lax.rem(head0 + i, RING)
        head_copy(i).wait()
        state = score(slot, i * TILE, TILE, state)

        @pl.when(i + RING < n_full)
        def _():
            head_copy(i + RING).start()
        if n_tail:
            @pl.when(i + RING == n_full)
            def _():
                head_copy(n_full, n_tail).start()
        return state

    state = (jnp.full((8, 2 * ROWS), -1e30, F32), jnp.zeros((8, 2 * ROWS), F32), jnp.zeros((8, 2 * ROWS), F32))
    state = lax.fori_loop(0, n_full, one_tile, state)
    if n_tail:
        head_copy(n_full, n_tail).wait()
        state = score((head0 + n_full) % RING, n_full * TILE, n_tail, state)
    top, tot, tgt = state
    peak = jnp.max(top, axis=0, keepdims=True)
    tot = jnp.sum(tot * jnp.exp(top - peak), axis=0, keepdims=True)
    tgt = jnp.sum(tgt, axis=0, keepdims=True)
    pad = jnp.zeros((5, ROWS), F32)
    for g in range(2):
        cols = slice(g * ROWS, (g + 1) * ROWS)
        st_s[g] = jnp.concatenate([peak[:, cols], tot[:, cols], tgt[:, cols], pad], axis=0)

    sends = []
    for k in range(1, 8):
        who = lax.rem(dev + k, 8)
        whod, whot = who // 4, lax.rem(who, 4)
        grp = lax.rem(whod + dp, 2)
        sends.append(remote(st_s.at[grp], st_r.at[dev], s_st.at[k - 1], r_st.at[k - 1], (whod, whot)))
    for c in sends:
        c.start()
    st_r[dev] = st_s[0]
    for c in sends:
        c.wait()
    stats = [st_r[i] for i in range(8)]
    peak = stats[0][0:1]
    for s in stats[1:]:
        peak = jnp.maximum(peak, s[0:1])
    tot = jnp.zeros_like(peak)
    tgt = jnp.zeros_like(peak)
    for s in stats:
        tot = tot + s[1:2] * jnp.exp(s[0:1] - peak)
        tgt = tgt + s[2:3]
    lse = peak + jnp.log(tot)
    lse_ref[...] = lse
    logp_ref[...] = tgt - lse

    for group in (d1, x1, ac, d2, x2, yo, yy, yf):
        for c in group:
            c.wait_send()


def emit_kernel(y_in, logp_in, lse_in, y_out, logp_out, lse_out):
    y_out[...] = y_in[...]
    logp_out[...] = logp_in[...]
    lse_out[...] = lse_in[...]


def local_step(tok_hidden, seq_lens, k_cache, v_cache, next_tok, g_attn, w_q, b_q, w_k, b_k, w_v, b_v, w_o, g_mlp, w_gate, w_up, w_down, g_final, w_head):
    steps = np.arange(HEAD // 2, dtype=np.float32) * np.float32(-2.0 / HEAD)
    freq = jnp.asarray(np.tile(np.power(np.float64(THETA), steps.astype(np.float64)).astype(np.float32), 2)[None])
    vm = pl.BlockSpec(memory_space=pltpu.VMEM)
    sm = pl.BlockSpec(memory_space=pltpu.SMEM)
    hb = pl.BlockSpec(memory_space=pltpu.HBM)
    dma = pltpu.SemaphoreType.DMA
    cache = jax.ShapeDtypeStruct((ROWS, SLOTS, HEAD), BF16)
    part, k_all, v_all = pl.pallas_call(
        attn_kernel,
        out_shape=(jax.ShapeDtypeStruct((NCH, ROWS, CHUNK), BF16), cache, cache),
        in_specs=[sm] + [hb] * 13,
        out_specs=(vm, hb, hb),
        scratch_shapes=[
            pltpu.VMEM((1, ROWS), jnp.int32), pltpu.VMEM((1, HEAD), F32), pltpu.VMEM((ROWS, WIDTH), BF16), pltpu.VMEM((WIDTH,), BF16),
            pltpu.VMEM((4 * HEAD,), BF16), pltpu.VMEM((HEAD,), BF16), pltpu.VMEM((HEAD,), BF16),
            pltpu.VMEM((ROWS, SLOTS, HEAD), BF16), pltpu.VMEM((ROWS, SLOTS, HEAD), BF16),
            pltpu.VMEM((WIDTH, 512), BF16), pltpu.VMEM((WIDTH, HEAD), BF16), pltpu.VMEM((WIDTH, HEAD), BF16), pltpu.VMEM((512, WIDTH), BF16),
            pltpu.VMEM((4, ROWS, HEAD), F32), pltpu.VMEM((ROWS, HEAD), F32), pltpu.VMEM((ROWS, HEAD), F32),
            pltpu.VMEM((128, HEAD), F32), pltpu.VMEM((HEAD, 128), BF16), pltpu.VMEM((SLOTS, 128), F32), pltpu.VMEM((128, SLOTS), BF16),
            pltpu.VMEM((128, HEAD), F32), pltpu.VMEM((ROWS, 512), BF16), pltpu.VMEM((8, 128), jnp.int32),
            dma((4,)), dma((4,)), dma((4,)), dma((4,)), dma((4,)), dma((7,)),
        ],
        compiler_params=pltpu.CompilerParams(vmem_limit_bytes=VMEM_BYTES),
        name="attention",
    )(seq_lens, seq_lens.reshape(1, ROWS), freq, tok_hidden, g_attn, b_q, b_k, b_v,
      w_q, w_k, w_v, w_o, k_cache.reshape(ROWS, SLOTS, HEAD), v_cache.reshape(ROWS, SLOTS, HEAD))

    ff = w_gate.shape[1]
    vocab_loc = w_head.shape[0]
    ff_pad = -(-ff // CHUNK) * CHUNK
    chunk4 = pltpu.VMEM((HALF, ROWS, CHUNK), BF16)
    chunk8 = pltpu.VMEM((NCH, ROWS, CHUNK), BF16)

    def kernel(*refs):
        tail_kernel(ff, vocab_loc, *refs)

    y_out, logp, lse = pl.pallas_call(
        kernel,
        out_shape=(jax.ShapeDtypeStruct((ROWS, WIDTH), BF16), jax.ShapeDtypeStruct((1, ROWS), F32), jax.ShapeDtypeStruct((1, ROWS), F32)),
        in_specs=[hb] * 9,
        out_specs=(vm, vm, vm),
        scratch_shapes=[
            chunk8, pltpu.VMEM((ROWS, WIDTH), BF16), pltpu.VMEM((WIDTH,), BF16), pltpu.VMEM((WIDTH,), BF16), pltpu.VMEM((1, ROWS), jnp.int32),
            pltpu.VMEM((RING, TILE, WIDTH), BF16),
            chunk4, chunk4, chunk4, chunk8, pltpu.VMEM((ROWS, WIDTH), BF16), pltpu.VMEM((ROWS, ff_pad), BF16),
            chunk8, chunk4, chunk4, chunk4, pltpu.VMEM((2, NCH, ROWS, CHUNK), BF16), pltpu.VMEM((2 * ROWS, WIDTH), BF16),
            pltpu.VMEM((1, ROWS), jnp.int32), pltpu.VMEM((2, 8, ROWS), F32), pltpu.VMEM((8, 8, ROWS), F32),
            dma((RING,)),
        ] + [dma((HALF,))] * 16 + [dma, dma, dma((7,)), dma((7,)), dma((5,))],
        compiler_params=pltpu.CompilerParams(vmem_limit_bytes=VMEM_BYTES, collective_id=0, has_side_effects=True),
        name="tail",
    )(part, tok_hidden, g_mlp, g_final, next_tok.reshape(1, ROWS), w_gate.T, w_up.T, w_down, w_head)
    vec = jax.ShapeDtypeStruct((1, ROWS), F32)
    y_out, logp, lse = pl.pallas_call(
        emit_kernel,
        out_shape=(jax.ShapeDtypeStruct((ROWS, WIDTH), BF16), vec, vec),
        in_specs=[vm] * 3,
        out_specs=(vm, vm, vm),
        name="emit",
    )(y_out, logp, lse)
    shape = (ROWS, SLOTS, 1, HEAD)
    return y_out, k_all.reshape(shape), v_all.reshape(shape), logp.reshape(ROWS), lse.reshape(ROWS)


def solution(mesh):
    row_spec = P('dp', None)
    vec_spec = P('dp')
    cache_spec = P('dp', None, 'tp', None)
    col_spec = P(None, 'tp')
    part_spec = P('tp')
    whole_spec = P(None)
    in_specs = (row_spec, vec_spec, cache_spec, cache_spec, vec_spec, whole_spec, col_spec, part_spec, col_spec, part_spec, col_spec, part_spec, P('tp', None), whole_spec, col_spec, col_spec, P('tp', None), whole_spec, P('tp', None))
    out_specs = (row_spec, cache_spec, cache_spec, vec_spec, vec_spec)
    return jax.shard_map(local_step, mesh=mesh, in_specs=in_specs, out_specs=out_specs, check_vma=False)
```

```python
import jax
import numpy as np
import jax.numpy as jnp
from jax import lax
from jax.experimental import pallas as pl
from jax.experimental.pallas import tpu as pltpu
from jax.sharding import PartitionSpec as P

THETA = 1000000.0
EPS = 1e-6
MESH = pl.DeviceIdType.MESH
F32 = jnp.float32
BF16 = jnp.bfloat16
VMEM_BYTES = 67043328

ROWS = 128
WIDTH = 2048
HEAD = 128
SLOTS = 512
GROUP = 32
CHUNK = 256
NCH = 8
HALF = 4
TILE = 768
RING = 18
STEP = 4


def dot(a, b):
    return lax.dot_general(a, b, (((1,), (0,)), ((), ())), preferred_element_type=F32)


def dot_t(a, b):
    return lax.dot_general(a, b, (((1,), (1,)), ((), ())), preferred_element_type=F32)


def attn_kernel(lens_ref, lenv_hbm, freq_hbm, x_hbm, g_hbm, bq_hbm, bk_hbm, bv_hbm,
                wq_hbm, wk_hbm, wv_hbm, wo_hbm, k_hbm, v_hbm,
                part_ref, ko_hbm, vo_hbm,
                lenv_ref, freq_ref, x_ref, g_ref, bq_ref, bk_ref, bv_ref,
                kbuf, vbuf, wq, wk, wv, wo, q_s, k_s, v_s, qg_s, qt_s, sc_s, pt_s, o_s, at_s, ll_s,
                wsem, ksem, vsem, kosem, vosem, insem):
    groups = ROWS // GROUP
    part = GROUP // 4
    small = [pltpu.make_async_copy(src, dst, insem.at[i]) for i, (src, dst) in enumerate((
        (x_hbm, x_ref), (lenv_hbm, lenv_ref), (freq_hbm, freq_ref), (g_hbm, g_ref), (bq_hbm, bq_ref), (bk_hbm, bk_ref), (bv_hbm, bv_ref)))]
    for c in small:
        c.start()
    for i, (src, dst) in enumerate(((wq_hbm, wq), (wk_hbm, wk), (wv_hbm, wv))):
        pltpu.make_async_copy(src, dst, wsem.at[i]).start()

    def start_in(g, hbm, buf, sem):
        for i in range(4):
            rows = pl.ds(g * GROUP + i * part, part)
            pltpu.make_async_copy(hbm.at[rows], buf.at[rows], sem.at[g]).start()

    start_in(0, k_hbm, kbuf, ksem)
    for c in small:
        c.wait()
    start_in(0, v_hbm, vbuf, vsem)
    len_rows = jnp.broadcast_to(lenv_ref[...].astype(F32), (ROWS, ROWS)).T
    angles = len_rows * freq_ref[...]
    cos = jnp.cos(angles)
    sin = jnp.sin(angles) * jnp.where(lax.broadcasted_iota(jnp.int32, (ROWS, HEAD), 1) < HEAD // 2, -1.0, 1.0)
    seq_of = lax.broadcasted_iota(jnp.int32, (GROUP, 128), 1) // 4
    pick = lax.broadcasted_iota(jnp.int32, (GROUP, 128), 0) == seq_of
    for g in range(groups):
        ll_s[g:g + 1, :] = jnp.sum(jnp.where(pick, len_rows[g * GROUP:(g + 1) * GROUP], 0.0), axis=0, keepdims=True).astype(jnp.int32)

    x = x_ref[...].astype(F32)
    inv = lax.rsqrt(jnp.mean(x * x, axis=-1, keepdims=True) + EPS)
    normed = (x * inv * g_ref[...].astype(F32).reshape(1, WIDTH)).astype(BF16)
    for i, (src, dst) in enumerate(((wq_hbm, wq), (wk_hbm, wk), (wv_hbm, wv))):
        pltpu.make_async_copy(src, dst, wsem.at[i]).wait()

    start_in(1, k_hbm, kbuf, ksem)

    def rope(u):
        return u * cos + pltpu.roll(u, HEAD // 2, 1) * sin

    k_s[...] = rope(dot(normed, wk[...]) + bk_ref[...].astype(F32).reshape(1, HEAD))
    v_s[...] = dot(normed, wv[...]) + bv_ref[...].astype(F32).reshape(1, HEAD)
    q_all = dot(normed, wq[...]) + bq_ref[...].astype(F32).reshape(1, 4 * HEAD)
    for h in range(4):
        q_s[h] = rope(q_all[:, h * HEAD:(h + 1) * HEAD])

    lane_seq = lax.broadcasted_iota(jnp.int32, (HEAD, 128), 1) // 4
    slot_id = lax.broadcasted_iota(jnp.int32, (SLOTS, 128), 0)
    row16 = lax.broadcasted_iota(jnp.int32, (16, HEAD), 0)
    row_seq = lax.broadcasted_iota(jnp.int32, (16, HEAD), 0) // 4

    def one_group(g, _):
        rows = pl.ds(pl.multiple_of(g * GROUP, GROUP), GROUP)
        pltpu.make_async_copy(k_hbm.at[rows], kbuf.at[rows], ksem.at[g]).wait()

        @pl.when(g + 1 < groups)
        def _():
            start_in(g + 1, v_hbm, vbuf, vsem)

        @pl.when(g + 1 == groups)
        def _():
            pltpu.make_async_copy(wo_hbm, wo, wsem.at[3]).start()

        def put(new_s, buf):
            def one(i, _):
                b = g * GROUP + i
                length = lens_ref[b]
                base = pl.multiple_of((length // 16) * 16, 16)
                old = buf[b, pl.ds(base, 16), :]
                new = jnp.broadcast_to(new_s[pl.ds(b, 1), :].astype(BF16), (16, HEAD))
                buf[b, pl.ds(base, 16), :] = jnp.where(row16 == length - base, new, old)
                return 0
            lax.fori_loop(0, GROUP, one, 0, unroll=8)

        put(k_s, kbuf)
        pltpu.make_async_copy(kbuf.at[rows], ko_hbm.at[rows], kosem.at[g]).start()
        for h in range(4):
            qg_s[pl.ds(h, GROUP, stride=4), :] = q_s[h, rows, :]
        qt_s[...] = qg_s[...].T.astype(BF16)
        qt = qt_s[...]
        zero = jnp.zeros_like(qt)
        top_half, low_half = None, None
        for p in range(GROUP // 2):
            b = g * GROUP + 2 * p
            rhs = jnp.concatenate([jnp.where(lane_seq == 2 * p, qt, zero), jnp.where(lane_seq == 2 * p + 1, qt, zero)], axis=0)
            t0 = dot(jnp.concatenate([kbuf[b, :SLOTS // 2], kbuf[b + 1, :SLOTS // 2]], axis=1), rhs)
            t1 = dot(jnp.concatenate([kbuf[b, SLOTS // 2:], kbuf[b + 1, SLOTS // 2:]], axis=1), rhs)
            top_half = t0 if top_half is None else top_half + t0
            low_half = t1 if low_half is None else low_half + t1
        sc_s[:SLOTS // 2] = top_half
        sc_s[SLOTS // 2:] = low_half
        live = slot_id <= ll_s[pl.ds(g, 1), :]
        scores = jnp.where(live, sc_s[...] * (HEAD ** -0.5), -jnp.inf)
        top = jnp.max(scores, axis=0, keepdims=True)
        exps = jnp.exp(scores - top)
        sc_s[...] = exps
        recip = 1.0 / jnp.sum(exps, axis=0, keepdims=True)
        for i in range(4):
            blk = sc_s[i * 128:(i + 1) * 128, :] * recip
            pt_s[:, i * 128:(i + 1) * 128] = blk.T.astype(BF16)

        pltpu.make_async_copy(v_hbm.at[rows], vbuf.at[rows], vsem.at[g]).wait()

        @pl.when(g + 2 < groups)
        def _():
            start_in(g + 2, k_hbm, kbuf, ksem)

        put(v_s, vbuf)
        pltpu.make_async_copy(vbuf.at[rows], vo_hbm.at[rows], vosem.at[g]).start()
        for j in range(GROUP // 4):
            b = g * GROUP + 4 * j
            probs = pt_s[16 * j:16 * j + 16, :]
            o = jnp.zeros((16, HEAD), F32)
            for i in range(0, 4, 2):
                out = dot(probs, jnp.concatenate([vbuf[b + i], vbuf[b + i + 1]], axis=1))
                o = jnp.where(row_seq == i, out[:, :HEAD], o)
                o = jnp.where(row_seq == i + 1, out[:, HEAD:], o)
            o_s[16 * j:16 * j + 16, :] = o
        for h in range(4):
            at_s[rows, h * HEAD:(h + 1) * HEAD] = o_s[pl.ds(h, GROUP, stride=4), :].astype(BF16)
        return 0

    lax.fori_loop(0, groups, one_group, 0)

    pltpu.make_async_copy(wo_hbm, wo, wsem.at[3]).wait()
    attn = at_s[...]
    for c in range(NCH):
        part_ref[c] = dot(attn, wo[:, c * CHUNK:(c + 1) * CHUNK]).astype(BF16)
    for g in range(groups):
        rows = pl.ds(g * GROUP, GROUP)
        pltpu.make_async_copy(kbuf.at[rows], ko_hbm.at[rows], kosem.at[g]).wait()
        pltpu.make_async_copy(vbuf.at[rows], vo_hbm.at[rows], vosem.at[g]).wait()


def tail_kernel(ff, vocab_loc,
                part_hbm, x_hbm, gm_hbm, gf_hbm, tok_hbm, wg_hbm, wu_hbm, wd_hbm, wh_hbm,
                y_ref, logp_ref, lse_ref,
                part_ref, x_ref, gm_ref, gf_ref, tok_ref, wbuf, r1, s1, r2, a_s, m_s, hid, p2, r1b, s2, r2b, y_s, f_s, tok2, st_s, st_r,
                wsem, s_d1, r_d1, s_x1, r_x1, s_a, r_a, s_d2, r_d2, s_x2, r_x2,
                s_y, r_y, s_o, r_o, s_f, r_f, s_t, r_t, s_st, r_st, insem, ysem):
    dp = lax.axis_index('dp')
    tp = lax.axis_index('tp')
    core = lax.rem(tp, 2)
    dev = dp * 4 + tp
    partner = (dp, tp + 1 - 2 * core)
    xnext = (dp, lax.rem(tp + 2, 4))
    ynext = (1 - dp, tp)
    mine = core * HALF
    other = (1 - core) * HALF

    mlp_tiles = [(i * TILE, min(TILE, ff - i * TILE)) for i in range(-(-ff // TILE))]
    n_mlp = len(mlp_tiles)
    tail_pad = -(-mlp_tiles[-1][1] // CHUNK) * CHUNK
    vocab_half = vocab_loc // 2
    n_full = vocab_half // TILE
    n_tail = vocab_half - n_full * TILE
    n_head = n_full + (1 if n_tail else 0)
    assert n_full % STEP == 0 and n_tail
    head0 = 3 * n_mlp
    vbase = dp * vocab_half

    def mlp_copy(i):
        if i < 2 * n_mlp:
            src, (r, n) = (wg_hbm, wu_hbm)[i % 2], mlp_tiles[i // 2]
        else:
            src, (r, n) = wd_hbm, mlp_tiles[i - 2 * n_mlp]
        slot = i % RING
        return pltpu.make_async_copy(src.at[pl.ds(r, n)], wbuf.at[slot, pl.ds(0, n)], wsem.at[slot])

    def head_copy(i, n=TILE):
        slot = lax.rem(head0 + i, RING)
        start = pl.multiple_of(vbase + i * TILE, 16)
        return pltpu.make_async_copy(wh_hbm.at[pl.ds(start, n)], wbuf.at[slot, pl.ds(0, n)], wsem.at[slot])

    def start_item(i):
        if i < head0:
            mlp_copy(i).start()
        elif i - head0 < n_full:
            head_copy(i - head0).start()
        elif i - head0 < n_head:
            head_copy(i - head0, n_tail).start()

    small = [pltpu.make_async_copy(src, dst, insem.at[i]) for i, (src, dst) in enumerate((
        (part_hbm, part_ref), (x_hbm, x_ref), (gm_hbm, gm_ref), (gf_hbm, gf_ref), (tok_hbm, tok_ref)))]
    for c in small:
        c.start()
    issued = [0]

    def issue(n, freed=0):
        for _ in range(n):
            if issued[0] < RING + freed:
                start_item(issued[0])
                issued[0] += 1

    issue(2)

    barrier = pltpu.get_barrier_semaphore()
    for d in range(2):
        for t in range(4):
            @pl.when(d * 4 + t != dev)
            def _():
                pl.semaphore_signal(barrier, inc=1, device_id=(d, t), device_id_type=MESH)
    last_n = mlp_tiles[-1][1]
    if tail_pad > last_n:
        for i in (2 * n_mlp - 2, 2 * n_mlp - 1, 3 * n_mlp - 1):
            wbuf[i % RING, last_n:tail_pad, :] = jnp.zeros((tail_pad - last_n, WIDTH), BF16)
    for c in small:
        c.wait()
    pl.semaphore_wait(barrier, 7)
    issue(2)

    def remote(src, dst, ssem, rsem, who):
        return pltpu.make_async_remote_copy(src_ref=src, dst_ref=dst, send_sem=ssem, recv_sem=rsem, device_id=who, device_id_type=MESH)

    tok_copy = remote(tok_ref, tok2, s_t, r_t, ynext)
    d1 = [remote(part_ref.at[other + j], r1.at[j], s_d1.at[j], r_d1.at[j], partner) for j in range(HALF)]
    x1 = [remote(s1.at[j], r2.at[j], s_x1.at[j], r_x1.at[j], xnext) for j in range(HALF)]
    ac = [remote(a_s.at[mine + j], a_s.at[mine + j], s_a.at[j], r_a.at[j], partner) for j in range(HALF)]
    d2 = [remote(p2.at[other + j], r1b.at[j], s_d2.at[j], r_d2.at[j], partner) for j in range(HALF)]
    x2 = [remote(s2.at[j], r2b.at[j], s_x2.at[j], r_x2.at[j], xnext) for j in range(HALF)]
    yo = [remote(y_s.at[0, mine + j], y_s.at[0, mine + j], s_o.at[j], r_o.at[j], partner) for j in range(HALF)]
    yy = [remote(y_s.at[0, mine + j], y_s.at[1, mine + j], s_y.at[j], r_y.at[j], ynext) for j in range(HALF)]
    yf = [remote(y_s.at[1, mine + j], y_s.at[1, mine + j], s_f.at[j], r_f.at[j], partner) for j in range(HALF)]

    def cols_of(c):
        return pl.ds(pl.multiple_of(c * CHUNK, CHUNK), CHUNK)

    for j in range(HALF):
        d1[j].start()
    tok_copy.start()
    for j in range(HALF):
        d1[j].wait_recv()
        s1[j] = (part_ref[mine + j].astype(F32) + r1[j].astype(F32)).astype(BF16)
        x1[j].start()
    issue(2)
    for j in range(HALF):
        x1[j].wait_recv()
        issue(2 if j % 2 == 0 else 1)
        total = s1[j].astype(F32) + r2[j].astype(F32)
        a_s[mine + j] = (x_ref[:, cols_of(mine + j)].astype(F32) + total).astype(BF16)
        ac[j].start()
    for j in range(HALF):
        ac[j].wait_recv()
    issue(1)

    def inv_rms(src):
        total = jnp.zeros((ROWS, CHUNK), F32)
        for c in range(NCH):
            v = src[c].astype(F32)
            total = total + v * v
        return lax.rsqrt(jnp.sum(total, axis=-1, keepdims=True) * (1.0 / WIDTH) + EPS)

    inv = inv_rms(a_s)
    gm = gm_ref[...].astype(F32).reshape(1, WIDTH)
    for c in range(NCH):
        cols = slice(c * CHUNK, (c + 1) * CHUNK)
        m_s[:, cols] = (a_s[c].astype(F32) * inv * gm[:, cols]).astype(BF16)

    for i, (r, n) in enumerate(mlp_tiles):
        mlp_copy(2 * i).wait()
        mlp_copy(2 * i + 1).wait()
        gslot, uslot = (2 * i) % RING, (2 * i + 1) % RING
        pad = -(-n // CHUNK) * CHUNK
        for b in range(0, pad, CHUNK):
            gate = dot_t(m_s[...], wbuf[gslot, b:b + CHUNK, :])
            up = dot_t(m_s[...], wbuf[uslot, b:b + CHUNK, :])
            hid[:, r + b:r + b + CHUNK] = (gate * jax.nn.sigmoid(gate) * up).astype(BF16)
            issue(1, 2 * i)

    for i in range(n_mlp):
        mlp_copy(2 * n_mlp + i).wait()

    def down(c):
        acc = None
        for i, (r, n) in enumerate(mlp_tiles):
            pad = -(-n // CHUNK) * CHUNK
            term = dot(hid[:, r:r + pad], wbuf[(2 * n_mlp + i) % RING, :pad, cols_of(c)])
            acc = term if acc is None else acc + term
        return acc.astype(BF16)

    def chip_sum(j):
        d2[j].wait_recv()
        s2[j] = (p2[mine + j].astype(F32) + r1b[j].astype(F32)).astype(BF16)
        x2[j].start()

    for j in range(HALF):
        theirs, ours = down(other + j), down(mine + j)
        p2[other + j] = theirs
        p2[mine + j] = ours
        d2[j].start()
        issue(1, 2 * n_mlp)
        if j:
            chip_sum(j - 1)
    chip_sum(HALF - 1)
    issue(1, 3 * n_mlp)

    def forward(j):
        yy[j].wait_recv()
        yf[j].start()

    for j in range(HALF):
        x2[j].wait_recv()
        issue(2, 3 * n_mlp)
        total = s2[j].astype(F32) + r2b[j].astype(F32)
        y_s[0, mine + j] = (a_s[mine + j].astype(F32) + total).astype(BF16)
        yy[j].start()
        yo[j].start()
        if j:
            forward(j - 1)
    forward(HALF - 1)
    for j in range(HALF):
        yo[j].wait_recv()
    issue(RING, 3 * n_mlp)
    y_out = [pltpu.make_async_copy(y_s.at[0, c], y_ref.at[:, pl.ds(c * CHUNK, CHUNK)], ysem.at[c]) for c in range(NCH)]
    for c in y_out:
        c.start()

    gf = gf_ref[...].astype(F32).reshape(1, WIDTH)

    def final_norm(grp):
        inv = inv_rms(y_s.at[grp])
        for c in range(NCH):
            cols = slice(c * CHUNK, (c + 1) * CHUNK)
            f_s[grp * ROWS:(grp + 1) * ROWS, cols] = (y_s[grp, c].astype(F32) * inv * gf[:, cols]).astype(BF16)

    final_norm(0)
    for j in range(HALF):
        yf[j].wait_recv()
    final_norm(1)
    tok_copy.wait()

    tok = jnp.concatenate([tok_ref[...], tok2[...]], axis=1) - (tp * vocab_loc + vbase)
    row_id = lax.broadcasted_iota(jnp.int32, (8, 2 * ROWS), 0)

    def score(slot, at, size, first, state):
        top, tot, tgt = state
        logits = dot_t(wbuf[slot, pl.ds(at, size), :], f_s[...])
        blocks = [logits[8 * i:8 * i + 8] for i in range(size // 8)]
        peak = blocks[0]
        for v in blocks[1:]:
            peak = jnp.maximum(peak, v)
        new = jnp.maximum(top, peak)
        part_sum = None
        for i, v in enumerate(blocks):
            e = jnp.exp(v - new)
            part_sum = e if part_sum is None else part_sum + e
            tgt = jnp.where(row_id + (first + 8 * i) == tok, v, tgt)
        tot = tot * jnp.exp(top - new) + part_sum
        return new, tot, tgt

    def some_tiles(k, state):
        for t in range(STEP):
            head_copy(k * STEP + t).wait()
        for t in range(STEP):
            i = k * STEP + t
            for b in range(0, TILE, CHUNK):
                state = score(lax.rem(head0 + i, RING), b, CHUNK, i * TILE + b, state)
        for t in range(STEP):
            i = k * STEP + t

            @pl.when(i + RING < n_full)
            def _():
                head_copy(i + RING).start()
            if n_tail:
                @pl.when(i + RING == n_full)
                def _():
                    head_copy(n_full, n_tail).start()
        return state

    state = (jnp.full((8, 2 * ROWS), -1e30, F32), jnp.zeros((8, 2 * ROWS), F32), jnp.zeros((8, 2 * ROWS), F32))
    state = lax.fori_loop(0, n_full // STEP, some_tiles, state)
    head_copy(n_full, n_tail).wait()
    cut = -(-n_tail // 32) * 16
    for b, size in ((0, cut), (cut, n_tail - cut)):
        state = score((head0 + n_full) % RING, b, size, n_full * TILE + b, state)
    top, tot, tgt = state
    peak = jnp.max(top, axis=0, keepdims=True)
    tot = jnp.sum(tot * jnp.exp(top - peak), axis=0, keepdims=True)
    tgt = jnp.sum(tgt, axis=0, keepdims=True)
    pad = jnp.zeros((5, ROWS), F32)
    for g in range(2):
        cols = slice(g * ROWS, (g + 1) * ROWS)
        st_s[g] = jnp.concatenate([peak[:, cols], tot[:, cols], tgt[:, cols], pad], axis=0)

    sends = []
    for k in range(1, 8):
        who = lax.rem(dev + k, 8)
        whod, whot = who // 4, lax.rem(who, 4)
        grp = lax.rem(whod + dp, 2)
        sends.append(remote(st_s.at[grp], st_r.at[dev], s_st.at[k - 1], r_st.at[k - 1], (whod, whot)))
    for c in sends:
        c.start()
    st_r[dev] = st_s[0]
    for c in sends:
        c.wait()
    stats = [st_r[i] for i in range(8)]
    peak = stats[0][0:1]
    for s in stats[1:]:
        peak = jnp.maximum(peak, s[0:1])
    tot = jnp.zeros_like(peak)
    tgt = jnp.zeros_like(peak)
    for s in stats:
        tot = tot + s[1:2] * jnp.exp(s[0:1] - peak)
        tgt = tgt + s[2:3]
    lse = peak + jnp.log(tot)
    lse_ref[...] = lse
    logp_ref[...] = tgt - lse

    for group in (d1, x1, ac, d2, x2, yo, yy, yf):
        for c in group:
            c.wait_send()
    for c in y_out:
        c.wait()


def emit_kernel(y_in, logp_in, lse_in, y_out, logp_out, lse_out):
    y_out[...] = y_in[...]
    logp_out[...] = logp_in[...]
    lse_out[...] = lse_in[...]


def local_step(tok_hidden, seq_lens, k_cache, v_cache, next_tok, g_attn, w_q, b_q, w_k, b_k, w_v, b_v, w_o, g_mlp, w_gate, w_up, w_down, g_final, w_head):
    steps = np.arange(HEAD // 2, dtype=np.float32) * np.float32(-2.0 / HEAD)
    freq = jnp.asarray(np.tile(np.power(np.float64(THETA), steps.astype(np.float64)).astype(np.float32), 2)[None])
    vm = pl.BlockSpec(memory_space=pltpu.VMEM)
    sm = pl.BlockSpec(memory_space=pltpu.SMEM)
    hb = pl.BlockSpec(memory_space=pltpu.HBM)
    dma = pltpu.SemaphoreType.DMA
    cache = jax.ShapeDtypeStruct((ROWS, SLOTS, HEAD), BF16)
    part, k_all, v_all = pl.pallas_call(
        attn_kernel,
        out_shape=(jax.ShapeDtypeStruct((NCH, ROWS, CHUNK), BF16), cache, cache),
        in_specs=[sm] + [hb] * 13,
        out_specs=(vm, hb, hb),
        scratch_shapes=[
            pltpu.VMEM((1, ROWS), jnp.int32), pltpu.VMEM((1, HEAD), F32), pltpu.VMEM((ROWS, WIDTH), BF16), pltpu.VMEM((WIDTH,), BF16),
            pltpu.VMEM((4 * HEAD,), BF16), pltpu.VMEM((HEAD,), BF16), pltpu.VMEM((HEAD,), BF16),
            pltpu.VMEM((ROWS, SLOTS, HEAD), BF16), pltpu.VMEM((ROWS, SLOTS, HEAD), BF16),
            pltpu.VMEM((WIDTH, 512), BF16), pltpu.VMEM((WIDTH, HEAD), BF16), pltpu.VMEM((WIDTH, HEAD), BF16), pltpu.VMEM((512, WIDTH), BF16),
            pltpu.VMEM((4, ROWS, HEAD), F32), pltpu.VMEM((ROWS, HEAD), F32), pltpu.VMEM((ROWS, HEAD), F32),
            pltpu.VMEM((128, HEAD), F32), pltpu.VMEM((HEAD, 128), BF16), pltpu.VMEM((SLOTS, 128), F32), pltpu.VMEM((128, SLOTS), BF16),
            pltpu.VMEM((128, HEAD), F32), pltpu.VMEM((ROWS, 512), BF16), pltpu.VMEM((8, 128), jnp.int32),
            dma((4,)), dma((4,)), dma((4,)), dma((4,)), dma((4,)), dma((7,)),
        ],
        compiler_params=pltpu.CompilerParams(vmem_limit_bytes=VMEM_BYTES),
        name="attention",
    )(seq_lens, seq_lens.reshape(1, ROWS), freq, tok_hidden, g_attn, b_q, b_k, b_v,
      w_q, w_k, w_v, w_o, k_cache.reshape(ROWS, SLOTS, HEAD), v_cache.reshape(ROWS, SLOTS, HEAD))

    ff = w_gate.shape[1]
    vocab_loc = w_head.shape[0]
    ff_pad = -(-ff // CHUNK) * CHUNK
    chunk4 = pltpu.VMEM((HALF, ROWS, CHUNK), BF16)
    chunk8 = pltpu.VMEM((NCH, ROWS, CHUNK), BF16)

    def kernel(*refs):
        tail_kernel(ff, vocab_loc, *refs)

    y_out, logp, lse = pl.pallas_call(
        kernel,
        out_shape=(jax.ShapeDtypeStruct((ROWS, WIDTH), BF16), jax.ShapeDtypeStruct((1, ROWS), F32), jax.ShapeDtypeStruct((1, ROWS), F32)),
        in_specs=[hb] * 9,
        out_specs=(hb, vm, vm),
        scratch_shapes=[
            chunk8, pltpu.VMEM((ROWS, WIDTH), BF16), pltpu.VMEM((WIDTH,), BF16), pltpu.VMEM((WIDTH,), BF16), pltpu.VMEM((1, ROWS), jnp.int32),
            pltpu.VMEM((RING, TILE, WIDTH), BF16),
            chunk4, chunk4, chunk4, chunk8, pltpu.VMEM((ROWS, WIDTH), BF16), pltpu.VMEM((ROWS, ff_pad), BF16),
            chunk8, chunk4, chunk4, chunk4, pltpu.VMEM((2, NCH, ROWS, CHUNK), BF16), pltpu.VMEM((2 * ROWS, WIDTH), BF16),
            pltpu.VMEM((1, ROWS), jnp.int32), pltpu.VMEM((2, 8, ROWS), F32), pltpu.VMEM((8, 8, ROWS), F32),
            dma((RING,)),
        ] + [dma((HALF,))] * 16 + [dma, dma, dma((7,)), dma((7,)), dma((5,)), dma((NCH,))],
        compiler_params=pltpu.CompilerParams(vmem_limit_bytes=VMEM_BYTES, collective_id=0, has_side_effects=True),
        name="tail",
    )(part, tok_hidden, g_mlp, g_final, next_tok.reshape(1, ROWS), w_gate.T, w_up.T, w_down, w_head)
    vec = jax.ShapeDtypeStruct((1, ROWS), F32)
    y_out, logp, lse = pl.pallas_call(
        emit_kernel,
        out_shape=(jax.ShapeDtypeStruct((ROWS, WIDTH), BF16), vec, vec),
        in_specs=[vm] * 3,
        out_specs=(vm, vm, vm),
        name="emit",
    )(y_out, logp, lse)
    shape = (ROWS, SLOTS, 1, HEAD)
    return y_out, k_all.reshape(shape), v_all.reshape(shape), logp.reshape(ROWS), lse.reshape(ROWS)


def solution(mesh):
    row_spec = P('dp', None)
    vec_spec = P('dp')
    cache_spec = P('dp', None, 'tp', None)
    col_spec = P(None, 'tp')
    part_spec = P('tp')
    whole_spec = P(None)
    in_specs = (row_spec, vec_spec, cache_spec, cache_spec, vec_spec, whole_spec, col_spec, part_spec, col_spec, part_spec, col_spec, part_spec, P('tp', None), whole_spec, col_spec, col_spec, P('tp', None), whole_spec, P('tp', None))
    out_specs = (row_spec, cache_spec, cache_spec, vec_spec, vec_spec)
    return jax.shard_map(local_step, mesh=mesh, in_specs=in_specs, out_specs=out_specs, check_vma=False)
```

```python
import jax
import numpy as np
import jax.numpy as jnp
from jax import lax
from jax.experimental import pallas as pl
from jax.experimental.pallas import tpu as pltpu
from jax.sharding import PartitionSpec as P

THETA = 1000000.0
EPS = 1e-6
MESH = pl.DeviceIdType.MESH
F32 = jnp.float32
BF16 = jnp.bfloat16
VMEM_BYTES = 67043328

ROWS = 128
WIDTH = 2048
HEAD = 128
SLOTS = 512
GROUP = 32
CHUNK = 128
NCH = 16
HALF = 8
BLOCK = 256
TILE = 768
RING = 18
STEP = 4


def dot(a, b):
    return lax.dot_general(a, b, (((1,), (0,)), ((), ())), preferred_element_type=F32)


def dot_t(a, b):
    return lax.dot_general(a, b, (((1,), (1,)), ((), ())), preferred_element_type=F32)


def attn_kernel(lens_ref, lenv_hbm, freq_hbm, x_hbm, g_hbm, bq_hbm, bk_hbm, bv_hbm,
                wq_hbm, wk_hbm, wv_hbm, wo_hbm, k_hbm, v_hbm,
                part_hbm, ko_hbm, vo_hbm,
                part_ref, lenv_ref, freq_ref, x_ref, g_ref, bq_ref, bk_ref, bv_ref,
                kbuf, vbuf, wq, wk, wv, wo, q_s, k_s, v_s, qg_s, qt_s, sc_s, pt_s, o_s, at_s, ll_s,
                wsem, ksem, vsem, kosem, vosem, insem):
    groups = ROWS // GROUP
    part = GROUP // 4
    small = [pltpu.make_async_copy(src, dst, insem.at[i]) for i, (src, dst) in enumerate((
        (x_hbm, x_ref), (lenv_hbm, lenv_ref), (freq_hbm, freq_ref), (g_hbm, g_ref), (bq_hbm, bq_ref), (bk_hbm, bk_ref), (bv_hbm, bv_ref)))]
    for c in small:
        c.start()
    for i, (src, dst) in enumerate(((wq_hbm, wq), (wk_hbm, wk), (wv_hbm, wv))):
        pltpu.make_async_copy(src, dst, wsem.at[i]).start()

    def start_in(g, hbm, buf, sem):
        for i in range(4):
            rows = pl.ds(g * GROUP + i * part, part)
            pltpu.make_async_copy(hbm.at[rows], buf.at[rows], sem.at[g]).start()

    start_in(0, k_hbm, kbuf, ksem)
    for c in small:
        c.wait()
    start_in(0, v_hbm, vbuf, vsem)
    len_rows = jnp.broadcast_to(lenv_ref[...].astype(F32), (ROWS, ROWS)).T
    angles = len_rows * freq_ref[...]
    cos = jnp.cos(angles)
    sin = jnp.sin(angles) * jnp.where(lax.broadcasted_iota(jnp.int32, (ROWS, HEAD), 1) < HEAD // 2, -1.0, 1.0)
    seq_of = lax.broadcasted_iota(jnp.int32, (GROUP, 128), 1) // 4
    pick = lax.broadcasted_iota(jnp.int32, (GROUP, 128), 0) == seq_of
    for g in range(groups):
        ll_s[g:g + 1, :] = jnp.sum(jnp.where(pick, len_rows[g * GROUP:(g + 1) * GROUP], 0.0), axis=0, keepdims=True).astype(jnp.int32)

    x = x_ref[...].astype(F32)
    inv = lax.rsqrt(jnp.mean(x * x, axis=-1, keepdims=True) + EPS)
    normed = (x * inv * g_ref[...].astype(F32).reshape(1, WIDTH)).astype(BF16)
    for i, (src, dst) in enumerate(((wq_hbm, wq), (wk_hbm, wk), (wv_hbm, wv))):
        pltpu.make_async_copy(src, dst, wsem.at[i]).wait()

    start_in(1, k_hbm, kbuf, ksem)

    def rope(u):
        return u * cos + pltpu.roll(u, HEAD // 2, 1) * sin

    k_s[...] = rope(dot(normed, wk[...]) + bk_ref[...].astype(F32).reshape(1, HEAD))
    v_s[...] = dot(normed, wv[...]) + bv_ref[...].astype(F32).reshape(1, HEAD)
    q_all = dot(normed, wq[...]) + bq_ref[...].astype(F32).reshape(1, 4 * HEAD)
    for h in range(4):
        q_s[h] = rope(q_all[:, h * HEAD:(h + 1) * HEAD])

    lane_seq = lax.broadcasted_iota(jnp.int32, (HEAD, 128), 1) // 4
    slot_id = lax.broadcasted_iota(jnp.int32, (SLOTS, 128), 0)
    row16 = lax.broadcasted_iota(jnp.int32, (16, HEAD), 0)
    row_seq = lax.broadcasted_iota(jnp.int32, (16, HEAD), 0) // 4

    def start_out(g):
        rows = pl.ds(g * GROUP, GROUP)
        pltpu.make_async_copy(kbuf.at[rows], ko_hbm.at[rows], kosem.at[g]).start()
        pltpu.make_async_copy(vbuf.at[rows], vo_hbm.at[rows], vosem.at[g]).start()

    def one_group(g, _):
        rows = pl.ds(pl.multiple_of(g * GROUP, GROUP), GROUP)
        pltpu.make_async_copy(k_hbm.at[rows], kbuf.at[rows], ksem.at[g]).wait()

        @pl.when(g + 1 < groups)
        def _():
            start_in(g + 1, v_hbm, vbuf, vsem)

        @pl.when(g + 1 == groups)
        def _():
            pltpu.make_async_copy(wo_hbm, wo, wsem.at[3]).start()

        def put(new_s, buf):
            def one(i, _):
                b = g * GROUP + i
                length = lens_ref[b]
                base = pl.multiple_of((length // 16) * 16, 16)
                old = buf[b, pl.ds(base, 16), :]
                new = jnp.broadcast_to(new_s[pl.ds(b, 1), :].astype(BF16), (16, HEAD))
                buf[b, pl.ds(base, 16), :] = jnp.where(row16 == length - base, new, old)
                return 0
            lax.fori_loop(0, GROUP, one, 0, unroll=8)

        put(k_s, kbuf)

        @pl.when(g + 1 == groups)
        def _():
            for i in range(groups - 1):
                start_out(i)
            pltpu.make_async_copy(kbuf.at[rows], ko_hbm.at[rows], kosem.at[g]).start()

        for h in range(4):
            qg_s[pl.ds(h, GROUP, stride=4), :] = q_s[h, rows, :]
        qt_s[...] = qg_s[...].T.astype(BF16)
        qt = qt_s[...]
        zero = jnp.zeros_like(qt)
        top_half, low_half = None, None
        for p in range(GROUP // 2):
            b = g * GROUP + 2 * p
            rhs = jnp.concatenate([jnp.where(lane_seq == 2 * p, qt, zero), jnp.where(lane_seq == 2 * p + 1, qt, zero)], axis=0)
            t0 = dot(jnp.concatenate([kbuf[b, :SLOTS // 2], kbuf[b + 1, :SLOTS // 2]], axis=1), rhs)
            t1 = dot(jnp.concatenate([kbuf[b, SLOTS // 2:], kbuf[b + 1, SLOTS // 2:]], axis=1), rhs)
            top_half = t0 if top_half is None else top_half + t0
            low_half = t1 if low_half is None else low_half + t1
        sc_s[:SLOTS // 2] = top_half
        sc_s[SLOTS // 2:] = low_half
        live = slot_id <= ll_s[pl.ds(g, 1), :]
        scores = jnp.where(live, sc_s[...] * (HEAD ** -0.5), -jnp.inf)
        top = jnp.max(scores, axis=0, keepdims=True)
        exps = jnp.exp(scores - top)
        sc_s[...] = exps
        recip = 1.0 / jnp.sum(exps, axis=0, keepdims=True)
        for i in range(4):
            blk = sc_s[i * 128:(i + 1) * 128, :] * recip
            pt_s[:, i * 128:(i + 1) * 128] = blk.T.astype(BF16)

        pltpu.make_async_copy(v_hbm.at[rows], vbuf.at[rows], vsem.at[g]).wait()

        @pl.when(g + 2 < groups)
        def _():
            start_in(g + 2, k_hbm, kbuf, ksem)

        put(v_s, vbuf)

        @pl.when(g + 1 == groups)
        def _():
            pltpu.make_async_copy(vbuf.at[rows], vo_hbm.at[rows], vosem.at[g]).start()

        for j in range(GROUP // 4):
            b = g * GROUP + 4 * j
            probs = pt_s[16 * j:16 * j + 16, :]
            o = jnp.zeros((16, HEAD), F32)
            for i in range(0, 4, 2):
                out = dot(probs, jnp.concatenate([vbuf[b + i], vbuf[b + i + 1]], axis=1))
                o = jnp.where(row_seq == i, out[:, :HEAD], o)
                o = jnp.where(row_seq == i + 1, out[:, HEAD:], o)
            o_s[16 * j:16 * j + 16, :] = o
        for h in range(4):
            at_s[rows, h * HEAD:(h + 1) * HEAD] = o_s[pl.ds(h, GROUP, stride=4), :].astype(BF16)
        return 0

    lax.fori_loop(0, groups, one_group, 0)

    pltpu.make_async_copy(wo_hbm, wo, wsem.at[3]).wait()
    attn = at_s[...]
    for c in range(WIDTH // BLOCK):
        block = dot(attn, wo[:, c * BLOCK:(c + 1) * BLOCK]).astype(BF16)
        part_ref[2 * c] = block[:, :CHUNK]
        part_ref[2 * c + 1] = block[:, CHUNK:]
    part_copy = pltpu.make_async_copy(part_ref, part_hbm, insem.at[7])
    part_copy.start()
    part_copy.wait()
    for g in range(groups):
        rows = pl.ds(g * GROUP, GROUP)
        pltpu.make_async_copy(kbuf.at[rows], ko_hbm.at[rows], kosem.at[g]).wait()
        pltpu.make_async_copy(vbuf.at[rows], vo_hbm.at[rows], vosem.at[g]).wait()


def tail_kernel(ff, vocab_loc,
                part_hbm, x_hbm, gm_hbm, gf_hbm, tok_hbm, wg_hbm, wu_hbm, wd_hbm, wh_hbm,
                y_ref, logp_ref, lse_ref,
                part_ref, x_ref, gm_ref, gf_ref, tok_ref, wbuf, r1, s1, r2, a_s, m_s, hid, p2, r1b, s2, r2b, y_s, f_s, tok2, st_s, st_r,
                wsem, s_d1, r_d1, s_x1, r_x1, s_a, r_a, s_d2, r_d2, s_x2, r_x2,
                s_y, r_y, s_o, r_o, s_f, r_f, s_t, r_t, s_st, r_st, insem, ysem):
    dp = lax.axis_index('dp')
    tp = lax.axis_index('tp')
    core = lax.rem(tp, 2)
    dev = dp * 4 + tp
    partner = (dp, tp + 1 - 2 * core)
    xnext = (dp, lax.rem(tp + 2, 4))
    ynext = (1 - dp, tp)
    mine = core * HALF
    other = (1 - core) * HALF

    mlp_tiles = [(i * TILE, min(TILE, ff - i * TILE)) for i in range(-(-ff // TILE))]
    n_mlp = len(mlp_tiles)
    tail_pad = -(-mlp_tiles[-1][1] // BLOCK) * BLOCK
    vocab_half = vocab_loc // 2
    n_full = vocab_half // TILE
    n_tail = vocab_half - n_full * TILE
    n_head = n_full + (1 if n_tail else 0)
    assert n_full % STEP == 0 and n_tail
    head0 = 3 * n_mlp
    vbase = dp * vocab_half

    def mlp_copy(i):
        if i < 2 * n_mlp:
            src, (r, n) = (wg_hbm, wu_hbm)[i % 2], mlp_tiles[i // 2]
        else:
            src, (r, n) = wd_hbm, mlp_tiles[i - 2 * n_mlp]
        slot = i % RING
        return pltpu.make_async_copy(src.at[pl.ds(r, n)], wbuf.at[slot, pl.ds(0, n)], wsem.at[slot])

    def head_copy(i, n=TILE):
        slot = lax.rem(head0 + i, RING)
        start = pl.multiple_of(vbase + i * TILE, 16)
        return pltpu.make_async_copy(wh_hbm.at[pl.ds(start, n)], wbuf.at[slot, pl.ds(0, n)], wsem.at[slot])

    def start_item(i):
        if i < head0:
            mlp_copy(i).start()
        elif i - head0 < n_full:
            head_copy(i - head0).start()
        elif i - head0 < n_head:
            head_copy(i - head0, n_tail).start()

    small = [pltpu.make_async_copy(src, dst, insem.at[i]) for i, (src, dst) in enumerate((
        (part_hbm, part_ref), (x_hbm, x_ref), (gm_hbm, gm_ref), (gf_hbm, gf_ref), (tok_hbm, tok_ref)))]
    for c in small:
        c.start()
    issued = [0]

    def issue(n, freed=0):
        for _ in range(n):
            if issued[0] < RING + freed:
                start_item(issued[0])
                issued[0] += 1

    issue(2)

    barrier = pltpu.get_barrier_semaphore()
    for d in range(2):
        for t in range(4):
            @pl.when(d * 4 + t != dev)
            def _():
                pl.semaphore_signal(barrier, inc=1, device_id=(d, t), device_id_type=MESH)
    last_n = mlp_tiles[-1][1]
    if tail_pad > last_n:
        for i in (2 * n_mlp - 2, 2 * n_mlp - 1, 3 * n_mlp - 1):
            wbuf[i % RING, last_n:tail_pad, :] = jnp.zeros((tail_pad - last_n, WIDTH), BF16)
    for c in small:
        c.wait()
    pl.semaphore_wait(barrier, 7)
    issue(2)

    def remote(src, dst, ssem, rsem, who):
        return pltpu.make_async_remote_copy(src_ref=src, dst_ref=dst, send_sem=ssem, recv_sem=rsem, device_id=who, device_id_type=MESH)

    tok_copy = remote(tok_ref, tok2, s_t, r_t, ynext)
    d1 = [remote(part_ref.at[other + j], r1.at[j], s_d1.at[j], r_d1.at[j], partner) for j in range(HALF)]
    x1 = [remote(s1.at[j], r2.at[j], s_x1.at[j], r_x1.at[j], xnext) for j in range(HALF)]
    ac = [remote(a_s.at[mine + j], a_s.at[mine + j], s_a.at[j], r_a.at[j], partner) for j in range(HALF)]
    d2 = [remote(p2.at[other + j], r1b.at[j], s_d2.at[j], r_d2.at[j], partner) for j in range(HALF)]
    x2 = [remote(s2.at[j], r2b.at[j], s_x2.at[j], r_x2.at[j], xnext) for j in range(HALF)]
    yo = [remote(y_s.at[0, mine + j], y_s.at[0, mine + j], s_o.at[j], r_o.at[j], partner) for j in range(HALF)]
    yy = [remote(y_s.at[0, mine + j], y_s.at[1, mine + j], s_y.at[j], r_y.at[j], ynext) for j in range(HALF)]
    yf = [remote(y_s.at[1, mine + j], y_s.at[1, mine + j], s_f.at[j], r_f.at[j], partner) for j in range(HALF)]

    def cols_of(c):
        return pl.ds(pl.multiple_of(c * CHUNK, CHUNK), CHUNK)

    for j in range(HALF):
        d1[j].start()
    tok_copy.start()
    for j in range(HALF):
        d1[j].wait_recv()
        s1[j] = (part_ref[mine + j].astype(F32) + r1[j].astype(F32)).astype(BF16)
        x1[j].start()
    issue(2)
    for j in range(HALF):
        x1[j].wait_recv()
        issue(1 if j % 4 < 3 else 0)
        total = s1[j].astype(F32) + r2[j].astype(F32)
        a_s[mine + j] = (x_ref[:, cols_of(mine + j)].astype(F32) + total).astype(BF16)
        ac[j].start()
    for j in range(HALF):
        ac[j].wait_recv()
    issue(1)

    def inv_rms(src):
        total = jnp.zeros((ROWS, CHUNK), F32)
        for c in range(NCH):
            v = src[c].astype(F32)
            total = total + v * v
        return lax.rsqrt(jnp.sum(total, axis=-1, keepdims=True) * (1.0 / WIDTH) + EPS)

    inv = inv_rms(a_s)
    gm = gm_ref[...].astype(F32).reshape(1, WIDTH)
    for c in range(NCH):
        cols = slice(c * CHUNK, (c + 1) * CHUNK)
        m_s[:, cols] = (a_s[c].astype(F32) * inv * gm[:, cols]).astype(BF16)

    for i, (r, n) in enumerate(mlp_tiles):
        mlp_copy(2 * i).wait()
        mlp_copy(2 * i + 1).wait()
        gslot, uslot = (2 * i) % RING, (2 * i + 1) % RING
        pad = -(-n // BLOCK) * BLOCK
        for b in range(0, pad, BLOCK):
            gate = dot_t(m_s[...], wbuf[gslot, b:b + BLOCK, :])
            up = dot_t(m_s[...], wbuf[uslot, b:b + BLOCK, :])
            hid[:, r + b:r + b + BLOCK] = (gate * jax.nn.sigmoid(gate) * up).astype(BF16)
            issue(1, 2 * i)

    for i in range(n_mlp):
        mlp_copy(2 * n_mlp + i).wait()

    def down(base, j):
        cols = pl.ds(pl.multiple_of((base + 2 * j) * CHUNK, BLOCK), BLOCK)
        acc = None
        for i, (r, n) in enumerate(mlp_tiles):
            pad = -(-n // BLOCK) * BLOCK
            term = dot(hid[:, r:r + pad], wbuf[(2 * n_mlp + i) % RING, :pad, cols])
            acc = term if acc is None else acc + term
        return acc.astype(BF16)

    def chip_sum(j):
        d2[j].wait_recv()
        s2[j] = (p2[mine + j].astype(F32) + r1b[j].astype(F32)).astype(BF16)
        x2[j].start()

    for j in range(HALF // 2):
        theirs, ours = down(other, j), down(mine, j)
        for i in range(2):
            cols = slice(i * CHUNK, (i + 1) * CHUNK)
            p2[other + 2 * j + i] = theirs[:, cols]
            p2[mine + 2 * j + i] = ours[:, cols]
        for i in range(2):
            d2[2 * j + i].start()
        issue(1, 2 * n_mlp)
        if j:
            chip_sum(2 * j - 2)
            chip_sum(2 * j - 1)
    chip_sum(HALF - 2)
    chip_sum(HALF - 1)
    issue(1, 3 * n_mlp)

    def forward(j):
        yy[j].wait_recv()
        yf[j].start()

    for j in range(HALF):
        x2[j].wait_recv()
        issue(1, 3 * n_mlp)
        total = s2[j].astype(F32) + r2b[j].astype(F32)
        y_s[0, mine + j] = (a_s[mine + j].astype(F32) + total).astype(BF16)
        yy[j].start()
        yo[j].start()
        if j:
            forward(j - 1)
    forward(HALF - 1)
    for j in range(HALF):
        yo[j].wait_recv()
    issue(RING, 3 * n_mlp)
    y_out = [pltpu.make_async_copy(y_s.at[0, c], y_ref.at[:, pl.ds(c * CHUNK, CHUNK)], ysem.at[c]) for c in range(NCH)]
    for c in y_out:
        c.start()

    gf = gf_ref[...].astype(F32).reshape(1, WIDTH)

    def final_norm(grp):
        inv = inv_rms(y_s.at[grp])
        for c in range(NCH):
            cols = slice(c * CHUNK, (c + 1) * CHUNK)
            f_s[grp * ROWS:(grp + 1) * ROWS, cols] = (y_s[grp, c].astype(F32) * inv * gf[:, cols]).astype(BF16)

    final_norm(0)
    for j in range(HALF):
        yf[j].wait_recv()
    final_norm(1)
    tok_copy.wait()

    tok = jnp.concatenate([tok_ref[...], tok2[...]], axis=1) - (tp * vocab_loc + vbase)
    row_id = lax.broadcasted_iota(jnp.int32, (8, 2 * ROWS), 0)

    def score(slot, at, size, first, state):
        top, tot, tgt = state
        logits = dot_t(wbuf[slot, pl.ds(at, size), :], f_s[...])
        blocks = [logits[8 * i:8 * i + 8] for i in range(size // 8)]
        peak = blocks[0]
        for v in blocks[1:]:
            peak = jnp.maximum(peak, v)
        new = jnp.maximum(top, peak)
        part_sum = None
        for i, v in enumerate(blocks):
            e = jnp.exp(v - new)
            part_sum = e if part_sum is None else part_sum + e
            tgt = jnp.where(row_id + (first + 8 * i) == tok, v, tgt)
        tot = tot * jnp.exp(top - new) + part_sum
        return new, tot, tgt

    def some_tiles(k, state):
        for t in range(STEP):
            head_copy(k * STEP + t).wait()
        for t in range(STEP):
            i = k * STEP + t
            for b in range(0, TILE, BLOCK):
                state = score(lax.rem(head0 + i, RING), b, BLOCK, i * TILE + b, state)
        for t in range(STEP):
            i = k * STEP + t

            @pl.when(i + RING < n_full)
            def _():
                head_copy(i + RING).start()
            if n_tail:
                @pl.when(i + RING == n_full)
                def _():
                    head_copy(n_full, n_tail).start()
        return state

    state = (jnp.full((8, 2 * ROWS), -1e30, F32), jnp.zeros((8, 2 * ROWS), F32), jnp.zeros((8, 2 * ROWS), F32))
    state = lax.fori_loop(0, n_full // STEP, some_tiles, state)
    head_copy(n_full, n_tail).wait()
    cut = -(-n_tail // 32) * 16
    for b, size in ((0, cut), (cut, n_tail - cut)):
        state = score((head0 + n_full) % RING, b, size, n_full * TILE + b, state)
    top, tot, tgt = state
    peak = jnp.max(top, axis=0, keepdims=True)
    tot = jnp.sum(tot * jnp.exp(top - peak), axis=0, keepdims=True)
    tgt = jnp.sum(tgt, axis=0, keepdims=True)
    pad = jnp.zeros((5, ROWS), F32)
    for g in range(2):
        cols = slice(g * ROWS, (g + 1) * ROWS)
        st_s[g] = jnp.concatenate([peak[:, cols], tot[:, cols], tgt[:, cols], pad], axis=0)

    sends = []
    for k in range(1, 8):
        who = lax.rem(dev + k, 8)
        whod, whot = who // 4, lax.rem(who, 4)
        grp = lax.rem(whod + dp, 2)
        sends.append(remote(st_s.at[grp], st_r.at[dev], s_st.at[k - 1], r_st.at[k - 1], (whod, whot)))
    for c in sends:
        c.start()
    st_r[dev] = st_s[0]
    for c in sends:
        c.wait()
    stats = [st_r[i] for i in range(8)]
    peak = stats[0][0:1]
    for s in stats[1:]:
        peak = jnp.maximum(peak, s[0:1])
    tot = jnp.zeros_like(peak)
    tgt = jnp.zeros_like(peak)
    for s in stats:
        tot = tot + s[1:2] * jnp.exp(s[0:1] - peak)
        tgt = tgt + s[2:3]
    lse = peak + jnp.log(tot)
    lse_ref[...] = lse
    logp_ref[...] = tgt - lse

    for group in (d1, x1, ac, d2, x2, yo, yy, yf):
        for c in group:
            c.wait_send()
    for c in y_out:
        c.wait()


def emit_kernel(y_in, logp_in, lse_in, y_out, logp_out, lse_out, sem):
    copies = [pltpu.make_async_copy(logp_in, logp_out, sem.at[0]), pltpu.make_async_copy(lse_in, lse_out, sem.at[1])]
    for i in range(8):
        rows = pl.ds(i * 16, 16)
        copies.append(pltpu.make_async_copy(y_in.at[rows], y_out.at[rows], sem.at[2 + i]))
    for c in copies:
        c.start()
    for c in copies:
        c.wait()


def local_step(tok_hidden, seq_lens, k_cache, v_cache, next_tok, g_attn, w_q, b_q, w_k, b_k, w_v, b_v, w_o, g_mlp, w_gate, w_up, w_down, g_final, w_head):
    steps = np.arange(HEAD // 2, dtype=np.float32) * np.float32(-2.0 / HEAD)
    freq = jnp.asarray(np.tile(np.power(np.float64(THETA), steps.astype(np.float64)).astype(np.float32), 2)[None])
    vm = pl.BlockSpec(memory_space=pltpu.VMEM)
    sm = pl.BlockSpec(memory_space=pltpu.SMEM)
    hb = pl.BlockSpec(memory_space=pltpu.HBM)
    dma = pltpu.SemaphoreType.DMA
    cache = jax.ShapeDtypeStruct((ROWS, SLOTS, HEAD), BF16)
    part, k_all, v_all = pl.pallas_call(
        attn_kernel,
        out_shape=(jax.ShapeDtypeStruct((NCH, ROWS, CHUNK), BF16), cache, cache),
        in_specs=[sm] + [hb] * 13,
        out_specs=(hb, hb, hb),
        scratch_shapes=[
            pltpu.VMEM((NCH, ROWS, CHUNK), BF16), pltpu.VMEM((1, ROWS), jnp.int32), pltpu.VMEM((1, HEAD), F32), pltpu.VMEM((ROWS, WIDTH), BF16), pltpu.VMEM((WIDTH,), BF16),
            pltpu.VMEM((4 * HEAD,), BF16), pltpu.VMEM((HEAD,), BF16), pltpu.VMEM((HEAD,), BF16),
            pltpu.VMEM((ROWS, SLOTS, HEAD), BF16), pltpu.VMEM((ROWS, SLOTS, HEAD), BF16),
            pltpu.VMEM((WIDTH, 512), BF16), pltpu.VMEM((WIDTH, HEAD), BF16), pltpu.VMEM((WIDTH, HEAD), BF16), pltpu.VMEM((512, WIDTH), BF16),
            pltpu.VMEM((4, ROWS, HEAD), F32), pltpu.VMEM((ROWS, HEAD), F32), pltpu.VMEM((ROWS, HEAD), F32),
            pltpu.VMEM((128, HEAD), F32), pltpu.VMEM((HEAD, 128), BF16), pltpu.VMEM((SLOTS, 128), F32), pltpu.VMEM((128, SLOTS), BF16),
            pltpu.VMEM((128, HEAD), F32), pltpu.VMEM((ROWS, 512), BF16), pltpu.VMEM((8, 128), jnp.int32),
            dma((4,)), dma((4,)), dma((4,)), dma((4,)), dma((4,)), dma((8,)),
        ],
        compiler_params=pltpu.CompilerParams(vmem_limit_bytes=VMEM_BYTES),
        name="attention",
    )(seq_lens, seq_lens.reshape(1, ROWS), freq, tok_hidden, g_attn, b_q, b_k, b_v,
      w_q, w_k, w_v, w_o, k_cache.reshape(ROWS, SLOTS, HEAD), v_cache.reshape(ROWS, SLOTS, HEAD))

    ff = w_gate.shape[1]
    vocab_loc = w_head.shape[0]
    ff_pad = -(-ff // BLOCK) * BLOCK
    chunk4 = pltpu.VMEM((HALF, ROWS, CHUNK), BF16)
    chunk8 = pltpu.VMEM((NCH, ROWS, CHUNK), BF16)

    def kernel(*refs):
        tail_kernel(ff, vocab_loc, *refs)

    y_out, logp, lse = pl.pallas_call(
        kernel,
        out_shape=(jax.ShapeDtypeStruct((ROWS, WIDTH), BF16), jax.ShapeDtypeStruct((1, ROWS), F32), jax.ShapeDtypeStruct((1, ROWS), F32)),
        in_specs=[hb] * 9,
        out_specs=(hb, vm, vm),
        scratch_shapes=[
            chunk8, pltpu.VMEM((ROWS, WIDTH), BF16), pltpu.VMEM((WIDTH,), BF16), pltpu.VMEM((WIDTH,), BF16), pltpu.VMEM((1, ROWS), jnp.int32),
            pltpu.VMEM((RING, TILE, WIDTH), BF16),
            chunk4, chunk4, chunk4, chunk8, pltpu.VMEM((ROWS, WIDTH), BF16), pltpu.VMEM((ROWS, ff_pad), BF16),
            chunk8, chunk4, chunk4, chunk4, pltpu.VMEM((2, NCH, ROWS, CHUNK), BF16), pltpu.VMEM((2 * ROWS, WIDTH), BF16),
            pltpu.VMEM((1, ROWS), jnp.int32), pltpu.VMEM((2, 8, ROWS), F32), pltpu.VMEM((8, 8, ROWS), F32),
            dma((RING,)),
        ] + [dma((HALF,))] * 16 + [dma, dma, dma((7,)), dma((7,)), dma((5,)), dma((NCH,))],
        compiler_params=pltpu.CompilerParams(vmem_limit_bytes=VMEM_BYTES, collective_id=0, has_side_effects=True),
        name="tail",
    )(part, tok_hidden, g_mlp, g_final, next_tok.reshape(1, ROWS), w_gate.T, w_up.T, w_down, w_head)
    vec = jax.ShapeDtypeStruct((1, ROWS), F32)
    y_out, logp, lse = pl.pallas_call(
        emit_kernel,
        out_shape=(jax.ShapeDtypeStruct((ROWS, WIDTH), BF16), vec, vec),
        in_specs=[hb] * 3,
        out_specs=(hb, hb, hb),
        scratch_shapes=[dma((10,))],
        name="emit",
    )(y_out, logp, lse)
    shape = (ROWS, SLOTS, 1, HEAD)
    return y_out, k_all.reshape(shape), v_all.reshape(shape), logp.reshape(ROWS), lse.reshape(ROWS)


def solution(mesh):
    row_spec = P('dp', None)
    vec_spec = P('dp')
    cache_spec = P('dp', None, 'tp', None)
    col_spec = P(None, 'tp')
    part_spec = P('tp')
    whole_spec = P(None)
    in_specs = (row_spec, vec_spec, cache_spec, cache_spec, vec_spec, whole_spec, col_spec, part_spec, col_spec, part_spec, col_spec, part_spec, P('tp', None), whole_spec, col_spec, col_spec, P('tp', None), whole_spec, P('tp', None))
    out_specs = (row_spec, cache_spec, cache_spec, vec_spec, vec_spec)
    return jax.shard_map(local_step, mesh=mesh, in_specs=in_specs, out_specs=out_specs, check_vma=False)
```

```python
import jax
import numpy as np
import jax.numpy as jnp
from jax import lax
from jax.experimental import pallas as pl
from jax.experimental.pallas import tpu as pltpu
from jax.sharding import PartitionSpec as P

THETA = 1000000.0
EPS = 1e-6
MESH = pl.DeviceIdType.MESH
F32 = jnp.float32
BF16 = jnp.bfloat16
VMEM_BYTES = 67043328

ROWS = 128
WIDTH = 2048
HEAD = 128
SLOTS = 512
GROUP = 32
CHUNK = 256
NCH = 8
HALF = 4
BLOCK = 256
SUM1 = ((0, 2), (2, 2))
SUM2 = ((0, 2), (2, 1), (3, 1))
TILE = 768
RING = 18
STEP = 4


def dot(a, b):
    return lax.dot_general(a, b, (((1,), (0,)), ((), ())), preferred_element_type=F32)


def dot_t(a, b):
    return lax.dot_general(a, b, (((1,), (1,)), ((), ())), preferred_element_type=F32)


def attn_kernel(lens_ref, lenv_hbm, freq_hbm, x_hbm, g_hbm, bq_hbm, bk_hbm, bv_hbm,
                wq_hbm, wk_hbm, wv_hbm, wo_hbm, k_hbm, v_hbm,
                part_hbm, ko_hbm, vo_hbm,
                part_ref, lenv_ref, freq_ref, x_ref, g_ref, bq_ref, bk_ref, bv_ref,
                kbuf, vbuf, wq, wk, wv, wo, q_s, k_s, v_s, qg_s, qt_s, sc_s, pt_s, o_s, at_s, ll_s,
                wsem, ksem, vsem, kosem, vosem, insem):
    groups = ROWS // GROUP
    part = GROUP // 4
    small = [pltpu.make_async_copy(src, dst, insem.at[i]) for i, (src, dst) in enumerate((
        (x_hbm, x_ref), (lenv_hbm, lenv_ref), (freq_hbm, freq_ref), (g_hbm, g_ref), (bq_hbm, bq_ref), (bk_hbm, bk_ref), (bv_hbm, bv_ref)))]
    for c in small:
        c.start()
    for i, (src, dst) in enumerate(((wq_hbm, wq), (wk_hbm, wk), (wv_hbm, wv))):
        pltpu.make_async_copy(src, dst, wsem.at[i]).start()

    def start_in(g, hbm, buf, sem):
        for i in range(4):
            rows = pl.ds(g * GROUP + i * part, part)
            pltpu.make_async_copy(hbm.at[rows], buf.at[rows], sem.at[g]).start()

    start_in(0, k_hbm, kbuf, ksem)
    for c in small:
        c.wait()
    start_in(0, v_hbm, vbuf, vsem)
    len_rows = jnp.broadcast_to(lenv_ref[...].astype(F32), (ROWS, ROWS)).T
    angles = len_rows * freq_ref[...]
    cos = jnp.cos(angles)
    sin = jnp.sin(angles) * jnp.where(lax.broadcasted_iota(jnp.int32, (ROWS, HEAD), 1) < HEAD // 2, -1.0, 1.0)
    seq_of = lax.broadcasted_iota(jnp.int32, (GROUP, 128), 1) // 4
    pick = lax.broadcasted_iota(jnp.int32, (GROUP, 128), 0) == seq_of
    for g in range(groups):
        ll_s[g:g + 1, :] = jnp.sum(jnp.where(pick, len_rows[g * GROUP:(g + 1) * GROUP], 0.0), axis=0, keepdims=True).astype(jnp.int32)

    x = x_ref[...].astype(F32)
    inv = lax.rsqrt(jnp.mean(x * x, axis=-1, keepdims=True) + EPS)
    normed = (x * inv * g_ref[...].astype(F32).reshape(1, WIDTH)).astype(BF16)
    for i, (src, dst) in enumerate(((wq_hbm, wq), (wk_hbm, wk), (wv_hbm, wv))):
        pltpu.make_async_copy(src, dst, wsem.at[i]).wait()

    start_in(1, k_hbm, kbuf, ksem)

    def rope(u):
        return u * cos + pltpu.roll(u, HEAD // 2, 1) * sin

    k_s[...] = rope(dot(normed, wk[...]) + bk_ref[...].astype(F32).reshape(1, HEAD))
    v_s[...] = dot(normed, wv[...]) + bv_ref[...].astype(F32).reshape(1, HEAD)
    q_all = dot(normed, wq[...]) + bq_ref[...].astype(F32).reshape(1, 4 * HEAD)
    for h in range(4):
        q_s[h] = rope(q_all[:, h * HEAD:(h + 1) * HEAD])

    lane_seq = lax.broadcasted_iota(jnp.int32, (HEAD, 128), 1) // 4
    slot_id = lax.broadcasted_iota(jnp.int32, (SLOTS, 128), 0)
    row16 = lax.broadcasted_iota(jnp.int32, (16, HEAD), 0)
    row_seq = lax.broadcasted_iota(jnp.int32, (16, HEAD), 0) // 4

    def start_out(g):
        rows = pl.ds(g * GROUP, GROUP)
        pltpu.make_async_copy(kbuf.at[rows], ko_hbm.at[rows], kosem.at[g]).start()
        pltpu.make_async_copy(vbuf.at[rows], vo_hbm.at[rows], vosem.at[g]).start()

    def one_group(g, _):
        rows = pl.ds(pl.multiple_of(g * GROUP, GROUP), GROUP)
        pltpu.make_async_copy(k_hbm.at[rows], kbuf.at[rows], ksem.at[g]).wait()

        @pl.when(g + 1 < groups)
        def _():
            start_in(g + 1, v_hbm, vbuf, vsem)

        @pl.when(g + 1 == groups)
        def _():
            pltpu.make_async_copy(wo_hbm, wo, wsem.at[3]).start()

        def put(new_s, buf):
            def one(i, _):
                b = g * GROUP + i
                length = lens_ref[b]
                base = pl.multiple_of((length // 16) * 16, 16)
                old = buf[b, pl.ds(base, 16), :]
                new = jnp.broadcast_to(new_s[pl.ds(b, 1), :].astype(BF16), (16, HEAD))
                buf[b, pl.ds(base, 16), :] = jnp.where(row16 == length - base, new, old)
                return 0
            lax.fori_loop(0, GROUP, one, 0, unroll=8)

        put(k_s, kbuf)

        @pl.when(g + 1 == groups)
        def _():
            for i in range(groups - 1):
                start_out(i)
            pltpu.make_async_copy(kbuf.at[rows], ko_hbm.at[rows], kosem.at[g]).start()

        for h in range(4):
            qg_s[pl.ds(h, GROUP, stride=4), :] = q_s[h, rows, :]
        qt_s[...] = qg_s[...].T.astype(BF16)
        qt = qt_s[...]
        zero = jnp.zeros_like(qt)
        top_half, low_half = None, None
        for p in range(GROUP // 2):
            b = g * GROUP + 2 * p
            rhs = jnp.concatenate([jnp.where(lane_seq == 2 * p, qt, zero), jnp.where(lane_seq == 2 * p + 1, qt, zero)], axis=0)
            t0 = dot(jnp.concatenate([kbuf[b, :SLOTS // 2], kbuf[b + 1, :SLOTS // 2]], axis=1), rhs)
            t1 = dot(jnp.concatenate([kbuf[b, SLOTS // 2:], kbuf[b + 1, SLOTS // 2:]], axis=1), rhs)
            top_half = t0 if top_half is None else top_half + t0
            low_half = t1 if low_half is None else low_half + t1
        sc_s[:SLOTS // 2] = top_half
        sc_s[SLOTS // 2:] = low_half
        live = slot_id <= ll_s[pl.ds(g, 1), :]
        scores = jnp.where(live, sc_s[...] * (HEAD ** -0.5), -jnp.inf)
        top = jnp.max(scores, axis=0, keepdims=True)
        exps = jnp.exp(scores - top)
        sc_s[...] = exps
        recip = 1.0 / jnp.sum(exps, axis=0, keepdims=True)
        for i in range(4):
            blk = sc_s[i * 128:(i + 1) * 128, :] * recip
            pt_s[:, i * 128:(i + 1) * 128] = blk.T.astype(BF16)

        pltpu.make_async_copy(v_hbm.at[rows], vbuf.at[rows], vsem.at[g]).wait()

        @pl.when(g + 2 < groups)
        def _():
            start_in(g + 2, k_hbm, kbuf, ksem)

        put(v_s, vbuf)

        @pl.when(g + 1 == groups)
        def _():
            pltpu.make_async_copy(vbuf.at[rows], vo_hbm.at[rows], vosem.at[g]).start()

        for j in range(GROUP // 4):
            b = g * GROUP + 4 * j
            probs = pt_s[16 * j:16 * j + 16, :]
            o = jnp.zeros((16, HEAD), F32)
            for i in range(0, 4, 2):
                out = dot(probs, jnp.concatenate([vbuf[b + i], vbuf[b + i + 1]], axis=1))
                o = jnp.where(row_seq == i, out[:, :HEAD], o)
                o = jnp.where(row_seq == i + 1, out[:, HEAD:], o)
            o_s[16 * j:16 * j + 16, :] = o
        for h in range(4):
            at_s[rows, h * HEAD:(h + 1) * HEAD] = o_s[pl.ds(h, GROUP, stride=4), :].astype(BF16)
        return 0

    lax.fori_loop(0, groups, one_group, 0)

    pltpu.make_async_copy(wo_hbm, wo, wsem.at[3]).wait()
    attn = at_s[...]
    for c in range(WIDTH // BLOCK):
        part_ref[c] = dot(attn, wo[:, c * BLOCK:(c + 1) * BLOCK]).astype(BF16)
    part_copy = pltpu.make_async_copy(part_ref, part_hbm, insem.at[7])
    part_copy.start()
    part_copy.wait()
    for g in range(groups):
        rows = pl.ds(g * GROUP, GROUP)
        pltpu.make_async_copy(kbuf.at[rows], ko_hbm.at[rows], kosem.at[g]).wait()
        pltpu.make_async_copy(vbuf.at[rows], vo_hbm.at[rows], vosem.at[g]).wait()


def tail_kernel(ff, vocab_loc,
                part_hbm, x_hbm, gm_hbm, gf_hbm, tok_hbm, wg_hbm, wu_hbm, wd_hbm, wh_hbm,
                y_ref, logp_ref, lse_ref,
                part_ref, x_ref, gm_ref, gf_ref, tok_ref, wbuf, r1, s1, r2, a_s, m_s, hid, p2, r1b, s2, r2b, y_s, f_s, tok2, st_s, st_r,
                wsem, s_d1, r_d1, s_x1, r_x1, s_a, r_a, s_d2, r_d2, s_x2, r_x2,
                s_y, r_y, s_o, r_o, s_f, r_f, s_t, r_t, s_st, r_st, insem, ysem):
    dp = lax.axis_index('dp')
    tp = lax.axis_index('tp')
    core = lax.rem(tp, 2)
    dev = dp * 4 + tp
    partner = (dp, tp + 1 - 2 * core)
    xnext = (dp, lax.rem(tp + 2, 4))
    ynext = (1 - dp, tp)
    mine = core * HALF
    other = (1 - core) * HALF

    mlp_tiles = [(i * TILE, min(TILE, ff - i * TILE)) for i in range(-(-ff // TILE))]
    n_mlp = len(mlp_tiles)
    tail_pad = -(-mlp_tiles[-1][1] // BLOCK) * BLOCK
    vocab_half = vocab_loc // 2
    n_full = vocab_half // TILE
    n_tail = vocab_half - n_full * TILE
    n_head = n_full + (1 if n_tail else 0)
    assert n_full % STEP == 0 and n_tail
    head0 = 3 * n_mlp
    vbase = dp * vocab_half

    def mlp_copy(i):
        if i < 2 * n_mlp:
            src, (r, n) = (wg_hbm, wu_hbm)[i % 2], mlp_tiles[i // 2]
        else:
            src, (r, n) = wd_hbm, mlp_tiles[i - 2 * n_mlp]
        slot = i % RING
        return pltpu.make_async_copy(src.at[pl.ds(r, n)], wbuf.at[slot, pl.ds(0, n)], wsem.at[slot])

    def head_copy(i, n=TILE):
        slot = lax.rem(head0 + i, RING)
        start = pl.multiple_of(vbase + i * TILE, 16)
        return pltpu.make_async_copy(wh_hbm.at[pl.ds(start, n)], wbuf.at[slot, pl.ds(0, n)], wsem.at[slot])

    def start_item(i):
        if i < head0:
            mlp_copy(i).start()
        elif i - head0 < n_full:
            head_copy(i - head0).start()
        elif i - head0 < n_head:
            head_copy(i - head0, n_tail).start()

    small = [pltpu.make_async_copy(src, dst, insem.at[i]) for i, (src, dst) in enumerate((
        (part_hbm, part_ref), (x_hbm, x_ref), (gm_hbm, gm_ref), (gf_hbm, gf_ref), (tok_hbm, tok_ref)))]
    for c in small:
        c.start()
    issued = [0]

    def issue(n, freed=0):
        for _ in range(n):
            if issued[0] < RING + freed:
                start_item(issued[0])
                issued[0] += 1

    issue(2)

    barrier = pltpu.get_barrier_semaphore()
    for d in range(2):
        for t in range(4):
            @pl.when(d * 4 + t != dev)
            def _():
                pl.semaphore_signal(barrier, inc=1, device_id=(d, t), device_id_type=MESH)
    last_n = mlp_tiles[-1][1]
    if tail_pad > last_n:
        for i in (2 * n_mlp - 2, 2 * n_mlp - 1, 3 * n_mlp - 1):
            wbuf[i % RING, last_n:tail_pad, :] = jnp.zeros((tail_pad - last_n, WIDTH), BF16)
    for c in small:
        c.wait()
    pl.semaphore_wait(barrier, 7)
    issue(2)

    def remote(src, dst, ssem, rsem, who):
        return pltpu.make_async_remote_copy(src_ref=src, dst_ref=dst, send_sem=ssem, recv_sem=rsem, device_id=who, device_id_type=MESH)

    tok_copy = remote(tok_ref, tok2, s_t, r_t, ynext)
    def part_of(ref, base, grp):
        return ref.at[pl.ds(base + grp[0], grp[1])]

    d1 = [remote(part_of(part_ref, other, p), part_of(r1, 0, p), s_d1.at[i], r_d1.at[i], partner) for i, p in enumerate(SUM1)]
    x1 = [remote(part_of(s1, 0, p), part_of(r2, 0, p), s_x1.at[i], r_x1.at[i], xnext) for i, p in enumerate(SUM1)]
    ac = [remote(part_of(a_s, mine, p), part_of(a_s, mine, p), s_a.at[i], r_a.at[i], partner) for i, p in enumerate(SUM1)]
    d2 = [remote(part_of(p2, other, p), part_of(r1b, 0, p), s_d2.at[i], r_d2.at[i], partner) for i, p in enumerate(SUM2)]
    x2 = [remote(part_of(s2, 0, p), part_of(r2b, 0, p), s_x2.at[i], r_x2.at[i], xnext) for i, p in enumerate(SUM2)]
    yo = [remote(part_of(y_s.at[0], mine, p), part_of(y_s.at[0], mine, p), s_o.at[i], r_o.at[i], partner) for i, p in enumerate(SUM2)]
    yy = [remote(part_of(y_s.at[0], mine, p), part_of(y_s.at[1], mine, p), s_y.at[i], r_y.at[i], ynext) for i, p in enumerate(SUM2)]
    yf = [remote(part_of(y_s.at[1], mine, p), part_of(y_s.at[1], mine, p), s_f.at[i], r_f.at[i], partner) for i, p in enumerate(SUM2)]

    def cols_of(c):
        return pl.ds(pl.multiple_of(c * CHUNK, CHUNK), CHUNK)

    for c in d1:
        c.start()
    tok_copy.start()
    for i, (first, n) in enumerate(SUM1):
        d1[i].wait_recv()
        for j in range(first, first + n):
            s1[j] = (part_ref[mine + j].astype(F32) + r1[j].astype(F32)).astype(BF16)
        x1[i].start()
    issue(2)
    for i, (first, n) in enumerate(SUM1):
        x1[i].wait_recv()
        issue(3)
        for j in range(first, first + n):
            total = s1[j].astype(F32) + r2[j].astype(F32)
            a_s[mine + j] = (x_ref[:, cols_of(mine + j)].astype(F32) + total).astype(BF16)
        ac[i].start()
    for c in ac:
        c.wait_recv()
    issue(1)

    def inv_rms(src):
        total = jnp.zeros((ROWS, CHUNK), F32)
        for c in range(NCH):
            v = src[c].astype(F32)
            total = total + v * v
        return lax.rsqrt(jnp.sum(total, axis=-1, keepdims=True) * (1.0 / WIDTH) + EPS)

    inv = inv_rms(a_s)
    gm = gm_ref[...].astype(F32).reshape(1, WIDTH)
    for c in range(NCH):
        cols = slice(c * CHUNK, (c + 1) * CHUNK)
        m_s[:, cols] = (a_s[c].astype(F32) * inv * gm[:, cols]).astype(BF16)

    for i, (r, n) in enumerate(mlp_tiles):
        mlp_copy(2 * i).wait()
        mlp_copy(2 * i + 1).wait()
        gslot, uslot = (2 * i) % RING, (2 * i + 1) % RING
        pad = -(-n // BLOCK) * BLOCK
        for b in range(0, pad, BLOCK):
            gate = dot_t(m_s[...], wbuf[gslot, b:b + BLOCK, :])
            up = dot_t(m_s[...], wbuf[uslot, b:b + BLOCK, :])
            hid[:, r + b:r + b + BLOCK] = (gate * jax.nn.sigmoid(gate) * up).astype(BF16)
            issue(1, 2 * i)

    for i in range(n_mlp):
        mlp_copy(2 * n_mlp + i).wait()

    def down(c):
        acc = None
        for i, (r, n) in enumerate(mlp_tiles):
            pad = -(-n // BLOCK) * BLOCK
            term = dot(hid[:, r:r + pad], wbuf[(2 * n_mlp + i) % RING, :pad, cols_of(c)])
            acc = term if acc is None else acc + term
        return acc.astype(BF16)

    def chip_sum(i):
        d2[i].wait_recv()
        first, n = SUM2[i]
        for j in range(first, first + n):
            s2[j] = (p2[mine + j].astype(F32) + r1b[j].astype(F32)).astype(BF16)
        x2[i].start()

    for i, (first, n) in enumerate(SUM2):
        for j in range(first, first + n):
            theirs, ours = down(other + j), down(mine + j)
            p2[other + j] = theirs
            p2[mine + j] = ours
            issue(1, 2 * n_mlp)
        d2[i].start()
        if i:
            chip_sum(i - 1)
    chip_sum(len(SUM2) - 1)
    issue(1, 3 * n_mlp)

    def forward(i):
        yy[i].wait_recv()
        yf[i].start()

    for i, (first, n) in enumerate(SUM2):
        x2[i].wait_recv()
        issue(2, 3 * n_mlp)
        for j in range(first, first + n):
            total = s2[j].astype(F32) + r2b[j].astype(F32)
            y_s[0, mine + j] = (a_s[mine + j].astype(F32) + total).astype(BF16)
        yy[i].start()
        yo[i].start()
        if i:
            forward(i - 1)
    forward(len(SUM2) - 1)
    for c in yo:
        c.wait_recv()
    issue(RING, 3 * n_mlp)
    y_out = [pltpu.make_async_copy(y_s.at[0, c], y_ref.at[:, pl.ds(c * CHUNK, CHUNK)], ysem.at[c]) for c in range(NCH)]
    for c in y_out:
        c.start()

    gf = gf_ref[...].astype(F32).reshape(1, WIDTH)

    def final_norm(grp):
        inv = inv_rms(y_s.at[grp])
        for c in range(NCH):
            cols = slice(c * CHUNK, (c + 1) * CHUNK)
            f_s[grp * ROWS:(grp + 1) * ROWS, cols] = (y_s[grp, c].astype(F32) * inv * gf[:, cols]).astype(BF16)

    final_norm(0)
    for c in yf:
        c.wait_recv()
    final_norm(1)
    tok_copy.wait()

    tok = jnp.concatenate([tok_ref[...], tok2[...]], axis=1) - (tp * vocab_loc + vbase)
    row_id = lax.broadcasted_iota(jnp.int32, (8, 2 * ROWS), 0)

    def score(slot, at, size, first, state):
        top, tot, tgt = state
        logits = dot_t(wbuf[slot, pl.ds(at, size), :], f_s[...])
        blocks = [logits[8 * i:8 * i + 8] for i in range(size // 8)]
        peak = blocks[0]
        for v in blocks[1:]:
            peak = jnp.maximum(peak, v)
        new = jnp.maximum(top, peak)
        part_sum = None
        for i, v in enumerate(blocks):
            e = jnp.exp(v - new)
            part_sum = e if part_sum is None else part_sum + e
            tgt = jnp.where(row_id + (first + 8 * i) == tok, v, tgt)
        tot = tot * jnp.exp(top - new) + part_sum
        return new, tot, tgt

    def some_tiles(k, state):
        for t in range(STEP):
            head_copy(k * STEP + t).wait()
        for t in range(STEP):
            i = k * STEP + t
            for b in range(0, TILE, BLOCK):
                state = score(lax.rem(head0 + i, RING), b, BLOCK, i * TILE + b, state)
        for t in range(STEP):
            i = k * STEP + t

            @pl.when(i + RING < n_full)
            def _():
                head_copy(i + RING).start()
            if n_tail:
                @pl.when(i + RING == n_full)
                def _():
                    head_copy(n_full, n_tail).start()
        return state

    state = (jnp.full((8, 2 * ROWS), -1e30, F32), jnp.zeros((8, 2 * ROWS), F32), jnp.zeros((8, 2 * ROWS), F32))
    state = lax.fori_loop(0, n_full // STEP, some_tiles, state)
    head_copy(n_full, n_tail).wait()
    cut = -(-n_tail // 32) * 16
    for b, size in ((0, cut), (cut, n_tail - cut)):
        state = score((head0 + n_full) % RING, b, size, n_full * TILE + b, state)
    top, tot, tgt = state
    peak = jnp.max(top, axis=0, keepdims=True)
    tot = jnp.sum(tot * jnp.exp(top - peak), axis=0, keepdims=True)
    tgt = jnp.sum(tgt, axis=0, keepdims=True)
    pad = jnp.zeros((5, ROWS), F32)
    for g in range(2):
        cols = slice(g * ROWS, (g + 1) * ROWS)
        st_s[g] = jnp.concatenate([peak[:, cols], tot[:, cols], tgt[:, cols], pad], axis=0)

    sends = []
    for k in range(1, 8):
        who = lax.rem(dev + k, 8)
        whod, whot = who // 4, lax.rem(who, 4)
        grp = lax.rem(whod + dp, 2)
        sends.append(remote(st_s.at[grp], st_r.at[dev], s_st.at[k - 1], r_st.at[k - 1], (whod, whot)))
    for c in sends:
        c.start()
    st_r[dev] = st_s[0]
    for c in sends:
        c.wait()
    stats = [st_r[i] for i in range(8)]
    peak = stats[0][0:1]
    for s in stats[1:]:
        peak = jnp.maximum(peak, s[0:1])
    tot = jnp.zeros_like(peak)
    tgt = jnp.zeros_like(peak)
    for s in stats:
        tot = tot + s[1:2] * jnp.exp(s[0:1] - peak)
        tgt = tgt + s[2:3]
    lse = peak + jnp.log(tot)
    lse_ref[...] = lse
    logp_ref[...] = tgt - lse

    for group in (d1, x1, ac, d2, x2, yo, yy, yf):
        for c in group:
            c.wait_send()
    for c in y_out:
        c.wait()


def emit_kernel(y_in, logp_in, lse_in, y_out, logp_out, lse_out):
    y_out[...] = y_in[...]
    logp_out[...] = logp_in[...]
    lse_out[...] = lse_in[...]


def local_step(tok_hidden, seq_lens, k_cache, v_cache, next_tok, g_attn, w_q, b_q, w_k, b_k, w_v, b_v, w_o, g_mlp, w_gate, w_up, w_down, g_final, w_head):
    steps = np.arange(HEAD // 2, dtype=np.float32) * np.float32(-2.0 / HEAD)
    freq = jnp.asarray(np.tile(np.power(np.float64(THETA), steps.astype(np.float64)).astype(np.float32), 2)[None])
    vm = pl.BlockSpec(memory_space=pltpu.VMEM)
    sm = pl.BlockSpec(memory_space=pltpu.SMEM)
    hb = pl.BlockSpec(memory_space=pltpu.HBM)
    dma = pltpu.SemaphoreType.DMA
    cache = jax.ShapeDtypeStruct((ROWS, SLOTS, HEAD), BF16)
    part, k_all, v_all = pl.pallas_call(
        attn_kernel,
        out_shape=(jax.ShapeDtypeStruct((NCH, ROWS, CHUNK), BF16), cache, cache),
        in_specs=[sm] + [hb] * 13,
        out_specs=(hb, hb, hb),
        scratch_shapes=[
            pltpu.VMEM((NCH, ROWS, CHUNK), BF16), pltpu.VMEM((1, ROWS), jnp.int32), pltpu.VMEM((1, HEAD), F32), pltpu.VMEM((ROWS, WIDTH), BF16), pltpu.VMEM((WIDTH,), BF16),
            pltpu.VMEM((4 * HEAD,), BF16), pltpu.VMEM((HEAD,), BF16), pltpu.VMEM((HEAD,), BF16),
            pltpu.VMEM((ROWS, SLOTS, HEAD), BF16), pltpu.VMEM((ROWS, SLOTS, HEAD), BF16),
            pltpu.VMEM((WIDTH, 512), BF16), pltpu.VMEM((WIDTH, HEAD), BF16), pltpu.VMEM((WIDTH, HEAD), BF16), pltpu.VMEM((512, WIDTH), BF16),
            pltpu.VMEM((4, ROWS, HEAD), F32), pltpu.VMEM((ROWS, HEAD), F32), pltpu.VMEM((ROWS, HEAD), F32),
            pltpu.VMEM((128, HEAD), F32), pltpu.VMEM((HEAD, 128), BF16), pltpu.VMEM((SLOTS, 128), F32), pltpu.VMEM((128, SLOTS), BF16),
            pltpu.VMEM((128, HEAD), F32), pltpu.VMEM((ROWS, 512), BF16), pltpu.VMEM((8, 128), jnp.int32),
            dma((4,)), dma((4,)), dma((4,)), dma((4,)), dma((4,)), dma((8,)),
        ],
        compiler_params=pltpu.CompilerParams(vmem_limit_bytes=VMEM_BYTES),
        name="attention",
    )(seq_lens, seq_lens.reshape(1, ROWS), freq, tok_hidden, g_attn, b_q, b_k, b_v,
      w_q, w_k, w_v, w_o, k_cache.reshape(ROWS, SLOTS, HEAD), v_cache.reshape(ROWS, SLOTS, HEAD))

    ff = w_gate.shape[1]
    vocab_loc = w_head.shape[0]
    ff_pad = -(-ff // BLOCK) * BLOCK
    chunk4 = pltpu.VMEM((HALF, ROWS, CHUNK), BF16)
    chunk8 = pltpu.VMEM((NCH, ROWS, CHUNK), BF16)

    def kernel(*refs):
        tail_kernel(ff, vocab_loc, *refs)

    y_out, logp, lse = pl.pallas_call(
        kernel,
        out_shape=(jax.ShapeDtypeStruct((ROWS, WIDTH), BF16), jax.ShapeDtypeStruct((1, ROWS), F32), jax.ShapeDtypeStruct((1, ROWS), F32)),
        in_specs=[hb] * 9,
        out_specs=(hb, vm, vm),
        scratch_shapes=[
            chunk8, pltpu.VMEM((ROWS, WIDTH), BF16), pltpu.VMEM((WIDTH,), BF16), pltpu.VMEM((WIDTH,), BF16), pltpu.VMEM((1, ROWS), jnp.int32),
            pltpu.VMEM((RING, TILE, WIDTH), BF16),
            chunk4, chunk4, chunk4, chunk8, pltpu.VMEM((ROWS, WIDTH), BF16), pltpu.VMEM((ROWS, ff_pad), BF16),
            chunk8, chunk4, chunk4, chunk4, pltpu.VMEM((2, NCH, ROWS, CHUNK), BF16), pltpu.VMEM((2 * ROWS, WIDTH), BF16),
            pltpu.VMEM((1, ROWS), jnp.int32), pltpu.VMEM((2, 8, ROWS), F32), pltpu.VMEM((8, 8, ROWS), F32),
            dma((RING,)),
        ] + [dma((HALF,))] * 16 + [dma, dma, dma((7,)), dma((7,)), dma((5,)), dma((NCH,))],
        compiler_params=pltpu.CompilerParams(vmem_limit_bytes=VMEM_BYTES, collective_id=0, has_side_effects=True),
        name="tail",
    )(part, tok_hidden, g_mlp, g_final, next_tok.reshape(1, ROWS), w_gate.T, w_up.T, w_down, w_head)
    vec = jax.ShapeDtypeStruct((1, ROWS), F32)
    y_out, logp, lse = pl.pallas_call(
        emit_kernel,
        out_shape=(jax.ShapeDtypeStruct((ROWS, WIDTH), BF16), vec, vec),
        in_specs=[vm] * 3,
        out_specs=(vm, vm, vm),
        name="emit",
    )(y_out, logp, lse)
    shape = (ROWS, SLOTS, 1, HEAD)
    return y_out, k_all.reshape(shape), v_all.reshape(shape), logp.reshape(ROWS), lse.reshape(ROWS)


def solution(mesh):
    row_spec = P('dp', None)
    vec_spec = P('dp')
    cache_spec = P('dp', None, 'tp', None)
    col_spec = P(None, 'tp')
    part_spec = P('tp')
    whole_spec = P(None)
    in_specs = (row_spec, vec_spec, cache_spec, cache_spec, vec_spec, whole_spec, col_spec, part_spec, col_spec, part_spec, col_spec, part_spec, P('tp', None), whole_spec, col_spec, col_spec, P('tp', None), whole_spec, P('tp', None))
    out_specs = (row_spec, cache_spec, cache_spec, vec_spec, vec_spec)
    return jax.shard_map(local_step, mesh=mesh, in_specs=in_specs, out_specs=out_specs, check_vma=False)
```

```python
import jax
import numpy as np
import jax.numpy as jnp
from jax import lax
from jax.experimental import pallas as pl
from jax.experimental.pallas import tpu as pltpu
from jax.sharding import PartitionSpec as P

THETA = 1000000.0
EPS = 1e-6
MESH = pl.DeviceIdType.MESH
F32 = jnp.float32
BF16 = jnp.bfloat16
VMEM_BYTES = 67043328

ROWS = 128
WIDTH = 2048
HEAD = 128
SLOTS = 512
GROUP = 32
CHUNK = 256
NCH = 8
HALF = 4
BLOCK = 256
SUM1 = ((0, 1), (1, 1), (2, 1), (3, 1))
SUM2 = ((0, 1), (1, 1), (2, 1), (3, 1))
TILE = 768
RING = 18
STEP = 4


def dot(a, b):
    return lax.dot_general(a, b, (((1,), (0,)), ((), ())), preferred_element_type=F32)


def dot_t(a, b):
    return lax.dot_general(a, b, (((1,), (1,)), ((), ())), preferred_element_type=F32)


def attn_kernel(lens_ref, lenv_hbm, freq_hbm, x_hbm, g_hbm, bq_hbm, bk_hbm, bv_hbm,
                wq_hbm, wk_hbm, wv_hbm, wo_hbm, k_hbm, v_hbm,
                part_hbm, ko_hbm, vo_hbm,
                part_ref, lenv_ref, freq_ref, x_ref, g_ref, bq_ref, bk_ref, bv_ref,
                kbuf, vbuf, wq, wk, wv, wo, q_s, k_s, v_s, qg_s, qt_s, sc_s, pt_s, o_s, at_s, ll_s,
                wsem, ksem, vsem, kosem, vosem, insem):
    groups = ROWS // GROUP
    part = GROUP // 4
    small = [pltpu.make_async_copy(src, dst, insem.at[i]) for i, (src, dst) in enumerate((
        (x_hbm, x_ref), (lenv_hbm, lenv_ref), (freq_hbm, freq_ref), (g_hbm, g_ref), (bq_hbm, bq_ref), (bk_hbm, bk_ref), (bv_hbm, bv_ref)))]
    for c in small:
        c.start()
    for i, (src, dst) in enumerate(((wq_hbm, wq), (wk_hbm, wk), (wv_hbm, wv))):
        pltpu.make_async_copy(src, dst, wsem.at[i]).start()

    def start_in(g, hbm, buf, sem):
        for i in range(4):
            rows = pl.ds(g * GROUP + i * part, part)
            pltpu.make_async_copy(hbm.at[rows], buf.at[rows], sem.at[g]).start()

    for c in small:
        c.wait()
    start_in(0, k_hbm, kbuf, ksem)
    start_in(0, v_hbm, vbuf, vsem)
    len_rows = jnp.broadcast_to(lenv_ref[...].astype(F32), (ROWS, ROWS)).T
    angles = len_rows * freq_ref[...]
    cos = jnp.cos(angles)
    sin = jnp.sin(angles) * jnp.where(lax.broadcasted_iota(jnp.int32, (ROWS, HEAD), 1) < HEAD // 2, -1.0, 1.0)
    seq_of = lax.broadcasted_iota(jnp.int32, (GROUP, 128), 1) // 4
    pick = lax.broadcasted_iota(jnp.int32, (GROUP, 128), 0) == seq_of
    for g in range(groups):
        ll_s[g:g + 1, :] = jnp.sum(jnp.where(pick, len_rows[g * GROUP:(g + 1) * GROUP], 0.0), axis=0, keepdims=True).astype(jnp.int32)

    x = x_ref[...].astype(F32)
    inv = lax.rsqrt(jnp.mean(x * x, axis=-1, keepdims=True) + EPS)
    normed = (x * inv * g_ref[...].astype(F32).reshape(1, WIDTH)).astype(BF16)
    for i, (src, dst) in enumerate(((wq_hbm, wq), (wk_hbm, wk), (wv_hbm, wv))):
        pltpu.make_async_copy(src, dst, wsem.at[i]).wait()

    start_in(1, k_hbm, kbuf, ksem)

    def rope(u):
        return u * cos + pltpu.roll(u, HEAD // 2, 1) * sin

    k_s[...] = rope(dot(normed, wk[...]) + bk_ref[...].astype(F32).reshape(1, HEAD))
    v_s[...] = dot(normed, wv[...]) + bv_ref[...].astype(F32).reshape(1, HEAD)
    q_all = dot(normed, wq[...]) + bq_ref[...].astype(F32).reshape(1, 4 * HEAD)
    for h in range(4):
        q_s[h] = rope(q_all[:, h * HEAD:(h + 1) * HEAD])

    lane_seq = lax.broadcasted_iota(jnp.int32, (HEAD, 128), 1) // 4
    slot_id = lax.broadcasted_iota(jnp.int32, (SLOTS, 128), 0)
    row16 = lax.broadcasted_iota(jnp.int32, (16, HEAD), 0)
    row_seq = lax.broadcasted_iota(jnp.int32, (16, HEAD), 0) // 4

    def start_out(g):
        rows = pl.ds(g * GROUP, GROUP)
        pltpu.make_async_copy(kbuf.at[rows], ko_hbm.at[rows], kosem.at[g]).start()
        pltpu.make_async_copy(vbuf.at[rows], vo_hbm.at[rows], vosem.at[g]).start()

    def one_group(g, _):
        rows = pl.ds(pl.multiple_of(g * GROUP, GROUP), GROUP)
        pltpu.make_async_copy(k_hbm.at[rows], kbuf.at[rows], ksem.at[g]).wait()

        @pl.when(g + 1 < groups)
        def _():
            start_in(g + 1, v_hbm, vbuf, vsem)

        @pl.when(g + 1 == groups)
        def _():
            pltpu.make_async_copy(wo_hbm, wo, wsem.at[3]).start()

        def put(new_s, buf):
            def one(i, _):
                b = g * GROUP + i
                length = lens_ref[b]
                base = pl.multiple_of((length // 16) * 16, 16)
                old = buf[b, pl.ds(base, 16), :]
                new = jnp.broadcast_to(new_s[pl.ds(b, 1), :].astype(BF16), (16, HEAD))
                buf[b, pl.ds(base, 16), :] = jnp.where(row16 == length - base, new, old)
                return 0
            lax.fori_loop(0, GROUP, one, 0, unroll=8)

        put(k_s, kbuf)

        @pl.when(g + 1 == groups)
        def _():
            start_out(groups - 2)
            pltpu.make_async_copy(kbuf.at[rows], ko_hbm.at[rows], kosem.at[g]).start()

        for h in range(4):
            qg_s[pl.ds(h, GROUP, stride=4), :] = q_s[h, rows, :]
        qt_s[...] = qg_s[...].T.astype(BF16)
        qt = qt_s[...]
        zero = jnp.zeros_like(qt)
        top_half, low_half = None, None
        for p in range(GROUP // 2):
            b = g * GROUP + 2 * p
            rhs = jnp.concatenate([jnp.where(lane_seq == 2 * p, qt, zero), jnp.where(lane_seq == 2 * p + 1, qt, zero)], axis=0)
            t0 = dot(jnp.concatenate([kbuf[b, :SLOTS // 2], kbuf[b + 1, :SLOTS // 2]], axis=1), rhs)
            t1 = dot(jnp.concatenate([kbuf[b, SLOTS // 2:], kbuf[b + 1, SLOTS // 2:]], axis=1), rhs)
            top_half = t0 if top_half is None else top_half + t0
            low_half = t1 if low_half is None else low_half + t1
        sc_s[:SLOTS // 2] = top_half
        sc_s[SLOTS // 2:] = low_half
        live = slot_id <= ll_s[pl.ds(g, 1), :]
        scores = jnp.where(live, sc_s[...] * (HEAD ** -0.5), -jnp.inf)
        top = jnp.max(scores, axis=0, keepdims=True)
        exps = jnp.exp(scores - top)
        sc_s[...] = exps
        recip = 1.0 / jnp.sum(exps, axis=0, keepdims=True)
        for i in range(4):
            blk = sc_s[i * 128:(i + 1) * 128, :] * recip
            pt_s[:, i * 128:(i + 1) * 128] = blk.T.astype(BF16)

        pltpu.make_async_copy(v_hbm.at[rows], vbuf.at[rows], vsem.at[g]).wait()

        @pl.when(g + 2 < groups)
        def _():
            start_in(g + 2, k_hbm, kbuf, ksem)

        @pl.when(g + 2 == groups)
        def _():
            for i in range(groups - 2):
                start_out(i)

        put(v_s, vbuf)

        @pl.when(g + 1 == groups)
        def _():
            pltpu.make_async_copy(vbuf.at[rows], vo_hbm.at[rows], vosem.at[g]).start()

        for j in range(GROUP // 4):
            b = g * GROUP + 4 * j
            probs = pt_s[16 * j:16 * j + 16, :]
            o = jnp.zeros((16, HEAD), F32)
            for i in range(0, 4, 2):
                out = dot(probs, jnp.concatenate([vbuf[b + i], vbuf[b + i + 1]], axis=1))
                o = jnp.where(row_seq == i, out[:, :HEAD], o)
                o = jnp.where(row_seq == i + 1, out[:, HEAD:], o)
            o_s[16 * j:16 * j + 16, :] = o
        for h in range(4):
            at_s[rows, h * HEAD:(h + 1) * HEAD] = o_s[pl.ds(h, GROUP, stride=4), :].astype(BF16)
        return 0

    lax.fori_loop(0, groups, one_group, 0)

    pltpu.make_async_copy(wo_hbm, wo, wsem.at[3]).wait()
    attn = at_s[...]
    for c in range(WIDTH // BLOCK):
        part_ref[c] = dot(attn, wo[:, c * BLOCK:(c + 1) * BLOCK]).astype(BF16)
    part_copy = pltpu.make_async_copy(part_ref, part_hbm, insem.at[7])
    part_copy.start()
    part_copy.wait()
    for g in range(groups):
        rows = pl.ds(g * GROUP, GROUP)
        pltpu.make_async_copy(kbuf.at[rows], ko_hbm.at[rows], kosem.at[g]).wait()
        pltpu.make_async_copy(vbuf.at[rows], vo_hbm.at[rows], vosem.at[g]).wait()


def tail_kernel(ff, vocab_loc,
                part_hbm, x_hbm, gm_hbm, gf_hbm, tok_hbm, wg_hbm, wu_hbm, wd_hbm, wh_hbm,
                y_ref, logp_ref, lse_ref,
                part_ref, x_ref, gm_ref, gf_ref, tok_ref, wbuf, r1, s1, r2, a_s, m_s, hid, p2, r1b, s2, r2b, y_s, f_s, tok2, st_s, st_r, late0, late1,
                wsem, s_d1, r_d1, s_x1, r_x1, s_a, r_a, s_d2, r_d2, s_x2, r_x2,
                s_y, r_y, s_o, r_o, s_f, r_f, s_t, r_t, s_st, r_st, insem, ysem):
    dp = lax.axis_index('dp')
    tp = lax.axis_index('tp')
    core = lax.rem(tp, 2)
    dev = dp * 4 + tp
    partner = (dp, tp + 1 - 2 * core)
    xnext = (dp, lax.rem(tp + 2, 4))
    ynext = (1 - dp, tp)
    mine = core * HALF
    other = (1 - core) * HALF

    mlp_tiles = [(i * TILE, min(TILE, ff - i * TILE)) for i in range(-(-ff // TILE))]
    n_mlp = len(mlp_tiles)
    tail_pad = -(-mlp_tiles[-1][1] // BLOCK) * BLOCK
    vocab_half = vocab_loc // 2
    n_full = vocab_half // TILE
    n_tail = vocab_half - n_full * TILE
    n_head = n_full + (1 if n_tail else 0)
    assert n_full % STEP == 0 and n_tail
    head0 = 3 * n_mlp
    vbase = dp * vocab_half

    def mlp_copy(i):
        if i < 2 * n_mlp:
            src, (r, n) = (wg_hbm, wu_hbm)[i % 2], mlp_tiles[i // 2]
        else:
            src, (r, n) = wd_hbm, mlp_tiles[i - 2 * n_mlp]
        slot = i % RING
        return pltpu.make_async_copy(src.at[pl.ds(r, n)], wbuf.at[slot, pl.ds(0, n)], wsem.at[slot])

    def head_copy(i, n=TILE):
        slot = lax.rem(head0 + i, RING)
        start = pl.multiple_of(vbase + i * TILE, 16)
        return pltpu.make_async_copy(wh_hbm.at[pl.ds(start, n)], wbuf.at[slot, pl.ds(0, n)], wsem.at[slot])

    def start_item(i):
        if i < head0:
            mlp_copy(i).start()
        elif i - head0 < n_full:
            head_copy(i - head0).start()
        elif i - head0 < n_head:
            head_copy(i - head0, n_tail).start()

    small = [pltpu.make_async_copy(src, dst, insem.at[i]) for i, (src, dst) in enumerate((
        (part_hbm, part_ref), (x_hbm, x_ref), (gm_hbm, gm_ref), (gf_hbm, gf_ref), (tok_hbm, tok_ref)))]
    for c in small:
        c.start()
    issued = [0]

    def issue(n, freed=0):
        for _ in range(n):
            if issued[0] < RING + freed:
                start_item(issued[0])
                issued[0] += 1

    issue(2)

    barrier = pltpu.get_barrier_semaphore()
    for d in range(2):
        for t in range(4):
            @pl.when(d * 4 + t != dev)
            def _():
                pl.semaphore_signal(barrier, inc=1, device_id=(d, t), device_id_type=MESH)
    last_n = mlp_tiles[-1][1]
    if tail_pad > last_n:
        for i in (2 * n_mlp - 2, 2 * n_mlp - 1, 3 * n_mlp - 1):
            wbuf[i % RING, last_n:tail_pad, :] = jnp.zeros((tail_pad - last_n, WIDTH), BF16)
    for c in small:
        c.wait()
    pl.semaphore_wait(barrier, 7)
    issue(2)

    def remote(src, dst, ssem, rsem, who):
        return pltpu.make_async_remote_copy(src_ref=src, dst_ref=dst, send_sem=ssem, recv_sem=rsem, device_id=who, device_id_type=MESH)

    tok_copy = remote(tok_ref, tok2, s_t, r_t, ynext)
    def part_of(ref, base, grp):
        return ref.at[pl.ds(base + grp[0], grp[1])]

    d1 = [remote(part_of(part_ref, other, p), part_of(r1, 0, p), s_d1.at[i], r_d1.at[i], partner) for i, p in enumerate(SUM1)]
    x1 = [remote(part_of(s1, 0, p), part_of(r2, 0, p), s_x1.at[i], r_x1.at[i], xnext) for i, p in enumerate(SUM1)]
    ac = [remote(part_of(a_s, mine, p), part_of(a_s, mine, p), s_a.at[i], r_a.at[i], partner) for i, p in enumerate(SUM1)]
    d2 = [remote(part_of(p2, other, p), part_of(r1b, 0, p), s_d2.at[i], r_d2.at[i], partner) for i, p in enumerate(SUM2)]
    x2 = [remote(part_of(s2, 0, p), part_of(r2b, 0, p), s_x2.at[i], r_x2.at[i], xnext) for i, p in enumerate(SUM2)]
    yo = [remote(part_of(y_s.at[0], mine, p), part_of(y_s.at[0], mine, p), s_o.at[i], r_o.at[i], partner) for i, p in enumerate(SUM2)]
    yy = [remote(part_of(y_s.at[0], mine, p), part_of(y_s.at[1], mine, p), s_y.at[i], r_y.at[i], ynext) for i, p in enumerate(SUM2)]
    yf = [remote(part_of(y_s.at[1], mine, p), part_of(y_s.at[1], mine, p), s_f.at[i], r_f.at[i], partner) for i, p in enumerate(SUM2)]

    def cols_of(c):
        return pl.ds(pl.multiple_of(c * CHUNK, CHUNK), CHUNK)

    for c in d1:
        c.start()
    tok_copy.start()
    for i, (first, n) in enumerate(SUM1):
        d1[i].wait_recv()
        for j in range(first, first + n):
            s1[j] = (part_ref[mine + j].astype(F32) + r1[j].astype(F32)).astype(BF16)
        x1[i].start()
    issue(2)
    for i, (first, n) in enumerate(SUM1):
        x1[i].wait_recv()
        issue(1 if i % 2 else 2)
        for j in range(first, first + n):
            total = s1[j].astype(F32) + r2[j].astype(F32)
            a_s[mine + j] = (x_ref[:, cols_of(mine + j)].astype(F32) + total).astype(BF16)
        ac[i].start()
    for c in ac:
        c.wait_recv()
    issue(1)

    def inv_rms(src):
        total = jnp.zeros((ROWS, CHUNK), F32)
        for c in range(NCH):
            v = src[c].astype(F32)
            total = total + v * v
        return lax.rsqrt(jnp.sum(total, axis=-1, keepdims=True) * (1.0 / WIDTH) + EPS)

    inv = inv_rms(a_s)
    gm = gm_ref[...].astype(F32).reshape(1, WIDTH)
    for c in range(NCH):
        cols = slice(c * CHUNK, (c + 1) * CHUNK)
        m_s[:, cols] = (a_s[c].astype(F32) * inv * gm[:, cols]).astype(BF16)

    for i in range(2 * n_mlp):
        mlp_copy(i).wait()
    for i, (r, n) in enumerate(mlp_tiles):
        gslot, uslot = (2 * i) % RING, (2 * i + 1) % RING
        pad = -(-n // BLOCK) * BLOCK
        for b in range(0, pad, BLOCK):
            gate = dot_t(wbuf[gslot, b:b + BLOCK, :], m_s[...])
            up = dot_t(wbuf[uslot, b:b + BLOCK, :], m_s[...])
            hid[:, r + b:r + b + BLOCK] = (gate * jax.nn.sigmoid(gate) * up).T.astype(BF16)
            issue(1, 2 * i)

    for i in range(n_mlp):
        mlp_copy(2 * n_mlp + i).wait()

    def down(c):
        acc = None
        for i, (r, n) in enumerate(mlp_tiles):
            pad = -(-n // BLOCK) * BLOCK
            term = dot(hid[:, r:r + pad], wbuf[(2 * n_mlp + i) % RING, :pad, cols_of(c)])
            acc = term if acc is None else acc + term
        return acc.astype(BF16)

    def chip_sum(i):
        d2[i].wait_recv()
        first, n = SUM2[i]
        for j in range(first, first + n):
            s2[j] = (p2[mine + j].astype(F32) + r1b[j].astype(F32)).astype(BF16)
        x2[i].start()

    for i, (first, n) in enumerate(SUM2):
        for j in range(first, first + n):
            theirs, ours = down(other + j), down(mine + j)
            p2[other + j] = theirs
            p2[mine + j] = ours
            issue(1, 2 * n_mlp)
        d2[i].start()
        if i:
            chip_sum(i - 1)
    chip_sum(len(SUM2) - 1)
    issue(1, 3 * n_mlp)

    def forward(i):
        yy[i].wait_recv()
        yf[i].start()

    for i, (first, n) in enumerate(SUM2):
        x2[i].wait_recv()
        issue(2, 3 * n_mlp)
        for j in range(first, first + n):
            total = s2[j].astype(F32) + r2b[j].astype(F32)
            y_s[0, mine + j] = (a_s[mine + j].astype(F32) + total).astype(BF16)
        yy[i].start()
        yo[i].start()
    for i in range(len(SUM2)):
        forward(i)
    for c in yo:
        c.wait_recv()
    issue(RING, 3 * n_mlp)
    y_out = [pltpu.make_async_copy(y_s.at[0, c], y_ref.at[:, pl.ds(c * CHUNK, CHUNK)], ysem.at[c]) for c in range(NCH)]
    for c in y_out:
        c.start()

    gf = gf_ref[...].astype(F32).reshape(1, WIDTH)

    def final_norm(grp):
        inv = inv_rms(y_s.at[grp])
        for c in range(NCH):
            cols = slice(c * CHUNK, (c + 1) * CHUNK)
            f_s[grp * ROWS:(grp + 1) * ROWS, cols] = (y_s[grp, c].astype(F32) * inv * gf[:, cols]).astype(BF16)

    final_norm(0)
    for c in yf:
        c.wait_recv()
    final_norm(1)
    tok_copy.wait()

    tok = jnp.concatenate([tok_ref[...], tok2[...]], axis=1) - (tp * vocab_loc + vbase)
    row_id = lax.broadcasted_iota(jnp.int32, (8, 2 * ROWS), 0)

    def tally(logits, first, state):
        top, tot, tgt = state
        blocks = [logits[8 * i:8 * i + 8] for i in range(logits.shape[0] // 8)]
        peak = blocks[0]
        for v in blocks[1:]:
            peak = jnp.maximum(peak, v)
        new = jnp.maximum(top, peak)
        part_sum = None
        for i, v in enumerate(blocks):
            e = jnp.exp(v - new)
            part_sum = e if part_sum is None else part_sum + e
            tgt = jnp.where(row_id + (first + 8 * i) == tok, v, tgt)
        tot = tot * jnp.exp(top - new) + part_sum
        return new, tot, tgt

    def late(k, state):
        end = (k + 1) * STEP * TILE
        for i, ref in enumerate((late0, late1)):
            state = tally(ref[...], jnp.where(k < 0, -(2 ** 30), end - (2 - i) * BLOCK), state)
        return state

    def some_tiles(k, state):
        for t in range(STEP):
            head_copy(k * STEP + t).wait()
        state = late(k - 1, state)
        todo = [(t, b) for t in range(STEP) for b in range(0, TILE, BLOCK)]
        for n, (t, b) in enumerate(todo):
            i = k * STEP + t
            logits = dot_t(wbuf[lax.rem(head0 + i, RING), pl.ds(b, BLOCK), :], f_s[...])
            if n < len(todo) - 2:
                state = tally(logits, i * TILE + b, state)
            elif n == len(todo) - 2:
                late0[...] = logits
            else:
                late1[...] = logits
        for t in range(STEP):
            i = k * STEP + t

            @pl.when(i + RING < n_full)
            def _():
                head_copy(i + RING).start()

            @pl.when(i + RING == n_full)
            def _():
                head_copy(n_full, n_tail).start()
        return state

    late0[...] = jnp.full(late0.shape, -1e30, F32)
    late1[...] = jnp.full(late1.shape, -1e30, F32)
    state = (jnp.full((8, 2 * ROWS), -1e30, F32), jnp.zeros((8, 2 * ROWS), F32), jnp.zeros((8, 2 * ROWS), F32))
    state = lax.fori_loop(0, n_full // STEP, some_tiles, state)
    head_copy(n_full, n_tail).wait()
    cut = -(-n_tail // 32) * 16
    state = late(n_full // STEP - 1, state)
    for b, size in ((0, cut), (cut, n_tail - cut)):
        logits = dot_t(wbuf[(head0 + n_full) % RING, pl.ds(b, size), :], f_s[...])
        state = tally(logits, n_full * TILE + b, state)
    top, tot, tgt = state
    peak = jnp.max(top, axis=0, keepdims=True)
    tot = jnp.sum(tot * jnp.exp(top - peak), axis=0, keepdims=True)
    tgt = jnp.sum(tgt, axis=0, keepdims=True)
    pad = jnp.zeros((5, ROWS), F32)
    for g in range(2):
        cols = slice(g * ROWS, (g + 1) * ROWS)
        st_s[g] = jnp.concatenate([peak[:, cols], tot[:, cols], tgt[:, cols], pad], axis=0)

    sends = []
    for k in range(1, 8):
        who = lax.rem(dev + k, 8)
        whod, whot = who // 4, lax.rem(who, 4)
        grp = lax.rem(whod + dp, 2)
        sends.append(remote(st_s.at[grp], st_r.at[dev], s_st.at[k - 1], r_st.at[k - 1], (whod, whot)))
    for c in sends:
        c.start()
    st_r[dev] = st_s[0]
    for c in sends:
        c.wait()
    stats = [st_r[i] for i in range(8)]
    peak = stats[0][0:1]
    for s in stats[1:]:
        peak = jnp.maximum(peak, s[0:1])
    tot = jnp.zeros_like(peak)
    tgt = jnp.zeros_like(peak)
    for s in stats:
        tot = tot + s[1:2] * jnp.exp(s[0:1] - peak)
        tgt = tgt + s[2:3]
    lse = peak + jnp.log(tot)
    lse_ref[...] = lse
    logp_ref[...] = tgt - lse

    for group in (d1, x1, ac, d2, x2, yo, yy, yf):
        for c in group:
            c.wait_send()
    for c in y_out:
        c.wait()


def emit_kernel(y_in, logp_in, lse_in, y_out, logp_out, lse_out):
    y_out[...] = y_in[...]
    logp_out[...] = logp_in[...]
    lse_out[...] = lse_in[...]


def local_step(tok_hidden, seq_lens, k_cache, v_cache, next_tok, g_attn, w_q, b_q, w_k, b_k, w_v, b_v, w_o, g_mlp, w_gate, w_up, w_down, g_final, w_head):
    steps = np.arange(HEAD // 2, dtype=np.float32) * np.float32(-2.0 / HEAD)
    freq = jnp.asarray(np.tile(np.power(np.float64(THETA), steps.astype(np.float64)).astype(np.float32), 2)[None])
    vm = pl.BlockSpec(memory_space=pltpu.VMEM)
    sm = pl.BlockSpec(memory_space=pltpu.SMEM)
    hb = pl.BlockSpec(memory_space=pltpu.HBM)
    dma = pltpu.SemaphoreType.DMA
    cache = jax.ShapeDtypeStruct((ROWS, SLOTS, HEAD), BF16)
    part, k_all, v_all = pl.pallas_call(
        attn_kernel,
        out_shape=(jax.ShapeDtypeStruct((NCH, ROWS, CHUNK), BF16), cache, cache),
        in_specs=[sm] + [hb] * 13,
        out_specs=(hb, hb, hb),
        scratch_shapes=[
            pltpu.VMEM((NCH, ROWS, CHUNK), BF16), pltpu.VMEM((1, ROWS), jnp.int32), pltpu.VMEM((1, HEAD), F32), pltpu.VMEM((ROWS, WIDTH), BF16), pltpu.VMEM((WIDTH,), BF16),
            pltpu.VMEM((4 * HEAD,), BF16), pltpu.VMEM((HEAD,), BF16), pltpu.VMEM((HEAD,), BF16),
            pltpu.VMEM((ROWS, SLOTS, HEAD), BF16), pltpu.VMEM((ROWS, SLOTS, HEAD), BF16),
            pltpu.VMEM((WIDTH, 512), BF16), pltpu.VMEM((WIDTH, HEAD), BF16), pltpu.VMEM((WIDTH, HEAD), BF16), pltpu.VMEM((512, WIDTH), BF16),
            pltpu.VMEM((4, ROWS, HEAD), F32), pltpu.VMEM((ROWS, HEAD), F32), pltpu.VMEM((ROWS, HEAD), F32),
            pltpu.VMEM((128, HEAD), F32), pltpu.VMEM((HEAD, 128), BF16), pltpu.VMEM((SLOTS, 128), F32), pltpu.VMEM((128, SLOTS), BF16),
            pltpu.VMEM((128, HEAD), F32), pltpu.VMEM((ROWS, 512), BF16), pltpu.VMEM((8, 128), jnp.int32),
            dma((4,)), dma((4,)), dma((4,)), dma((4,)), dma((4,)), dma((8,)),
        ],
        compiler_params=pltpu.CompilerParams(vmem_limit_bytes=VMEM_BYTES),
        name="attention",
    )(seq_lens, seq_lens.reshape(1, ROWS), freq, tok_hidden, g_attn, b_q, b_k, b_v,
      w_q, w_k, w_v, w_o, k_cache.reshape(ROWS, SLOTS, HEAD), v_cache.reshape(ROWS, SLOTS, HEAD))

    ff = w_gate.shape[1]
    vocab_loc = w_head.shape[0]
    ff_pad = -(-ff // BLOCK) * BLOCK
    chunk4 = pltpu.VMEM((HALF, ROWS, CHUNK), BF16)
    chunk8 = pltpu.VMEM((NCH, ROWS, CHUNK), BF16)

    def kernel(*refs):
        tail_kernel(ff, vocab_loc, *refs)

    y_out, logp, lse = pl.pallas_call(
        kernel,
        out_shape=(jax.ShapeDtypeStruct((ROWS, WIDTH), BF16), jax.ShapeDtypeStruct((1, ROWS), F32), jax.ShapeDtypeStruct((1, ROWS), F32)),
        in_specs=[hb] * 9,
        out_specs=(hb, vm, vm),
        scratch_shapes=[
            chunk8, pltpu.VMEM((ROWS, WIDTH), BF16), pltpu.VMEM((WIDTH,), BF16), pltpu.VMEM((WIDTH,), BF16), pltpu.VMEM((1, ROWS), jnp.int32),
            pltpu.VMEM((RING, TILE, WIDTH), BF16),
            chunk4, chunk4, chunk4, chunk8, pltpu.VMEM((ROWS, WIDTH), BF16), pltpu.VMEM((ROWS, ff_pad), BF16),
            chunk8, chunk4, chunk4, chunk4, pltpu.VMEM((2, NCH, ROWS, CHUNK), BF16), pltpu.VMEM((2 * ROWS, WIDTH), BF16),
            pltpu.VMEM((1, ROWS), jnp.int32), pltpu.VMEM((2, 8, ROWS), F32), pltpu.VMEM((8, 8, ROWS), F32),
            pltpu.VMEM((BLOCK, 2 * ROWS), F32), pltpu.VMEM((BLOCK, 2 * ROWS), F32),
            dma((RING,)),
        ] + [dma((HALF,))] * 16 + [dma, dma, dma((7,)), dma((7,)), dma((5,)), dma((NCH,))],
        compiler_params=pltpu.CompilerParams(vmem_limit_bytes=VMEM_BYTES, collective_id=0, has_side_effects=True),
        name="tail",
    )(part, tok_hidden, g_mlp, g_final, next_tok.reshape(1, ROWS), w_gate.T, w_up.T, w_down, w_head)
    vec = jax.ShapeDtypeStruct((1, ROWS), F32)
    y_out, logp, lse = pl.pallas_call(
        emit_kernel,
        out_shape=(jax.ShapeDtypeStruct((ROWS, WIDTH), BF16), vec, vec),
        in_specs=[vm] * 3,
        out_specs=(vm, vm, vm),
        name="emit",
    )(y_out, logp, lse)
    shape = (ROWS, SLOTS, 1, HEAD)
    return y_out, k_all.reshape(shape), v_all.reshape(shape), logp.reshape(ROWS), lse.reshape(ROWS)


def solution(mesh):
    row_spec = P('dp', None)
    vec_spec = P('dp')
    cache_spec = P('dp', None, 'tp', None)
    col_spec = P(None, 'tp')
    part_spec = P('tp')
    whole_spec = P(None)
    in_specs = (row_spec, vec_spec, cache_spec, cache_spec, vec_spec, whole_spec, col_spec, part_spec, col_spec, part_spec, col_spec, part_spec, P('tp', None), whole_spec, col_spec, col_spec, P('tp', None), whole_spec, P('tp', None))
    out_specs = (row_spec, cache_spec, cache_spec, vec_spec, vec_spec)
    return jax.shard_map(local_step, mesh=mesh, in_specs=in_specs, out_specs=out_specs, check_vma=False)
```

```python
import jax
import numpy as np
import jax.numpy as jnp
from jax import lax
from jax.experimental import pallas as pl
from jax.experimental.pallas import tpu as pltpu
from jax.sharding import PartitionSpec as P

THETA = 1000000.0
EPS = 1e-6
MESH = pl.DeviceIdType.MESH
F32 = jnp.float32
BF16 = jnp.bfloat16
ATTN_BYTES = 62 * 2 ** 20
TAIL_BYTES = 65500000

ROWS = 128
WIDTH = 2048
HEAD = 128
SLOTS = 512
GROUP = 32
CHUNK = 256
NCH = 8
HALF = 4
BLOCK = 256
SUM1 = ((0, 1), (1, 1), (2, 1), (3, 1))
SUM2 = ((0, 1), (1, 1), (2, 1), (3, 1))
TILE = 768
RING = 18
STEP = 4


def dot(a, b):
    return lax.dot_general(a, b, (((1,), (0,)), ((), ())), preferred_element_type=F32)


def dot_t(a, b):
    return lax.dot_general(a, b, (((1,), (1,)), ((), ())), preferred_element_type=F32)


def attn_kernel(lens_ref, lenv_hbm, freq_hbm, x_hbm, g_hbm, bq_hbm, bk_hbm, bv_hbm,
                wq_hbm, wk_hbm, wv_hbm, wo_hbm, k_hbm, v_hbm,
                part_ref, ko_hbm, vo_hbm,
                lenv_ref, freq_ref, x_ref, g_ref, bq_ref, bk_ref, bv_ref,
                kbuf, vbuf, wq, wk, wv, wo, q_s, k_s, v_s, qg_s, qt_s, sc_s, pt_s, o_s, at_s, ll_s,
                wsem, ksem, vsem, kosem, vosem, insem):
    groups = ROWS // GROUP
    part = GROUP // 4
    small = [pltpu.make_async_copy(src, dst, insem.at[i]) for i, (src, dst) in enumerate((
        (x_hbm, x_ref), (lenv_hbm, lenv_ref), (freq_hbm, freq_ref), (g_hbm, g_ref), (bq_hbm, bq_ref), (bk_hbm, bk_ref), (bv_hbm, bv_ref)))]
    for c in small:
        c.start()
    for i, (src, dst) in enumerate(((wq_hbm, wq), (wk_hbm, wk), (wv_hbm, wv))):
        pltpu.make_async_copy(src, dst, wsem.at[i]).start()

    def start_in(g, hbm, buf, sem):
        for i in range(4):
            rows = pl.ds(g * GROUP + i * part, part)
            pltpu.make_async_copy(hbm.at[rows], buf.at[rows], sem.at[g]).start()

    for c in small:
        c.wait()
    start_in(0, k_hbm, kbuf, ksem)
    start_in(0, v_hbm, vbuf, vsem)
    len_rows = jnp.broadcast_to(lenv_ref[...].astype(F32), (ROWS, ROWS)).T
    angles = len_rows * freq_ref[...]
    cos = jnp.cos(angles)
    sin = jnp.sin(angles) * jnp.where(lax.broadcasted_iota(jnp.int32, (ROWS, HEAD), 1) < HEAD // 2, -1.0, 1.0)
    seq_of = lax.broadcasted_iota(jnp.int32, (GROUP, 128), 1) // 4
    pick = lax.broadcasted_iota(jnp.int32, (GROUP, 128), 0) == seq_of
    for g in range(groups):
        ll_s[g:g + 1, :] = jnp.sum(jnp.where(pick, len_rows[g * GROUP:(g + 1) * GROUP], 0.0), axis=0, keepdims=True).astype(jnp.int32)

    x = x_ref[...].astype(F32)
    inv = lax.rsqrt(jnp.mean(x * x, axis=-1, keepdims=True) + EPS)
    normed = (x * inv * g_ref[...].astype(F32).reshape(1, WIDTH)).astype(BF16)
    for i, (src, dst) in enumerate(((wq_hbm, wq), (wk_hbm, wk), (wv_hbm, wv))):
        pltpu.make_async_copy(src, dst, wsem.at[i]).wait()

    start_in(1, k_hbm, kbuf, ksem)

    def rope(u):
        return u * cos + pltpu.roll(u, HEAD // 2, 1) * sin

    k_s[...] = rope(dot(normed, wk[...]) + bk_ref[...].astype(F32).reshape(1, HEAD))
    v_s[...] = dot(normed, wv[...]) + bv_ref[...].astype(F32).reshape(1, HEAD)
    q_all = dot(normed, wq[...]) + bq_ref[...].astype(F32).reshape(1, 4 * HEAD)
    for h in range(4):
        q_s[h] = rope(q_all[:, h * HEAD:(h + 1) * HEAD])

    lane_seq = lax.broadcasted_iota(jnp.int32, (HEAD, 128), 1) // 4
    slot_id = lax.broadcasted_iota(jnp.int32, (SLOTS, 128), 0)
    row16 = lax.broadcasted_iota(jnp.int32, (16, HEAD), 0)
    row_seq = lax.broadcasted_iota(jnp.int32, (16, HEAD), 0) // 4

    def start_out(g):
        write(g, kbuf, ko_hbm, kosem)
        write(g, vbuf, vo_hbm, vosem)

    def write(g, buf, hbm, sem):
        for i in range(4):
            rows = pl.ds(g * GROUP + i * part, part)
            pltpu.make_async_copy(buf.at[rows], hbm.at[rows], sem.at[g]).start()

    def one_group(g, _):
        rows = pl.ds(pl.multiple_of(g * GROUP, GROUP), GROUP)
        pltpu.make_async_copy(k_hbm.at[rows], kbuf.at[rows], ksem.at[g]).wait()

        @pl.when(g + 1 < groups)
        def _():
            start_in(g + 1, v_hbm, vbuf, vsem)

        @pl.when(g + 1 == groups)
        def _():
            pltpu.make_async_copy(wo_hbm, wo, wsem.at[3]).start()

        def put(new_s, buf):
            def one(i, _):
                b = g * GROUP + i
                length = lens_ref[b]
                base = pl.multiple_of((length // 16) * 16, 16)
                old = buf[b, pl.ds(base, 16), :]
                new = jnp.broadcast_to(new_s[pl.ds(b, 1), :].astype(BF16), (16, HEAD))
                buf[b, pl.ds(base, 16), :] = jnp.where(row16 == length - base, new, old)
                return 0
            lax.fori_loop(0, GROUP, one, 0, unroll=8)

        put(k_s, kbuf)

        @pl.when(g + 1 == groups)
        def _():
            start_out(groups - 2)
            write(g, kbuf, ko_hbm, kosem)

        for h in range(4):
            qg_s[pl.ds(h, GROUP, stride=4), :] = q_s[h, rows, :]
        qt_s[...] = qg_s[...].T.astype(BF16)
        qt = qt_s[...]
        zero = jnp.zeros_like(qt)
        top_half, low_half = None, None
        for p in range(GROUP // 2):
            b = g * GROUP + 2 * p
            rhs = jnp.concatenate([jnp.where(lane_seq == 2 * p, qt, zero), jnp.where(lane_seq == 2 * p + 1, qt, zero)], axis=0)
            t0 = dot(jnp.concatenate([kbuf[b, :SLOTS // 2], kbuf[b + 1, :SLOTS // 2]], axis=1), rhs)
            t1 = dot(jnp.concatenate([kbuf[b, SLOTS // 2:], kbuf[b + 1, SLOTS // 2:]], axis=1), rhs)
            top_half = t0 if top_half is None else top_half + t0
            low_half = t1 if low_half is None else low_half + t1
        sc_s[:SLOTS // 2] = top_half
        sc_s[SLOTS // 2:] = low_half
        live = slot_id <= ll_s[pl.ds(g, 1), :]
        scores = jnp.where(live, sc_s[...] * (HEAD ** -0.5), -jnp.inf)
        top = jnp.max(scores, axis=0, keepdims=True)
        exps = jnp.exp(scores - top)
        sc_s[...] = exps
        recip = 1.0 / jnp.sum(exps, axis=0, keepdims=True)
        for i in range(4):
            blk = sc_s[i * 128:(i + 1) * 128, :] * recip
            pt_s[:, i * 128:(i + 1) * 128] = blk.T.astype(BF16)

        pltpu.make_async_copy(v_hbm.at[rows], vbuf.at[rows], vsem.at[g]).wait()

        @pl.when(g + 2 < groups)
        def _():
            start_in(g + 2, k_hbm, kbuf, ksem)

        @pl.when(g + 2 == groups)
        def _():
            for i in range(groups - 2):
                start_out(i)

        put(v_s, vbuf)

        @pl.when(g + 1 == groups)
        def _():
            write(g, vbuf, vo_hbm, vosem)

        for j in range(GROUP // 4):
            b = g * GROUP + 4 * j
            probs = pt_s[16 * j:16 * j + 16, :]
            o = jnp.zeros((16, HEAD), F32)
            for i in range(0, 4, 2):
                out = dot(probs, jnp.concatenate([vbuf[b + i], vbuf[b + i + 1]], axis=1))
                o = jnp.where(row_seq == i, out[:, :HEAD], o)
                o = jnp.where(row_seq == i + 1, out[:, HEAD:], o)
            o_s[16 * j:16 * j + 16, :] = o
        for h in range(4):
            at_s[rows, h * HEAD:(h + 1) * HEAD] = o_s[pl.ds(h, GROUP, stride=4), :].astype(BF16)
        return 0

    lax.fori_loop(0, groups, one_group, 0)

    pltpu.make_async_copy(wo_hbm, wo, wsem.at[3]).wait()
    attn = at_s[...]
    for c in range(WIDTH // BLOCK):
        part_ref[c] = dot(attn, wo[:, c * BLOCK:(c + 1) * BLOCK]).astype(BF16)
    for g in range(groups):
        rows = pl.ds(g * GROUP, GROUP)
        pltpu.make_async_copy(kbuf.at[rows], ko_hbm.at[rows], kosem.at[g]).wait()
        pltpu.make_async_copy(vbuf.at[rows], vo_hbm.at[rows], vosem.at[g]).wait()


def tail_kernel(ff, vocab_loc,
                part_ref, x_hbm, gm_hbm, gf_hbm, tok_hbm, wg_hbm, wu_hbm, wd_hbm, wh_hbm,
                y_ref, logp_ref, lse_ref,
                x_ref, gm_ref, gf_ref, tok_ref, wbuf, r1, s1, r2, a_s, m_s, hid, p2, r1b, s2, r2b, y_s, f_s, tok2, st_s, st_r, late0, late1,
                wsem, s_d1, r_d1, s_x1, r_x1, s_a, r_a, s_d2, r_d2, s_x2, r_x2,
                s_y, r_y, s_o, r_o, s_f, r_f, s_t, r_t, s_st, r_st, insem):
    dp = lax.axis_index('dp')
    tp = lax.axis_index('tp')
    core = lax.rem(tp, 2)
    dev = dp * 4 + tp
    partner = (dp, tp + 1 - 2 * core)
    xnext = (dp, lax.rem(tp + 2, 4))
    ynext = (1 - dp, tp)
    mine = core * HALF
    other = (1 - core) * HALF

    mlp_tiles = [(i * TILE, min(TILE, ff - i * TILE)) for i in range(-(-ff // TILE))]
    n_mlp = len(mlp_tiles)
    tail_pad = -(-mlp_tiles[-1][1] // BLOCK) * BLOCK
    vocab_half = vocab_loc // 2
    n_full = vocab_half // TILE
    n_tail = vocab_half - n_full * TILE
    n_head = n_full + (1 if n_tail else 0)
    assert n_full % STEP == 0 and n_tail
    head0 = 3 * n_mlp
    vbase = dp * vocab_half

    def mlp_copy(i):
        if i < 2 * n_mlp:
            src, (r, n) = (wg_hbm, wu_hbm)[i % 2], mlp_tiles[i // 2]
        else:
            src, (r, n) = wd_hbm, mlp_tiles[i - 2 * n_mlp]
        slot = i % RING
        return pltpu.make_async_copy(src.at[pl.ds(r, n)], wbuf.at[slot, pl.ds(0, n)], wsem.at[slot])

    def head_copy(i, n=TILE):
        slot = lax.rem(head0 + i, RING)
        start = pl.multiple_of(vbase + i * TILE, 16)
        return pltpu.make_async_copy(wh_hbm.at[pl.ds(start, n)], wbuf.at[slot, pl.ds(0, n)], wsem.at[slot])

    def start_item(i):
        if i < head0:
            mlp_copy(i).start()
        elif i - head0 < n_full:
            head_copy(i - head0).start()
        elif i - head0 < n_head:
            head_copy(i - head0, n_tail).start()

    small = [pltpu.make_async_copy(src, dst, insem.at[i]) for i, (src, dst) in enumerate((
        (x_hbm, x_ref), (gm_hbm, gm_ref), (gf_hbm, gf_ref), (tok_hbm, tok_ref)))]
    for c in small:
        c.start()
    issued = [0]

    def issue(n, freed=0):
        for _ in range(n):
            if issued[0] < RING + freed:
                start_item(issued[0])
                issued[0] += 1

    issue(2)

    barrier = pltpu.get_barrier_semaphore()
    for d in range(2):
        for t in range(4):
            @pl.when(d * 4 + t != dev)
            def _():
                pl.semaphore_signal(barrier, inc=1, device_id=(d, t), device_id_type=MESH)
    last_n = mlp_tiles[-1][1]
    if tail_pad > last_n:
        for i in (2 * n_mlp - 2, 2 * n_mlp - 1, 3 * n_mlp - 1):
            wbuf[i % RING, last_n:tail_pad, :] = jnp.zeros((tail_pad - last_n, WIDTH), BF16)
    pl.semaphore_wait(barrier, 7)
    issue(2)

    def remote(src, dst, ssem, rsem, who):
        return pltpu.make_async_remote_copy(src_ref=src, dst_ref=dst, send_sem=ssem, recv_sem=rsem, device_id=who, device_id_type=MESH)

    tok_copy = remote(tok_ref, tok2, s_t, r_t, ynext)
    def part_of(ref, base, grp):
        return ref.at[pl.ds(base + grp[0], grp[1])]

    d1 = [remote(part_of(part_ref, other, p), part_of(r1, 0, p), s_d1.at[i], r_d1.at[i], partner) for i, p in enumerate(SUM1)]
    x1 = [remote(part_of(s1, 0, p), part_of(r2, 0, p), s_x1.at[i], r_x1.at[i], xnext) for i, p in enumerate(SUM1)]
    ac = [remote(part_of(a_s, mine, p), part_of(a_s, mine, p), s_a.at[i], r_a.at[i], partner) for i, p in enumerate(SUM1)]
    d2 = [remote(part_of(p2, other, p), part_of(r1b, 0, p), s_d2.at[i], r_d2.at[i], partner) for i, p in enumerate(SUM2)]
    x2 = [remote(part_of(s2, 0, p), part_of(r2b, 0, p), s_x2.at[i], r_x2.at[i], xnext) for i, p in enumerate(SUM2)]
    yo = [remote(part_of(y_s.at[0], mine, p), part_of(y_s.at[0], mine, p), s_o.at[i], r_o.at[i], partner) for i, p in enumerate(SUM2)]
    yy = [remote(part_of(y_s.at[0], mine, p), part_of(y_s.at[1], mine, p), s_y.at[i], r_y.at[i], ynext) for i, p in enumerate(SUM2)]
    yf = [remote(part_of(y_s.at[1], mine, p), part_of(y_s.at[1], mine, p), s_f.at[i], r_f.at[i], partner) for i, p in enumerate(SUM2)]

    def cols_of(c):
        return pl.ds(pl.multiple_of(c * CHUNK, CHUNK), CHUNK)

    for c in d1:
        c.start()
    for c in small:
        c.wait()
    tok_copy.start()
    for i, (first, n) in enumerate(SUM1):
        d1[i].wait_recv()
        for j in range(first, first + n):
            s1[j] = (part_ref[mine + j].astype(F32) + r1[j].astype(F32)).astype(BF16)
        x1[i].start()
    issue(2)
    for i, (first, n) in enumerate(SUM1):
        x1[i].wait_recv()
        issue(1 if i % 2 else 2)
        for j in range(first, first + n):
            total = s1[j].astype(F32) + r2[j].astype(F32)
            a_s[mine + j] = (x_ref[:, cols_of(mine + j)].astype(F32) + total).astype(BF16)
        ac[i].start()
    for c in ac:
        c.wait_recv()
    issue(1)

    def inv_rms(src):
        total = jnp.zeros((ROWS, CHUNK), F32)
        for c in range(NCH):
            v = src[c].astype(F32)
            total = total + v * v
        return lax.rsqrt(jnp.sum(total, axis=-1, keepdims=True) * (1.0 / WIDTH) + EPS)

    inv = inv_rms(a_s)
    gm = gm_ref[...].astype(F32).reshape(1, WIDTH)
    for c in range(NCH):
        cols = slice(c * CHUNK, (c + 1) * CHUNK)
        m_s[:, cols] = (a_s[c].astype(F32) * inv * gm[:, cols]).astype(BF16)

    for i in range(2 * n_mlp):
        mlp_copy(i).wait()
    for i, (r, n) in enumerate(mlp_tiles):
        gslot, uslot = (2 * i) % RING, (2 * i + 1) % RING
        pad = -(-n // BLOCK) * BLOCK
        for b in range(0, pad, BLOCK):
            gate = dot_t(wbuf[gslot, b:b + BLOCK, :], m_s[...])
            up = dot_t(wbuf[uslot, b:b + BLOCK, :], m_s[...])
            hid[:, r + b:r + b + BLOCK] = (gate * jax.nn.sigmoid(gate) * up).T.astype(BF16)
            issue(1, 2 * i)

    for i in range(n_mlp):
        mlp_copy(2 * n_mlp + i).wait()

    def down(c):
        acc = None
        for i, (r, n) in enumerate(mlp_tiles):
            pad = -(-n // BLOCK) * BLOCK
            term = dot(hid[:, r:r + pad], wbuf[(2 * n_mlp + i) % RING, :pad, cols_of(c)])
            acc = term if acc is None else acc + term
        return acc.astype(BF16)

    def chip_sum(i):
        d2[i].wait_recv()
        first, n = SUM2[i]
        for j in range(first, first + n):
            s2[j] = (p2[mine + j].astype(F32) + r1b[j].astype(F32)).astype(BF16)
        x2[i].start()

    for i, (first, n) in enumerate(SUM2):
        for j in range(first, first + n):
            theirs, ours = down(other + j), down(mine + j)
            p2[other + j] = theirs
            p2[mine + j] = ours
            issue(1, 2 * n_mlp)
        d2[i].start()
        if i:
            chip_sum(i - 1)
    chip_sum(len(SUM2) - 1)
    issue(1, 3 * n_mlp)

    def forward(i):
        yy[i].wait_recv()
        yf[i].start()

    for i, (first, n) in enumerate(SUM2):
        x2[i].wait_recv()
        issue(2, 3 * n_mlp)
        for j in range(first, first + n):
            total = s2[j].astype(F32) + r2b[j].astype(F32)
            y_s[0, mine + j] = (a_s[mine + j].astype(F32) + total).astype(BF16)
        yy[i].start()
        yo[i].start()
    for i in range(len(SUM2)):
        forward(i)
    for c in yo:
        c.wait_recv()
    issue(RING, 3 * n_mlp)
    for c in range(NCH):
        y_ref[:, c * CHUNK:(c + 1) * CHUNK] = y_s[0, c]

    gf = gf_ref[...].astype(F32).reshape(1, WIDTH)

    def final_norm(grp):
        inv = inv_rms(y_s.at[grp])
        for c in range(NCH):
            cols = slice(c * CHUNK, (c + 1) * CHUNK)
            f_s[grp * ROWS:(grp + 1) * ROWS, cols] = (y_s[grp, c].astype(F32) * inv * gf[:, cols]).astype(BF16)

    final_norm(0)
    for c in yf:
        c.wait_recv()
    final_norm(1)
    tok_copy.wait()

    tok = jnp.concatenate([tok_ref[...], tok2[...]], axis=1) - (tp * vocab_loc + vbase)
    row_id = lax.broadcasted_iota(jnp.int32, (8, 2 * ROWS), 0)

    def tally(logits, first, state):
        top, tot, tgt = state
        blocks = [logits[8 * i:8 * i + 8] for i in range(logits.shape[0] // 8)]
        peak = blocks[0]
        for v in blocks[1:]:
            peak = jnp.maximum(peak, v)
        new = jnp.maximum(top, peak)
        part_sum = None
        for i, v in enumerate(blocks):
            e = jnp.exp(v - new)
            part_sum = e if part_sum is None else part_sum + e
            tgt = jnp.where(row_id + (first + 8 * i) == tok, v, tgt)
        tot = tot * jnp.exp(top - new) + part_sum
        return new, tot, tgt

    def late(k, state):
        end = (k + 1) * STEP * TILE
        for i, ref in enumerate((late0, late1)):
            state = tally(ref[...], jnp.where(k < 0, -(2 ** 30), end - (2 - i) * BLOCK), state)
        return state

    def some_tiles(k, state):
        for t in range(STEP):
            head_copy(k * STEP + t).wait()
        state = late(k - 1, state)
        todo = [(t, b) for t in range(STEP) for b in range(0, TILE, BLOCK)]
        for n, (t, b) in enumerate(todo):
            i = k * STEP + t
            logits = dot_t(wbuf[lax.rem(head0 + i, RING), pl.ds(b, BLOCK), :], f_s[...])
            if n < len(todo) - 2:
                state = tally(logits, i * TILE + b, state)
            elif n == len(todo) - 2:
                late0[...] = logits
            else:
                late1[...] = logits
        for t in range(STEP):
            i = k * STEP + t

            @pl.when(i + RING < n_full)
            def _():
                head_copy(i + RING).start()

            @pl.when(i + RING == n_full)
            def _():
                head_copy(n_full, n_tail).start()
        return state

    late0[...] = jnp.full(late0.shape, -1e30, F32)
    late1[...] = jnp.full(late1.shape, -1e30, F32)
    state = (jnp.full((8, 2 * ROWS), -1e30, F32), jnp.zeros((8, 2 * ROWS), F32), jnp.zeros((8, 2 * ROWS), F32))
    state = lax.fori_loop(0, n_full // STEP, some_tiles, state)
    head_copy(n_full, n_tail).wait()
    cut = -(-n_tail // 32) * 16
    state = late(n_full // STEP - 1, state)
    for b, size in ((0, cut), (cut, n_tail - cut)):
        logits = dot_t(wbuf[(head0 + n_full) % RING, pl.ds(b, size), :], f_s[...])
        state = tally(logits, n_full * TILE + b, state)
    top, tot, tgt = state
    peak = jnp.max(top, axis=0, keepdims=True)
    tot = jnp.sum(tot * jnp.exp(top - peak), axis=0, keepdims=True)
    tgt = jnp.sum(tgt, axis=0, keepdims=True)
    pad = jnp.zeros((5, ROWS), F32)
    for g in range(2):
        cols = slice(g * ROWS, (g + 1) * ROWS)
        st_s[g] = jnp.concatenate([peak[:, cols], tot[:, cols], tgt[:, cols], pad], axis=0)

    sends = []
    for k in range(1, 8):
        who = lax.rem(dev + k, 8)
        whod, whot = who // 4, lax.rem(who, 4)
        grp = lax.rem(whod + dp, 2)
        sends.append(remote(st_s.at[grp], st_r.at[dev], s_st.at[k - 1], r_st.at[k - 1], (whod, whot)))
    for c in sends:
        c.start()
    st_r[dev] = st_s[0]
    for c in sends:
        c.wait()
    stats = [st_r[i] for i in range(8)]
    peak = stats[0][0:1]
    for s in stats[1:]:
        peak = jnp.maximum(peak, s[0:1])
    tot = jnp.zeros_like(peak)
    tgt = jnp.zeros_like(peak)
    for s in stats:
        tot = tot + s[1:2] * jnp.exp(s[0:1] - peak)
        tgt = tgt + s[2:3]
    lse = peak + jnp.log(tot)
    lse_ref[...] = lse
    logp_ref[...] = tgt - lse

    for group in (d1, x1, ac, d2, x2, yo, yy, yf):
        for c in group:
            c.wait_send()


def emit_kernel(y_in, logp_in, lse_in, y_out, logp_out, lse_out, sem):
    copies = [pltpu.make_async_copy(src, dst, sem.at[i]) for i, (src, dst) in enumerate(((y_in, y_out), (logp_in, logp_out), (lse_in, lse_out)))]
    for c in copies:
        c.start()
    for c in copies:
        c.wait()


def local_step(tok_hidden, seq_lens, k_cache, v_cache, next_tok, g_attn, w_q, b_q, w_k, b_k, w_v, b_v, w_o, g_mlp, w_gate, w_up, w_down, g_final, w_head):
    steps = np.arange(HEAD // 2, dtype=np.float32) * np.float32(-2.0 / HEAD)
    freq = jnp.asarray(np.tile(np.power(np.float64(THETA), steps.astype(np.float64)).astype(np.float32), 2)[None])
    vm = pl.BlockSpec(memory_space=pltpu.VMEM)
    sm = pl.BlockSpec(memory_space=pltpu.SMEM)
    hb = pl.BlockSpec(memory_space=pltpu.HBM)
    dma = pltpu.SemaphoreType.DMA
    cache = jax.ShapeDtypeStruct((ROWS, SLOTS, HEAD), BF16)
    part, k_all, v_all = pl.pallas_call(
        attn_kernel,
        out_shape=(pltpu.VMEM((NCH, ROWS, CHUNK), BF16), cache, cache),
        in_specs=[sm] + [hb] * 13,
        out_specs=(vm, hb, hb),
        scratch_shapes=[
            pltpu.VMEM((1, ROWS), jnp.int32), pltpu.VMEM((1, HEAD), F32), pltpu.VMEM((ROWS, WIDTH), BF16), pltpu.VMEM((WIDTH,), BF16),
            pltpu.VMEM((4 * HEAD,), BF16), pltpu.VMEM((HEAD,), BF16), pltpu.VMEM((HEAD,), BF16),
            pltpu.VMEM((ROWS, SLOTS, HEAD), BF16), pltpu.VMEM((ROWS, SLOTS, HEAD), BF16),
            pltpu.VMEM((WIDTH, 512), BF16), pltpu.VMEM((WIDTH, HEAD), BF16), pltpu.VMEM((WIDTH, HEAD), BF16), pltpu.VMEM((512, WIDTH), BF16),
            pltpu.VMEM((4, ROWS, HEAD), F32), pltpu.VMEM((ROWS, HEAD), F32), pltpu.VMEM((ROWS, HEAD), F32),
            pltpu.VMEM((128, HEAD), F32), pltpu.VMEM((HEAD, 128), BF16), pltpu.VMEM((SLOTS, 128), F32), pltpu.VMEM((128, SLOTS), BF16),
            pltpu.VMEM((128, HEAD), F32), pltpu.VMEM((ROWS, 512), BF16), pltpu.VMEM((8, 128), jnp.int32),
            dma((4,)), dma((4,)), dma((4,)), dma((4,)), dma((4,)), dma((7,)),
        ],
        compiler_params=pltpu.CompilerParams(vmem_limit_bytes=ATTN_BYTES),
        name="attention",
    )(seq_lens, seq_lens.reshape(1, ROWS), freq, tok_hidden, g_attn, b_q, b_k, b_v,
      w_q, w_k, w_v, w_o, k_cache.reshape(ROWS, SLOTS, HEAD), v_cache.reshape(ROWS, SLOTS, HEAD))

    ff = w_gate.shape[1]
    vocab_loc = w_head.shape[0]
    ff_pad = -(-ff // BLOCK) * BLOCK
    chunk4 = pltpu.VMEM((HALF, ROWS, CHUNK), BF16)
    chunk8 = pltpu.VMEM((NCH, ROWS, CHUNK), BF16)

    def kernel(*refs):
        tail_kernel(ff, vocab_loc, *refs)

    y_out, logp, lse = pl.pallas_call(
        kernel,
        out_shape=(pltpu.VMEM((ROWS, WIDTH), BF16), pltpu.VMEM((1, ROWS), F32), pltpu.VMEM((1, ROWS), F32)),
        in_specs=[vm] + [hb] * 8,
        out_specs=(vm, vm, vm),
        scratch_shapes=[
            pltpu.VMEM((ROWS, WIDTH), BF16), pltpu.VMEM((WIDTH,), BF16), pltpu.VMEM((WIDTH,), BF16), pltpu.VMEM((1, ROWS), jnp.int32),
            pltpu.VMEM((RING, TILE, WIDTH), BF16),
            chunk4, chunk4, chunk4, chunk8, pltpu.VMEM((ROWS, WIDTH), BF16), pltpu.VMEM((ROWS, ff_pad), BF16),
            chunk8, chunk4, chunk4, chunk4, pltpu.VMEM((2, NCH, ROWS, CHUNK), BF16), pltpu.VMEM((2 * ROWS, WIDTH), BF16),
            pltpu.VMEM((1, ROWS), jnp.int32), pltpu.VMEM((2, 8, ROWS), F32), pltpu.VMEM((8, 8, ROWS), F32),
            pltpu.VMEM((BLOCK, 2 * ROWS), F32), pltpu.VMEM((BLOCK, 2 * ROWS), F32),
            dma((RING,)),
        ] + [dma((HALF,))] * 16 + [dma, dma, dma((7,)), dma((7,)), dma((4,))],
        compiler_params=pltpu.CompilerParams(vmem_limit_bytes=TAIL_BYTES, collective_id=0, has_side_effects=True),
        name="tail",
    )(pltpu.with_memory_space_constraint(part, pltpu.VMEM), tok_hidden, g_mlp, g_final, next_tok.reshape(1, ROWS), w_gate.T, w_up.T, w_down, w_head)
    vec = jax.ShapeDtypeStruct((1, ROWS), F32)
    y_out, logp, lse = pl.pallas_call(
        emit_kernel,
        out_shape=(jax.ShapeDtypeStruct((ROWS, WIDTH), BF16), vec, vec),
        in_specs=[vm] * 3,
        out_specs=(hb, hb, hb),
        scratch_shapes=[dma((3,))],
        name="emit",
    )(*(pltpu.with_memory_space_constraint(v, pltpu.VMEM) for v in (y_out, logp, lse)))
    shape = (ROWS, SLOTS, 1, HEAD)
    return y_out, k_all.reshape(shape), v_all.reshape(shape), logp.reshape(ROWS), lse.reshape(ROWS)


def solution(mesh):
    row_spec = P('dp', None)
    vec_spec = P('dp')
    cache_spec = P('dp', None, 'tp', None)
    col_spec = P(None, 'tp')
    part_spec = P('tp')
    whole_spec = P(None)
    in_specs = (row_spec, vec_spec, cache_spec, cache_spec, vec_spec, whole_spec, col_spec, part_spec, col_spec, part_spec, col_spec, part_spec, P('tp', None), whole_spec, col_spec, col_spec, P('tp', None), whole_spec, P('tp', None))
    out_specs = (row_spec, cache_spec, cache_spec, vec_spec, vec_spec)
    return jax.shard_map(local_step, mesh=mesh, in_specs=in_specs, out_specs=out_specs, check_vma=False)
```

```python
import jax
import numpy as np
import jax.numpy as jnp
from jax import lax
from jax.experimental import pallas as pl
from jax.experimental.pallas import tpu as pltpu
from jax.sharding import PartitionSpec as P

THETA = 1000000.0
EPS = 1e-6
MESH = pl.DeviceIdType.MESH
F32 = jnp.float32
BF16 = jnp.bfloat16
ATTN_BYTES = 62 * 2 ** 20
TAIL_BYTES = 65500000

ROWS = 128
WIDTH = 2048
HEAD = 128
SLOTS = 512
GROUP = 32
CHUNK = 256
NCH = 8
HALF = 4
BLOCK = 256
HBLK = 192
SUM1 = ((0, 1), (1, 1), (2, 1), (3, 1))
SUM2 = ((0, 1), (1, 1), (2, 1), (3, 1))
TILE = 768
RING = 18
STEP = 8


def dot(a, b):
    return lax.dot_general(a, b, (((1,), (0,)), ((), ())), preferred_element_type=F32)


def dot_t(a, b):
    return lax.dot_general(a, b, (((1,), (1,)), ((), ())), preferred_element_type=F32)


def attn_kernel(lens_ref, lenv_hbm, freq_hbm, x_hbm, g_hbm, bq_hbm, bk_hbm, bv_hbm,
                wq_hbm, wk_hbm, wv_hbm, wo_hbm, k_hbm, v_hbm,
                part_ref, ko_hbm, vo_hbm,
                lenv_ref, freq_ref, x_ref, g_ref, bq_ref, bk_ref, bv_ref,
                kbuf, vbuf, wq, wk, wv, wo, q_s, k_s, v_s, qg_s, qt_s, sc_s, pt_s, o_s, at_s, ll_s,
                wsem, ksem, vsem, kosem, vosem, insem):
    groups = ROWS // GROUP
    part = GROUP // 4
    small = [pltpu.make_async_copy(src, dst, insem.at[i]) for i, (src, dst) in enumerate((
        (x_hbm, x_ref), (lenv_hbm, lenv_ref), (freq_hbm, freq_ref), (g_hbm, g_ref), (bq_hbm, bq_ref), (bk_hbm, bk_ref), (bv_hbm, bv_ref)))]
    for c in small:
        c.start()
    for i, (src, dst) in enumerate(((wq_hbm, wq), (wk_hbm, wk), (wv_hbm, wv))):
        pltpu.make_async_copy(src, dst, wsem.at[i]).start()

    def start_in(g, hbm, buf, sem):
        for i in range(4):
            rows = pl.ds(g * GROUP + i * part, part)
            pltpu.make_async_copy(hbm.at[rows], buf.at[rows], sem.at[g]).start()

    for c in small:
        c.wait()
    start_in(0, k_hbm, kbuf, ksem)
    start_in(0, v_hbm, vbuf, vsem)
    len_rows = jnp.broadcast_to(lenv_ref[...].astype(F32), (ROWS, ROWS)).T
    angles = len_rows * freq_ref[...]
    cos = jnp.cos(angles)
    sin = jnp.sin(angles) * jnp.where(lax.broadcasted_iota(jnp.int32, (ROWS, HEAD), 1) < HEAD // 2, -1.0, 1.0)
    seq_of = lax.broadcasted_iota(jnp.int32, (GROUP, 128), 1) // 4
    pick = lax.broadcasted_iota(jnp.int32, (GROUP, 128), 0) == seq_of
    for g in range(groups):
        ll_s[g:g + 1, :] = jnp.sum(jnp.where(pick, len_rows[g * GROUP:(g + 1) * GROUP], 0.0), axis=0, keepdims=True).astype(jnp.int32)

    x = x_ref[...].astype(F32)
    inv = lax.rsqrt(jnp.mean(x * x, axis=-1, keepdims=True) + EPS)
    normed = (x * inv * g_ref[...].astype(F32).reshape(1, WIDTH)).astype(BF16)
    for i, (src, dst) in enumerate(((wq_hbm, wq), (wk_hbm, wk), (wv_hbm, wv))):
        pltpu.make_async_copy(src, dst, wsem.at[i]).wait()

    start_in(1, k_hbm, kbuf, ksem)

    def rope(u):
        return u * cos + pltpu.roll(u, HEAD // 2, 1) * sin

    k_s[...] = rope(dot(normed, wk[...]) + bk_ref[...].astype(F32).reshape(1, HEAD))
    v_s[...] = dot(normed, wv[...]) + bv_ref[...].astype(F32).reshape(1, HEAD)
    q_all = dot(normed, wq[...]) + bq_ref[...].astype(F32).reshape(1, 4 * HEAD)
    for h in range(4):
        q_s[h] = rope(q_all[:, h * HEAD:(h + 1) * HEAD])

    lane_seq = lax.broadcasted_iota(jnp.int32, (HEAD, 128), 1) // 4
    slot_id = lax.broadcasted_iota(jnp.int32, (SLOTS, 128), 0)
    row16 = lax.broadcasted_iota(jnp.int32, (16, HEAD), 0)
    row_seq = lax.broadcasted_iota(jnp.int32, (16, HEAD), 0) // 4

    def start_out(g):
        write(g, kbuf, ko_hbm, kosem)
        write(g, vbuf, vo_hbm, vosem)

    def write(g, buf, hbm, sem):
        for i in range(4):
            rows = pl.ds(g * GROUP + i * part, part)
            pltpu.make_async_copy(buf.at[rows], hbm.at[rows], sem.at[g]).start()

    def one_group(g, _):
        rows = pl.ds(pl.multiple_of(g * GROUP, GROUP), GROUP)
        pltpu.make_async_copy(k_hbm.at[rows], kbuf.at[rows], ksem.at[g]).wait()

        @pl.when(g + 1 < groups)
        def _():
            start_in(g + 1, v_hbm, vbuf, vsem)

        @pl.when(g + 1 == groups)
        def _():
            pltpu.make_async_copy(wo_hbm, wo, wsem.at[3]).start()

        def put(new_s, buf):
            def one(i, _):
                b = g * GROUP + i
                length = lens_ref[b]
                base = pl.multiple_of((length // 16) * 16, 16)
                old = buf[b, pl.ds(base, 16), :]
                new = jnp.broadcast_to(new_s[pl.ds(b, 1), :].astype(BF16), (16, HEAD))
                buf[b, pl.ds(base, 16), :] = jnp.where(row16 == length - base, new, old)
                return 0
            lax.fori_loop(0, GROUP, one, 0, unroll=8)

        put(k_s, kbuf)

        @pl.when(g + 1 == groups)
        def _():
            start_out(groups - 2)
            write(g, kbuf, ko_hbm, kosem)

        for h in range(4):
            qg_s[pl.ds(h, GROUP, stride=4), :] = q_s[h, rows, :]
        qt_s[...] = qg_s[...].T.astype(BF16)
        qt = qt_s[...]
        zero = jnp.zeros_like(qt)
        top_half, low_half = None, None
        for p in range(GROUP // 2):
            b = g * GROUP + 2 * p
            rhs = jnp.concatenate([jnp.where(lane_seq == 2 * p, qt, zero), jnp.where(lane_seq == 2 * p + 1, qt, zero)], axis=0)
            t0 = dot(jnp.concatenate([kbuf[b, :SLOTS // 2], kbuf[b + 1, :SLOTS // 2]], axis=1), rhs)
            t1 = dot(jnp.concatenate([kbuf[b, SLOTS // 2:], kbuf[b + 1, SLOTS // 2:]], axis=1), rhs)
            top_half = t0 if top_half is None else top_half + t0
            low_half = t1 if low_half is None else low_half + t1
        sc_s[:SLOTS // 2] = top_half
        sc_s[SLOTS // 2:] = low_half
        live = slot_id <= ll_s[pl.ds(g, 1), :]
        scores = jnp.where(live, sc_s[...] * (HEAD ** -0.5), -jnp.inf)
        top = jnp.max(scores, axis=0, keepdims=True)
        exps = jnp.exp(scores - top)
        sc_s[...] = exps
        recip = 1.0 / jnp.sum(exps, axis=0, keepdims=True)
        for i in range(4):
            blk = sc_s[i * 128:(i + 1) * 128, :] * recip
            pt_s[:, i * 128:(i + 1) * 128] = blk.T.astype(BF16)

        pltpu.make_async_copy(v_hbm.at[rows], vbuf.at[rows], vsem.at[g]).wait()

        @pl.when(g + 2 < groups)
        def _():
            start_in(g + 2, k_hbm, kbuf, ksem)

        @pl.when(g + 2 == groups)
        def _():
            for i in range(groups - 2):
                start_out(i)

        put(v_s, vbuf)

        @pl.when(g + 1 == groups)
        def _():
            write(g, vbuf, vo_hbm, vosem)

        for j in range(GROUP // 4):
            b = g * GROUP + 4 * j
            probs = pt_s[16 * j:16 * j + 16, :]
            o = jnp.zeros((16, HEAD), F32)
            for i in range(0, 4, 2):
                out = dot(probs, jnp.concatenate([vbuf[b + i], vbuf[b + i + 1]], axis=1))
                o = jnp.where(row_seq == i, out[:, :HEAD], o)
                o = jnp.where(row_seq == i + 1, out[:, HEAD:], o)
            o_s[16 * j:16 * j + 16, :] = o
        for h in range(4):
            at_s[rows, h * HEAD:(h + 1) * HEAD] = o_s[pl.ds(h, GROUP, stride=4), :].astype(BF16)
        return 0

    lax.fori_loop(0, groups, one_group, 0)

    pltpu.make_async_copy(wo_hbm, wo, wsem.at[3]).wait()
    attn = at_s[...]
    for c in range(WIDTH // BLOCK):
        part_ref[c] = dot(attn, wo[:, c * BLOCK:(c + 1) * BLOCK]).astype(BF16)
    for g in range(groups):
        rows = pl.ds(g * GROUP, GROUP)
        pltpu.make_async_copy(kbuf.at[rows], ko_hbm.at[rows], kosem.at[g]).wait()
        pltpu.make_async_copy(vbuf.at[rows], vo_hbm.at[rows], vosem.at[g]).wait()


def tail_kernel(ff, vocab_loc,
                part_ref, x_hbm, gm_hbm, gf_hbm, tok_hbm, wg_hbm, wu_hbm, wd_hbm, wh_hbm,
                y_ref, logp_ref, lse_ref,
                x_ref, gm_ref, gf_ref, tok_ref, wbuf, r1, s1, r2, a_s, m_s, hid, p2, r1b, s2, r2b, y_s, f_s, tok2, st_s, st_r, late0, late1,
                wsem, s_d1, r_d1, s_x1, r_x1, s_a, r_a, s_d2, r_d2, s_x2, r_x2,
                s_y, r_y, s_o, r_o, s_f, r_f, s_t, r_t, s_st, r_st, insem):
    dp = lax.axis_index('dp')
    tp = lax.axis_index('tp')
    core = lax.rem(tp, 2)
    dev = dp * 4 + tp
    partner = (dp, tp + 1 - 2 * core)
    xnext = (dp, lax.rem(tp + 2, 4))
    ynext = (1 - dp, tp)
    mine = core * HALF
    other = (1 - core) * HALF

    mlp_tiles = [(i * TILE, min(TILE, ff - i * TILE)) for i in range(-(-ff // TILE))]
    n_mlp = len(mlp_tiles)
    tail_pad = -(-mlp_tiles[-1][1] // BLOCK) * BLOCK
    vocab_half = vocab_loc // 2
    n_full = vocab_half // TILE
    n_tail = vocab_half - n_full * TILE
    n_head = n_full + (1 if n_tail else 0)
    assert n_full % STEP == 0 and n_tail
    head0 = 3 * n_mlp
    vbase = dp * vocab_half

    def mlp_copy(i):
        if i < 2 * n_mlp:
            src, (r, n) = (wg_hbm, wu_hbm)[i % 2], mlp_tiles[i // 2]
        else:
            src, (r, n) = wd_hbm, mlp_tiles[i - 2 * n_mlp]
        slot = i % RING
        return pltpu.make_async_copy(src.at[pl.ds(r, n)], wbuf.at[slot, pl.ds(0, n)], wsem.at[slot])

    def head_copy(i, n=TILE):
        slot = lax.rem(head0 + i, RING)
        start = pl.multiple_of(vbase + i * TILE, 16)
        return pltpu.make_async_copy(wh_hbm.at[pl.ds(start, n)], wbuf.at[slot, pl.ds(0, n)], wsem.at[slot])

    def start_item(i):
        if i < head0:
            mlp_copy(i).start()
        elif i - head0 < n_full:
            head_copy(i - head0).start()
        elif i - head0 < n_head:
            head_copy(i - head0, n_tail).start()

    small = [pltpu.make_async_copy(src, dst, insem.at[i]) for i, (src, dst) in enumerate((
        (x_hbm, x_ref), (gm_hbm, gm_ref), (gf_hbm, gf_ref), (tok_hbm, tok_ref)))]
    for c in small:
        c.start()
    issued = [0]

    def issue(n, freed=0):
        for _ in range(n):
            if issued[0] < RING + freed:
                start_item(issued[0])
                issued[0] += 1

    issue(2)

    barrier = pltpu.get_barrier_semaphore()
    for d in range(2):
        for t in range(4):
            @pl.when(d * 4 + t != dev)
            def _():
                pl.semaphore_signal(barrier, inc=1, device_id=(d, t), device_id_type=MESH)
    last_n = mlp_tiles[-1][1]
    if tail_pad > last_n:
        for i in (2 * n_mlp - 2, 2 * n_mlp - 1, 3 * n_mlp - 1):
            wbuf[i % RING, last_n:tail_pad, :] = jnp.zeros((tail_pad - last_n, WIDTH), BF16)
    pl.semaphore_wait(barrier, 7)
    issue(2)

    def remote(src, dst, ssem, rsem, who):
        return pltpu.make_async_remote_copy(src_ref=src, dst_ref=dst, send_sem=ssem, recv_sem=rsem, device_id=who, device_id_type=MESH)

    tok_copy = remote(tok_ref, tok2, s_t, r_t, ynext)
    def part_of(ref, base, grp):
        return ref.at[pl.ds(base + grp[0], grp[1])]

    d1 = [remote(part_of(part_ref, other, p), part_of(r1, 0, p), s_d1.at[i], r_d1.at[i], partner) for i, p in enumerate(SUM1)]
    x1 = [remote(part_of(s1, 0, p), part_of(r2, 0, p), s_x1.at[i], r_x1.at[i], xnext) for i, p in enumerate(SUM1)]
    ac = [remote(part_of(a_s, mine, p), part_of(a_s, mine, p), s_a.at[i], r_a.at[i], partner) for i, p in enumerate(SUM1)]
    d2 = [remote(part_of(p2, other, p), part_of(r1b, 0, p), s_d2.at[i], r_d2.at[i], partner) for i, p in enumerate(SUM2)]
    x2 = [remote(part_of(s2, 0, p), part_of(r2b, 0, p), s_x2.at[i], r_x2.at[i], xnext) for i, p in enumerate(SUM2)]
    yo = [remote(part_of(y_s.at[0], mine, p), part_of(y_s.at[0], mine, p), s_o.at[i], r_o.at[i], partner) for i, p in enumerate(SUM2)]
    yy = [remote(part_of(y_s.at[0], mine, p), part_of(y_s.at[1], mine, p), s_y.at[i], r_y.at[i], ynext) for i, p in enumerate(SUM2)]
    yf = [remote(part_of(y_s.at[1], mine, p), part_of(y_s.at[1], mine, p), s_f.at[i], r_f.at[i], partner) for i, p in enumerate(SUM2)]

    def cols_of(c):
        return pl.ds(pl.multiple_of(c * CHUNK, CHUNK), CHUNK)

    for c in d1:
        c.start()
    for c in small:
        c.wait()
    tok_copy.start()
    for i, (first, n) in enumerate(SUM1):
        d1[i].wait_recv()
        for j in range(first, first + n):
            s1[j] = (part_ref[mine + j].astype(F32) + r1[j].astype(F32)).astype(BF16)
        x1[i].start()
    issue(2)
    for i, (first, n) in enumerate(SUM1):
        x1[i].wait_recv()
        issue(1 if i % 2 else 2)
        for j in range(first, first + n):
            total = s1[j].astype(F32) + r2[j].astype(F32)
            a_s[mine + j] = (x_ref[:, cols_of(mine + j)].astype(F32) + total).astype(BF16)
        ac[i].start()
    for c in ac:
        c.wait_recv()
    issue(1)

    def inv_rms(src):
        total = jnp.zeros((ROWS, CHUNK), F32)
        for c in range(NCH):
            v = src[c].astype(F32)
            total = total + v * v
        return lax.rsqrt(jnp.sum(total, axis=-1, keepdims=True) * (1.0 / WIDTH) + EPS)

    inv = inv_rms(a_s)
    gm = gm_ref[...].astype(F32).reshape(1, WIDTH)
    for c in range(NCH):
        cols = slice(c * CHUNK, (c + 1) * CHUNK)
        m_s[:, cols] = (a_s[c].astype(F32) * inv * gm[:, cols]).astype(BF16)

    for i in range(2 * n_mlp):
        mlp_copy(i).wait()
    for i, (r, n) in enumerate(mlp_tiles):
        gslot, uslot = (2 * i) % RING, (2 * i + 1) % RING
        pad = -(-n // BLOCK) * BLOCK
        for b in range(0, pad, BLOCK):
            gate = dot_t(wbuf[gslot, b:b + BLOCK, :], m_s[...])
            up = dot_t(wbuf[uslot, b:b + BLOCK, :], m_s[...])
            hid[:, r + b:r + b + BLOCK] = (gate * jax.nn.sigmoid(gate) * up).T.astype(BF16)
            issue(1, 2 * i)

    for i in range(n_mlp):
        mlp_copy(2 * n_mlp + i).wait()

    def down(c):
        acc = None
        for i, (r, n) in enumerate(mlp_tiles):
            pad = -(-n // BLOCK) * BLOCK
            term = dot(hid[:, r:r + pad], wbuf[(2 * n_mlp + i) % RING, :pad, cols_of(c)])
            acc = term if acc is None else acc + term
        return acc.astype(BF16)

    def chip_sum(i):
        d2[i].wait_recv()
        first, n = SUM2[i]
        for j in range(first, first + n):
            s2[j] = (p2[mine + j].astype(F32) + r1b[j].astype(F32)).astype(BF16)
        x2[i].start()

    for i, (first, n) in enumerate(SUM2):
        for j in range(first, first + n):
            theirs, ours = down(other + j), down(mine + j)
            p2[other + j] = theirs
            p2[mine + j] = ours
            issue(1, 2 * n_mlp)
        d2[i].start()
        if i:
            chip_sum(i - 1)
    chip_sum(len(SUM2) - 1)
    issue(1, 3 * n_mlp)

    def forward(i):
        yy[i].wait_recv()
        yf[i].start()

    for i, (first, n) in enumerate(SUM2):
        x2[i].wait_recv()
        issue(2, 3 * n_mlp)
        for j in range(first, first + n):
            total = s2[j].astype(F32) + r2b[j].astype(F32)
            y_s[0, mine + j] = (a_s[mine + j].astype(F32) + total).astype(BF16)
        yy[i].start()
        yo[i].start()
    for i in range(len(SUM2)):
        forward(i)
    for c in yo:
        c.wait_recv()
    issue(RING, 3 * n_mlp)
    for c in range(NCH):
        y_ref[:, c * CHUNK:(c + 1) * CHUNK] = y_s[0, c]

    gf = gf_ref[...].astype(F32).reshape(1, WIDTH)

    def final_norm(grp):
        inv = inv_rms(y_s.at[grp])
        for c in range(NCH):
            cols = slice(c * CHUNK, (c + 1) * CHUNK)
            f_s[cols, grp * ROWS:(grp + 1) * ROWS] = (y_s[grp, c].astype(F32) * inv * gf[:, cols]).T.astype(BF16)

    final_norm(0)
    for c in yf:
        c.wait_recv()
    final_norm(1)
    tok_copy.wait()

    tok = jnp.concatenate([tok_ref[...], tok2[...]], axis=1) - (tp * vocab_loc + vbase)
    row_id = lax.broadcasted_iota(jnp.int32, (8, 2 * ROWS), 0)

    def tally(logits, first, state):
        top, tot, tgt = state
        blocks = [logits[8 * i:8 * i + 8] for i in range(logits.shape[0] // 8)]
        peak = blocks[0]
        for v in blocks[1:]:
            peak = jnp.maximum(peak, v)
        new = jnp.maximum(top, peak)
        part_sum = None
        for i, v in enumerate(blocks):
            e = jnp.exp(v - new)
            part_sum = e if part_sum is None else part_sum + e
            tgt = jnp.where(row_id + (first + 8 * i) == tok, v, tgt)
        tot = tot * jnp.exp(top - new) + part_sum
        return new, tot, tgt

    def late(k, state):
        end = (k + 1) * STEP * TILE
        for i, ref in enumerate((late0, late1)):
            state = tally(ref[...], jnp.where(k < 0, -(2 ** 30), end - (2 - i) * HBLK), state)
        return state

    def some_tiles(k, state):
        for t in range(STEP):
            head_copy(k * STEP + t).wait()
        state = late(k - 1, state)
        todo = [(t, b) for t in range(STEP) for b in range(0, TILE, HBLK)]
        for n, (t, b) in enumerate(todo):
            i = k * STEP + t
            logits = dot(wbuf[lax.rem(head0 + i, RING), pl.ds(b, HBLK), :], f_s[...])
            if n < len(todo) - 2:
                state = tally(logits, i * TILE + b, state)
            elif n == len(todo) - 2:
                late0[...] = logits
            else:
                late1[...] = logits
        for t in range(STEP):
            i = k * STEP + t

            @pl.when(i + RING < n_full)
            def _():
                head_copy(i + RING).start()

            @pl.when(i + RING == n_full)
            def _():
                head_copy(n_full, n_tail).start()
        return state

    late0[...] = jnp.full(late0.shape, -1e30, F32)
    late1[...] = jnp.full(late1.shape, -1e30, F32)
    state = (jnp.full((8, 2 * ROWS), -1e30, F32), jnp.zeros((8, 2 * ROWS), F32), jnp.zeros((8, 2 * ROWS), F32))
    state = lax.fori_loop(0, n_full // STEP, some_tiles, state)
    head_copy(n_full, n_tail).wait()
    state = late(n_full // STEP - 1, state)
    cut = -(-n_tail // 64) * 16
    for b in range(0, n_tail, cut):
        logits = dot(wbuf[(head0 + n_full) % RING, pl.ds(b, min(cut, n_tail - b)), :], f_s[...])
        state = tally(logits, n_full * TILE + b, state)
    top, tot, tgt = state
    peak = jnp.max(top, axis=0, keepdims=True)
    tot = jnp.sum(tot * jnp.exp(top - peak), axis=0, keepdims=True)
    tgt = jnp.sum(tgt, axis=0, keepdims=True)
    pad = jnp.zeros((5, ROWS), F32)
    for g in range(2):
        cols = slice(g * ROWS, (g + 1) * ROWS)
        st_s[g] = jnp.concatenate([peak[:, cols], tot[:, cols], tgt[:, cols], pad], axis=0)

    sends = []
    for k in range(1, 8):
        who = lax.rem(dev + k, 8)
        whod, whot = who // 4, lax.rem(who, 4)
        grp = lax.rem(whod + dp, 2)
        sends.append(remote(st_s.at[grp], st_r.at[dev], s_st.at[k - 1], r_st.at[k - 1], (whod, whot)))
    for c in sends:
        c.start()
    st_r[dev] = st_s[0]
    for c in sends:
        c.wait()
    stats = [st_r[i] for i in range(8)]
    peak = stats[0][0:1]
    for s in stats[1:]:
        peak = jnp.maximum(peak, s[0:1])
    tot = jnp.zeros_like(peak)
    tgt = jnp.zeros_like(peak)
    for s in stats:
        tot = tot + s[1:2] * jnp.exp(s[0:1] - peak)
        tgt = tgt + s[2:3]
    lse = peak + jnp.log(tot)
    lse_ref[...] = lse
    logp_ref[...] = tgt - lse

    for group in (d1, x1, ac, d2, x2, yo, yy, yf):
        for c in group:
            c.wait_send()


def emit_kernel(y_in, logp_in, lse_in, y_out, logp_out, lse_out, sem):
    copies = [pltpu.make_async_copy(src, dst, sem.at[i]) for i, (src, dst) in enumerate(((y_in, y_out), (logp_in, logp_out), (lse_in, lse_out)))]
    for c in copies:
        c.start()
    for c in copies:
        c.wait()


def local_step(tok_hidden, seq_lens, k_cache, v_cache, next_tok, g_attn, w_q, b_q, w_k, b_k, w_v, b_v, w_o, g_mlp, w_gate, w_up, w_down, g_final, w_head):
    steps = np.arange(HEAD // 2, dtype=np.float32) * np.float32(-2.0 / HEAD)
    freq = jnp.asarray(np.tile(np.power(np.float64(THETA), steps.astype(np.float64)).astype(np.float32), 2)[None])
    vm = pl.BlockSpec(memory_space=pltpu.VMEM)
    sm = pl.BlockSpec(memory_space=pltpu.SMEM)
    hb = pl.BlockSpec(memory_space=pltpu.HBM)
    dma = pltpu.SemaphoreType.DMA
    cache = jax.ShapeDtypeStruct((ROWS, SLOTS, HEAD), BF16)
    part, k_all, v_all = pl.pallas_call(
        attn_kernel,
        out_shape=(pltpu.VMEM((NCH, ROWS, CHUNK), BF16), cache, cache),
        in_specs=[sm] + [hb] * 13,
        out_specs=(vm, hb, hb),
        scratch_shapes=[
            pltpu.VMEM((1, ROWS), jnp.int32), pltpu.VMEM((1, HEAD), F32), pltpu.VMEM((ROWS, WIDTH), BF16), pltpu.VMEM((WIDTH,), BF16),
            pltpu.VMEM((4 * HEAD,), BF16), pltpu.VMEM((HEAD,), BF16), pltpu.VMEM((HEAD,), BF16),
            pltpu.VMEM((ROWS, SLOTS, HEAD), BF16), pltpu.VMEM((ROWS, SLOTS, HEAD), BF16),
            pltpu.VMEM((WIDTH, 512), BF16), pltpu.VMEM((WIDTH, HEAD), BF16), pltpu.VMEM((WIDTH, HEAD), BF16), pltpu.VMEM((512, WIDTH), BF16),
            pltpu.VMEM((4, ROWS, HEAD), F32), pltpu.VMEM((ROWS, HEAD), F32), pltpu.VMEM((ROWS, HEAD), F32),
            pltpu.VMEM((128, HEAD), F32), pltpu.VMEM((HEAD, 128), BF16), pltpu.VMEM((SLOTS, 128), F32), pltpu.VMEM((128, SLOTS), BF16),
            pltpu.VMEM((128, HEAD), F32), pltpu.VMEM((ROWS, 512), BF16), pltpu.VMEM((8, 128), jnp.int32),
            dma((4,)), dma((4,)), dma((4,)), dma((4,)), dma((4,)), dma((7,)),
        ],
        compiler_params=pltpu.CompilerParams(vmem_limit_bytes=ATTN_BYTES),
        name="attention",
    )(seq_lens, seq_lens.reshape(1, ROWS), freq, tok_hidden, g_attn, b_q, b_k, b_v,
      w_q, w_k, w_v, w_o, k_cache.reshape(ROWS, SLOTS, HEAD), v_cache.reshape(ROWS, SLOTS, HEAD))

    ff = w_gate.shape[1]
    vocab_loc = w_head.shape[0]
    ff_pad = -(-ff // BLOCK) * BLOCK
    chunk4 = pltpu.VMEM((HALF, ROWS, CHUNK), BF16)
    chunk8 = pltpu.VMEM((NCH, ROWS, CHUNK), BF16)

    def kernel(*refs):
        tail_kernel(ff, vocab_loc, *refs)

    y_out, logp, lse = pl.pallas_call(
        kernel,
        out_shape=(pltpu.VMEM((ROWS, WIDTH), BF16), pltpu.VMEM((1, ROWS), F32), pltpu.VMEM((1, ROWS), F32)),
        in_specs=[vm] + [hb] * 8,
        out_specs=(vm, vm, vm),
        scratch_shapes=[
            pltpu.VMEM((ROWS, WIDTH), BF16), pltpu.VMEM((WIDTH,), BF16), pltpu.VMEM((WIDTH,), BF16), pltpu.VMEM((1, ROWS), jnp.int32),
            pltpu.VMEM((RING, TILE, WIDTH), BF16),
            chunk4, chunk4, chunk4, chunk8, pltpu.VMEM((ROWS, WIDTH), BF16), pltpu.VMEM((ROWS, ff_pad), BF16),
            chunk8, chunk4, chunk4, chunk4, pltpu.VMEM((2, NCH, ROWS, CHUNK), BF16), pltpu.VMEM((WIDTH, 2 * ROWS), BF16),
            pltpu.VMEM((1, ROWS), jnp.int32), pltpu.VMEM((2, 8, ROWS), F32), pltpu.VMEM((8, 8, ROWS), F32),
            pltpu.VMEM((HBLK, 2 * ROWS), F32), pltpu.VMEM((HBLK, 2 * ROWS), F32),
            dma((RING,)),
        ] + [dma((HALF,))] * 16 + [dma, dma, dma((7,)), dma((7,)), dma((4,))],
        compiler_params=pltpu.CompilerParams(vmem_limit_bytes=TAIL_BYTES, collective_id=0, has_side_effects=True),
        name="tail",
    )(pltpu.with_memory_space_constraint(part, pltpu.VMEM), tok_hidden, g_mlp, g_final, next_tok.reshape(1, ROWS), w_gate.T, w_up.T, w_down, w_head)
    vec = jax.ShapeDtypeStruct((1, ROWS), F32)
    y_out, logp, lse = pl.pallas_call(
        emit_kernel,
        out_shape=(jax.ShapeDtypeStruct((ROWS, WIDTH), BF16), vec, vec),
        in_specs=[vm] * 3,
        out_specs=(hb, hb, hb),
        scratch_shapes=[dma((3,))],
        name="emit",
    )(*(pltpu.with_memory_space_constraint(v, pltpu.VMEM) for v in (y_out, logp, lse)))
    shape = (ROWS, SLOTS, 1, HEAD)
    return y_out, k_all.reshape(shape), v_all.reshape(shape), logp.reshape(ROWS), lse.reshape(ROWS)


def solution(mesh):
    row_spec = P('dp', None)
    vec_spec = P('dp')
    cache_spec = P('dp', None, 'tp', None)
    col_spec = P(None, 'tp')
    part_spec = P('tp')
    whole_spec = P(None)
    in_specs = (row_spec, vec_spec, cache_spec, cache_spec, vec_spec, whole_spec, col_spec, part_spec, col_spec, part_spec, col_spec, part_spec, P('tp', None), whole_spec, col_spec, col_spec, P('tp', None), whole_spec, P('tp', None))
    out_specs = (row_spec, cache_spec, cache_spec, vec_spec, vec_spec)
    return jax.shard_map(local_step, mesh=mesh, in_specs=in_specs, out_specs=out_specs, check_vma=False)
```

```python
import jax
import numpy as np
import jax.numpy as jnp
from jax import lax
from jax.experimental import pallas as pl
from jax.experimental.pallas import tpu as pltpu
from jax.sharding import PartitionSpec as P

THETA = 1000000.0
EPS = 1e-6
MESH = pl.DeviceIdType.MESH
F32 = jnp.float32
BF16 = jnp.bfloat16
ATTN_BYTES = 62 * 2 ** 20
TAIL_BYTES = 65500000

ROWS = 128
WIDTH = 2048
HEAD = 128
SLOTS = 512
GROUP = 32
CHUNK = 256
NCH = 8
BLOCK = 256
OWN = ((0, 1, 2), (3, 4, 5, 6, 7))
MOST = 5
TILE = 768
RING = 17
STEP = 4


def dot(a, b):
    return lax.dot_general(a, b, (((1,), (0,)), ((), ())), preferred_element_type=F32)


def dot_t(a, b):
    return lax.dot_general(a, b, (((1,), (1,)), ((), ())), preferred_element_type=F32)


def attn_kernel(lens_ref, lenv_hbm, freq_hbm, x_hbm, g_hbm, bq_hbm, bk_hbm, bv_hbm,
                wq_hbm, wk_hbm, wv_hbm, wo_hbm, k_hbm, v_hbm,
                part_ref, ko_hbm, vo_hbm,
                lenv_ref, freq_ref, x_ref, g_ref, bq_ref, bk_ref, bv_ref,
                kbuf, vbuf, wq, wk, wv, wo, q_s, k_s, v_s, qg_s, qt_s, sc_s, pt_s, o_s, at_s, ll_s,
                wsem, ksem, vsem, kosem, vosem, insem):
    groups = ROWS // GROUP
    part = GROUP // 4
    small = [pltpu.make_async_copy(src, dst, insem.at[i]) for i, (src, dst) in enumerate((
        (x_hbm, x_ref), (lenv_hbm, lenv_ref), (freq_hbm, freq_ref), (g_hbm, g_ref), (bq_hbm, bq_ref), (bk_hbm, bk_ref), (bv_hbm, bv_ref)))]
    for c in small:
        c.start()
    for i, (src, dst) in enumerate(((wq_hbm, wq), (wk_hbm, wk), (wv_hbm, wv))):
        pltpu.make_async_copy(src, dst, wsem.at[i]).start()

    def start_in(g, hbm, buf, sem):
        for i in range(4):
            rows = pl.ds(g * GROUP + i * part, part)
            pltpu.make_async_copy(hbm.at[rows], buf.at[rows], sem.at[g]).start()

    for c in small:
        c.wait()
    start_in(0, k_hbm, kbuf, ksem)
    start_in(0, v_hbm, vbuf, vsem)
    len_rows = jnp.broadcast_to(lenv_ref[...].astype(F32), (ROWS, ROWS)).T
    angles = len_rows * freq_ref[...]
    cos = jnp.cos(angles)
    sin = jnp.sin(angles) * jnp.where(lax.broadcasted_iota(jnp.int32, (ROWS, HEAD), 1) < HEAD // 2, -1.0, 1.0)
    seq_of = lax.broadcasted_iota(jnp.int32, (GROUP, 128), 1) // 4
    pick = lax.broadcasted_iota(jnp.int32, (GROUP, 128), 0) == seq_of
    for g in range(groups):
        ll_s[g:g + 1, :] = jnp.sum(jnp.where(pick, len_rows[g * GROUP:(g + 1) * GROUP], 0.0), axis=0, keepdims=True).astype(jnp.int32)

    x = x_ref[...].astype(F32)
    inv = lax.rsqrt(jnp.mean(x * x, axis=-1, keepdims=True) + EPS)
    normed = (x * inv * g_ref[...].astype(F32).reshape(1, WIDTH)).astype(BF16)
    for i, (src, dst) in enumerate(((wq_hbm, wq), (wk_hbm, wk), (wv_hbm, wv))):
        pltpu.make_async_copy(src, dst, wsem.at[i]).wait()

    start_in(1, k_hbm, kbuf, ksem)

    def rope(u):
        return u * cos + pltpu.roll(u, HEAD // 2, 1) * sin

    k_s[...] = rope(dot(normed, wk[...]) + bk_ref[...].astype(F32).reshape(1, HEAD))
    v_s[...] = dot(normed, wv[...]) + bv_ref[...].astype(F32).reshape(1, HEAD)
    q_all = dot(normed, wq[...]) + bq_ref[...].astype(F32).reshape(1, 4 * HEAD)
    for h in range(4):
        q_s[h] = rope(q_all[:, h * HEAD:(h + 1) * HEAD])

    lane_seq = lax.broadcasted_iota(jnp.int32, (HEAD, 128), 1) // 4
    slot_id = lax.broadcasted_iota(jnp.int32, (SLOTS, 128), 0)
    row16 = lax.broadcasted_iota(jnp.int32, (16, HEAD), 0)
    row_seq = lax.broadcasted_iota(jnp.int32, (16, HEAD), 0) // 4

    def start_out(g):
        write(g, kbuf, ko_hbm, kosem)
        write(g, vbuf, vo_hbm, vosem)

    def write(g, buf, hbm, sem):
        for i in range(4):
            rows = pl.ds(g * GROUP + i * part, part)
            pltpu.make_async_copy(buf.at[rows], hbm.at[rows], sem.at[g]).start()

    def one_group(g, _):
        rows = pl.ds(pl.multiple_of(g * GROUP, GROUP), GROUP)
        pltpu.make_async_copy(k_hbm.at[rows], kbuf.at[rows], ksem.at[g]).wait()

        @pl.when(g + 1 < groups)
        def _():
            start_in(g + 1, v_hbm, vbuf, vsem)

        @pl.when(g + 1 == groups)
        def _():
            pltpu.make_async_copy(wo_hbm, wo, wsem.at[3]).start()

        def put(new_s, buf):
            def one(i, _):
                b = g * GROUP + i
                length = lens_ref[b]
                base = pl.multiple_of((length // 16) * 16, 16)
                old = buf[b, pl.ds(base, 16), :]
                new = jnp.broadcast_to(new_s[pl.ds(b, 1), :].astype(BF16), (16, HEAD))
                buf[b, pl.ds(base, 16), :] = jnp.where(row16 == length - base, new, old)
                return 0
            lax.fori_loop(0, GROUP, one, 0, unroll=8)

        put(k_s, kbuf)

        @pl.when(g + 1 == groups)
        def _():
            start_out(groups - 2)
            write(g, kbuf, ko_hbm, kosem)

        for h in range(4):
            qg_s[pl.ds(h, GROUP, stride=4), :] = q_s[h, rows, :]
        qt_s[...] = qg_s[...].T.astype(BF16)
        qt = qt_s[...]
        zero = jnp.zeros_like(qt)
        top_half, low_half = None, None
        for p in range(GROUP // 2):
            b = g * GROUP + 2 * p
            rhs = jnp.concatenate([jnp.where(lane_seq == 2 * p, qt, zero), jnp.where(lane_seq == 2 * p + 1, qt, zero)], axis=0)
            t0 = dot(jnp.concatenate([kbuf[b, :SLOTS // 2], kbuf[b + 1, :SLOTS // 2]], axis=1), rhs)
            t1 = dot(jnp.concatenate([kbuf[b, SLOTS // 2:], kbuf[b + 1, SLOTS // 2:]], axis=1), rhs)
            top_half = t0 if top_half is None else top_half + t0
            low_half = t1 if low_half is None else low_half + t1
        sc_s[:SLOTS // 2] = top_half
        sc_s[SLOTS // 2:] = low_half
        live = slot_id <= ll_s[pl.ds(g, 1), :]
        scores = jnp.where(live, sc_s[...] * (HEAD ** -0.5), -jnp.inf)
        top = jnp.max(scores, axis=0, keepdims=True)
        exps = jnp.exp(scores - top)
        sc_s[...] = exps
        recip = 1.0 / jnp.sum(exps, axis=0, keepdims=True)
        for i in range(4):
            blk = sc_s[i * 128:(i + 1) * 128, :] * recip
            pt_s[:, i * 128:(i + 1) * 128] = blk.T.astype(BF16)

        pltpu.make_async_copy(v_hbm.at[rows], vbuf.at[rows], vsem.at[g]).wait()

        @pl.when(g + 2 < groups)
        def _():
            start_in(g + 2, k_hbm, kbuf, ksem)

        @pl.when(g + 2 == groups)
        def _():
            for i in range(groups - 2):
                start_out(i)

        put(v_s, vbuf)

        @pl.when(g + 1 == groups)
        def _():
            write(g, vbuf, vo_hbm, vosem)

        for j in range(GROUP // 4):
            b = g * GROUP + 4 * j
            probs = pt_s[16 * j:16 * j + 16, :]
            o = jnp.zeros((16, HEAD), F32)
            for i in range(0, 4, 2):
                out = dot(probs, jnp.concatenate([vbuf[b + i], vbuf[b + i + 1]], axis=1))
                o = jnp.where(row_seq == i, out[:, :HEAD], o)
                o = jnp.where(row_seq == i + 1, out[:, HEAD:], o)
            o_s[16 * j:16 * j + 16, :] = o
        for h in range(4):
            at_s[rows, h * HEAD:(h + 1) * HEAD] = o_s[pl.ds(h, GROUP, stride=4), :].astype(BF16)
        return 0

    lax.fori_loop(0, groups, one_group, 0)

    pltpu.make_async_copy(wo_hbm, wo, wsem.at[3]).wait()
    attn = at_s[...]
    for c in range(WIDTH // BLOCK):
        part_ref[c] = dot(attn, wo[:, c * BLOCK:(c + 1) * BLOCK]).astype(BF16)
    for g in range(groups):
        rows = pl.ds(g * GROUP, GROUP)
        pltpu.make_async_copy(kbuf.at[rows], ko_hbm.at[rows], kosem.at[g]).wait()
        pltpu.make_async_copy(vbuf.at[rows], vo_hbm.at[rows], vosem.at[g]).wait()


def tail_kernel(ff, vocab_loc,
                part_ref, x_hbm, gm_hbm, gf_hbm, tok_hbm, wg_hbm, wu_hbm, wd_hbm, wh_hbm,
                y_ref, logp_ref, lse_ref,
                x_ref, gm_ref, gf_ref, tok_ref, wbuf, r1, s1, r2, a_s, m_s, hid, p2, r1b, s2, r2b, y_s, f_s, tok2, st_s, st_r, late0, late1,
                wsem, s_d1, r_d1, s_x1, r_x1, s_a, r_a, s_d2, r_d2, s_x2, r_x2,
                s_y, r_y, s_o, r_o, s_f, r_f, s_t, r_t, s_st, r_st, insem):
    dp = lax.axis_index('dp')
    tp = lax.axis_index('tp')
    core = lax.rem(tp, 2)
    dev = dp * 4 + tp
    partner = (dp, tp + 1 - 2 * core)
    xnext = (dp, lax.rem(tp + 2, 4))
    ynext = (1 - dp, tp)

    mlp_tiles = [(i * TILE, min(TILE, ff - i * TILE)) for i in range(-(-ff // TILE))]
    n_mlp = len(mlp_tiles)
    tail_pad = -(-mlp_tiles[-1][1] // BLOCK) * BLOCK
    vocab_half = vocab_loc // 2
    n_full = vocab_half // TILE
    n_tail = vocab_half - n_full * TILE
    n_head = n_full + (1 if n_tail else 0)
    assert n_full % STEP == 0 and n_tail
    head0 = 3 * n_mlp
    vbase = dp * vocab_half

    def mlp_copy(i):
        if i < 2 * n_mlp:
            src, (r, n) = (wg_hbm, wu_hbm)[i % 2], mlp_tiles[i // 2]
        else:
            src, (r, n) = wd_hbm, mlp_tiles[i - 2 * n_mlp]
        slot = i % RING
        return pltpu.make_async_copy(src.at[pl.ds(r, n)], wbuf.at[slot, pl.ds(0, n)], wsem.at[slot])

    def head_copy(i, n=TILE):
        slot = lax.rem(head0 + i, RING)
        start = pl.multiple_of(vbase + i * TILE, 16)
        return pltpu.make_async_copy(wh_hbm.at[pl.ds(start, n)], wbuf.at[slot, pl.ds(0, n)], wsem.at[slot])

    def start_item(i):
        if i < head0:
            mlp_copy(i).start()
        elif i - head0 < n_full:
            head_copy(i - head0).start()
        elif i - head0 < n_head:
            head_copy(i - head0, n_tail).start()

    small = [pltpu.make_async_copy(src, dst, insem.at[i]) for i, (src, dst) in enumerate((
        (x_hbm, x_ref), (gm_hbm, gm_ref), (gf_hbm, gf_ref), (tok_hbm, tok_ref)))]
    for c in small:
        c.start()
    issued = [0]

    def issue(n, freed=0):
        for _ in range(n):
            if issued[0] < RING + freed:
                start_item(issued[0])
                issued[0] += 1

    issue(2)

    barrier = pltpu.get_barrier_semaphore()
    for d in range(2):
        for t in range(4):
            @pl.when(d * 4 + t != dev)
            def _():
                pl.semaphore_signal(barrier, inc=1, device_id=(d, t), device_id_type=MESH)
    last_n = mlp_tiles[-1][1]
    if tail_pad > last_n:
        for i in (2 * n_mlp - 2, 2 * n_mlp - 1, 3 * n_mlp - 1):
            wbuf[i % RING, last_n:tail_pad, :] = jnp.zeros((tail_pad - last_n, WIDTH), BF16)
    pl.semaphore_wait(barrier, 7)
    issue(2)

    def remote(src, dst, ssem, rsem, who):
        return pltpu.make_async_remote_copy(src_ref=src, dst_ref=dst, send_sem=ssem, recv_sem=rsem, device_id=who, device_id_type=MESH)

    tok_copy = remote(tok_ref, tok2, s_t, r_t, ynext)
    def cols_of(c):
        return slice(c * CHUNK, (c + 1) * CHUNK)

    def copies(o):
        own, their = OWN[o], OWN[1 - o]
        d1 = [remote(part_ref.at[c], r1.at[i], s_d1.at[i], r_d1.at[i], partner) for i, c in enumerate(their)]
        x1 = [remote(s1.at[i], r2.at[i], s_x1.at[i], r_x1.at[i], xnext) for i, c in enumerate(own)]
        ac = [remote(a_s.at[c], a_s.at[c], s_a.at[i], r_a.at[i], partner) for i, c in enumerate(own)]
        d2 = [remote(p2.at[c], r1b.at[i], s_d2.at[i], r_d2.at[i], partner) for i, c in enumerate(their)]
        x2 = [remote(s2.at[i], r2b.at[i], s_x2.at[i], r_x2.at[i], xnext) for i, c in enumerate(own)]
        yo = [remote(y_s.at[0, c], y_s.at[0, c], s_o.at[i], r_o.at[i], partner) for i, c in enumerate(own)]
        yy = [remote(y_s.at[0, c], y_s.at[1, c], s_y.at[i], r_y.at[i], ynext) for i, c in enumerate(own)]
        yf = [remote(y_s.at[1, c], y_s.at[1, c], s_f.at[i], r_f.at[i], partner) for i, c in enumerate(own)]
        return d1, x1, ac, d2, x2, yo, yy, yf

    def per_core(run):
        before = issued[0]
        for o in range(2):
            issued[0] = before

            @pl.when(core == o)
            def _():
                run(o)

    def first_sum(o):
        own, their = OWN[o], OWN[1 - o]
        d1, x1, ac = copies(o)[:3]
        arrive = [c for c in copies(1 - o)[0]]
        back = copies(1 - o)[2]
        for c in d1:
            c.start()
        for i, c in enumerate(own):
            arrive[i].wait_recv()
            s1[i] = (part_ref[c].astype(F32) + r1[i].astype(F32)).astype(BF16)
            x1[i].start()
        issue(2)
        for c in small:
            c.wait()
        tok_copy.start()
        for i, c in enumerate(own):
            x1[i].wait_recv()
            issue(min(6 // len(own), 12 - issued[0]))
            total = s1[i].astype(F32) + r2[i].astype(F32)
            a_s[c] = (x_ref[:, cols_of(c)].astype(F32) + total).astype(BF16)
            ac[i].start()
        issue(12 - issued[0])
        for i in range(len(their)):
            back[i].wait_recv()

    per_core(first_sum)
    issue(1)

    def inv_rms(src):
        total = jnp.zeros((ROWS, CHUNK), F32)
        for c in range(NCH):
            v = src[c].astype(F32)
            total = total + v * v
        return lax.rsqrt(jnp.sum(total, axis=-1, keepdims=True) * (1.0 / WIDTH) + EPS)

    inv = inv_rms(a_s)
    gm = gm_ref[...].astype(F32).reshape(1, WIDTH)
    for c in range(NCH):
        cols = slice(c * CHUNK, (c + 1) * CHUNK)
        m_s[:, cols] = (a_s[c].astype(F32) * inv * gm[:, cols]).astype(BF16)

    for i in range(2 * n_mlp):
        mlp_copy(i).wait()
    for i, (r, n) in enumerate(mlp_tiles):
        gslot, uslot = (2 * i) % RING, (2 * i + 1) % RING
        pad = -(-n // BLOCK) * BLOCK
        for b in range(0, pad, BLOCK):
            gate = dot_t(wbuf[gslot, b:b + BLOCK, :], m_s[...])
            up = dot_t(wbuf[uslot, b:b + BLOCK, :], m_s[...])
            hid[:, r + b:r + b + BLOCK] = (gate * jax.nn.sigmoid(gate) * up).T.astype(BF16)
            issue(1, 2 * i)

    for i in range(n_mlp):
        mlp_copy(2 * n_mlp + i).wait()

    def down(c):
        acc = None
        for i, (r, n) in enumerate(mlp_tiles):
            pad = -(-n // BLOCK) * BLOCK
            term = dot(hid[:, r:r + pad], wbuf[(2 * n_mlp + i) % RING, :pad, cols_of(c)])
            acc = term if acc is None else acc + term
        return acc.astype(BF16)

    def second_sum(o):
        own, their = OWN[o], OWN[1 - o]
        _, _, _, d2, x2, yo, yy, yf = copies(o)
        arrive, back = copies(1 - o)[3], copies(1 - o)[5]

        def chip_sum(i):
            arrive[i].wait_recv()
            s2[i] = (p2[own[i]].astype(F32) + r1b[i].astype(F32)).astype(BF16)
            x2[i].start()

        both = min(len(own), len(their))
        rest = (own + their)[both:len(own)] if len(own) > both else their[both:]
        steps = [(their[i], own[i]) for i in range(both)] + [tuple(rest)]
        summed = 0
        for n, pair in enumerate(steps):
            for c, val in zip(pair, [down(c) for c in pair]):
                p2[c] = val
            for c in pair:
                if c in their:
                    d2[their.index(c)].start()
            issue(1, 2 * n_mlp)
            if n and summed < len(own):
                chip_sum(summed)
                summed += 1
        for i in range(summed, len(own)):
            chip_sum(i)
        issue(1, 3 * n_mlp)
        for i, c in enumerate(own):
            x2[i].wait_recv()
            issue(2, 3 * n_mlp)
            total = s2[i].astype(F32) + r2b[i].astype(F32)
            y_s[0, c] = (a_s[c].astype(F32) + total).astype(BF16)
            yy[i].start()
            yo[i].start()
        for i in range(len(own)):
            yy[i].wait_recv()
            yf[i].start()
        issue(RING, 3 * n_mlp)
        for i in range(len(their)):
            back[i].wait_recv()

    per_core(second_sum)
    for c in range(NCH):
        y_ref[:, c * CHUNK:(c + 1) * CHUNK] = y_s[0, c]

    gf = gf_ref[...].astype(F32).reshape(1, WIDTH)

    def final_norm(grp):
        inv = inv_rms(y_s.at[grp])
        for c in range(NCH):
            cols = slice(c * CHUNK, (c + 1) * CHUNK)
            f_s[grp * ROWS:(grp + 1) * ROWS, cols] = (y_s[grp, c].astype(F32) * inv * gf[:, cols]).astype(BF16)

    final_norm(0)

    def forwarded(o):
        for c in copies(1 - o)[7]:
            c.wait_recv()

    per_core(forwarded)
    final_norm(1)
    tok_copy.wait()

    tok = jnp.concatenate([tok_ref[...], tok2[...]], axis=1) - (tp * vocab_loc + vbase)
    row_id = lax.broadcasted_iota(jnp.int32, (8, 2 * ROWS), 0)

    def tally(logits, first, state):
        top, tot, tgt = state
        blocks = [logits[8 * i:8 * i + 8] for i in range(logits.shape[0] // 8)]
        peak = blocks[0]
        for v in blocks[1:]:
            peak = jnp.maximum(peak, v)
        new = jnp.maximum(top, peak)
        part_sum = None
        for i, v in enumerate(blocks):
            e = jnp.exp(v - new)
            part_sum = e if part_sum is None else part_sum + e
            tgt = jnp.where(row_id + (first + 8 * i) == tok, v, tgt)
        tot = tot * jnp.exp(top - new) + part_sum
        return new, tot, tgt

    def late(k, state):
        end = (k + 1) * STEP * TILE
        for i, ref in enumerate((late0, late1)):
            state = tally(ref[...], jnp.where(k < 0, -(2 ** 30), end - (2 - i) * BLOCK), state)
        return state

    def some_tiles(k, state):
        for t in range(STEP):
            head_copy(k * STEP + t).wait()
        state = late(k - 1, state)
        todo = [(t, b) for t in range(STEP) for b in range(0, TILE, BLOCK)]
        for n, (t, b) in enumerate(todo):
            i = k * STEP + t
            logits = dot_t(wbuf[lax.rem(head0 + i, RING), pl.ds(b, BLOCK), :], f_s[...])
            if n < len(todo) - 2:
                state = tally(logits, i * TILE + b, state)
            elif n == len(todo) - 2:
                late0[...] = logits
            else:
                late1[...] = logits
        for t in range(STEP):
            i = k * STEP + t

            @pl.when(i + RING < n_full)
            def _():
                head_copy(i + RING).start()

            @pl.when(i + RING == n_full)
            def _():
                head_copy(n_full, n_tail).start()
        return state

    late0[...] = jnp.full(late0.shape, -1e30, F32)
    late1[...] = jnp.full(late1.shape, -1e30, F32)
    state = (jnp.full((8, 2 * ROWS), -1e30, F32), jnp.zeros((8, 2 * ROWS), F32), jnp.zeros((8, 2 * ROWS), F32))
    state = lax.fori_loop(0, n_full // STEP, some_tiles, state)
    head_copy(n_full, n_tail).wait()
    cut = -(-n_tail // 32) * 16
    state = late(n_full // STEP - 1, state)
    for b, size in ((0, cut), (cut, n_tail - cut)):
        logits = dot_t(wbuf[(head0 + n_full) % RING, pl.ds(b, size), :], f_s[...])
        state = tally(logits, n_full * TILE + b, state)
    top, tot, tgt = state
    peak = jnp.max(top, axis=0, keepdims=True)
    tot = jnp.sum(tot * jnp.exp(top - peak), axis=0, keepdims=True)
    tgt = jnp.sum(tgt, axis=0, keepdims=True)
    pad = jnp.zeros((5, ROWS), F32)
    for g in range(2):
        cols = slice(g * ROWS, (g + 1) * ROWS)
        st_s[g] = jnp.concatenate([peak[:, cols], tot[:, cols], tgt[:, cols], pad], axis=0)

    sends = []
    for k in range(1, 8):
        who = lax.rem(dev + k, 8)
        whod, whot = who // 4, lax.rem(who, 4)
        grp = lax.rem(whod + dp, 2)
        sends.append(remote(st_s.at[grp], st_r.at[dev], s_st.at[k - 1], r_st.at[k - 1], (whod, whot)))
    for c in sends:
        c.start()
    st_r[dev] = st_s[0]
    for c in sends:
        c.wait()
    stats = [st_r[i] for i in range(8)]
    peak = stats[0][0:1]
    for s in stats[1:]:
        peak = jnp.maximum(peak, s[0:1])
    tot = jnp.zeros_like(peak)
    tgt = jnp.zeros_like(peak)
    for s in stats:
        tot = tot + s[1:2] * jnp.exp(s[0:1] - peak)
        tgt = tgt + s[2:3]
    lse = peak + jnp.log(tot)
    lse_ref[...] = lse
    logp_ref[...] = tgt - lse

    def sent(o):
        for group in copies(o):
            for c in group:
                c.wait_send()

    per_core(sent)


def emit_kernel(y_in, logp_in, lse_in, y_out, logp_out, lse_out, sem):
    copies = [pltpu.make_async_copy(src, dst, sem.at[i]) for i, (src, dst) in enumerate(((y_in, y_out), (logp_in, logp_out), (lse_in, lse_out)))]
    for c in copies:
        c.start()
    for c in copies:
        c.wait()


def local_step(tok_hidden, seq_lens, k_cache, v_cache, next_tok, g_attn, w_q, b_q, w_k, b_k, w_v, b_v, w_o, g_mlp, w_gate, w_up, w_down, g_final, w_head):
    steps = np.arange(HEAD // 2, dtype=np.float32) * np.float32(-2.0 / HEAD)
    freq = jnp.asarray(np.tile(np.power(np.float64(THETA), steps.astype(np.float64)).astype(np.float32), 2)[None])
    vm = pl.BlockSpec(memory_space=pltpu.VMEM)
    sm = pl.BlockSpec(memory_space=pltpu.SMEM)
    hb = pl.BlockSpec(memory_space=pltpu.HBM)
    dma = pltpu.SemaphoreType.DMA
    cache = jax.ShapeDtypeStruct((ROWS, SLOTS, HEAD), BF16)
    part, k_all, v_all = pl.pallas_call(
        attn_kernel,
        out_shape=(pltpu.VMEM((NCH, ROWS, CHUNK), BF16), cache, cache),
        in_specs=[sm] + [hb] * 13,
        out_specs=(vm, hb, hb),
        scratch_shapes=[
            pltpu.VMEM((1, ROWS), jnp.int32), pltpu.VMEM((1, HEAD), F32), pltpu.VMEM((ROWS, WIDTH), BF16), pltpu.VMEM((WIDTH,), BF16),
            pltpu.VMEM((4 * HEAD,), BF16), pltpu.VMEM((HEAD,), BF16), pltpu.VMEM((HEAD,), BF16),
            pltpu.VMEM((ROWS, SLOTS, HEAD), BF16), pltpu.VMEM((ROWS, SLOTS, HEAD), BF16),
            pltpu.VMEM((WIDTH, 512), BF16), pltpu.VMEM((WIDTH, HEAD), BF16), pltpu.VMEM((WIDTH, HEAD), BF16), pltpu.VMEM((512, WIDTH), BF16),
            pltpu.VMEM((4, ROWS, HEAD), F32), pltpu.VMEM((ROWS, HEAD), F32), pltpu.VMEM((ROWS, HEAD), F32),
            pltpu.VMEM((128, HEAD), F32), pltpu.VMEM((HEAD, 128), BF16), pltpu.VMEM((SLOTS, 128), F32), pltpu.VMEM((128, SLOTS), BF16),
            pltpu.VMEM((128, HEAD), F32), pltpu.VMEM((ROWS, 512), BF16), pltpu.VMEM((8, 128), jnp.int32),
            dma((4,)), dma((4,)), dma((4,)), dma((4,)), dma((4,)), dma((7,)),
        ],
        compiler_params=pltpu.CompilerParams(vmem_limit_bytes=ATTN_BYTES),
        name="attention",
    )(seq_lens, seq_lens.reshape(1, ROWS), freq, tok_hidden, g_attn, b_q, b_k, b_v,
      w_q, w_k, w_v, w_o, k_cache.reshape(ROWS, SLOTS, HEAD), v_cache.reshape(ROWS, SLOTS, HEAD))

    ff = w_gate.shape[1]
    vocab_loc = w_head.shape[0]
    ff_pad = -(-ff // BLOCK) * BLOCK
    some = pltpu.VMEM((MOST, ROWS, CHUNK), BF16)
    chunk8 = pltpu.VMEM((NCH, ROWS, CHUNK), BF16)

    def kernel(*refs):
        tail_kernel(ff, vocab_loc, *refs)

    y_out, logp, lse = pl.pallas_call(
        kernel,
        out_shape=(pltpu.VMEM((ROWS, WIDTH), BF16), pltpu.VMEM((1, ROWS), F32), pltpu.VMEM((1, ROWS), F32)),
        in_specs=[vm] + [hb] * 8,
        out_specs=(vm, vm, vm),
        scratch_shapes=[
            pltpu.VMEM((ROWS, WIDTH), BF16), pltpu.VMEM((WIDTH,), BF16), pltpu.VMEM((WIDTH,), BF16), pltpu.VMEM((1, ROWS), jnp.int32),
            pltpu.VMEM((RING, TILE, WIDTH), BF16),
            some, some, some, chunk8, pltpu.VMEM((ROWS, WIDTH), BF16), pltpu.VMEM((ROWS, ff_pad), BF16),
            chunk8, some, some, some, pltpu.VMEM((2, NCH, ROWS, CHUNK), BF16), pltpu.VMEM((2 * ROWS, WIDTH), BF16),
            pltpu.VMEM((1, ROWS), jnp.int32), pltpu.VMEM((2, 8, ROWS), F32), pltpu.VMEM((8, 8, ROWS), F32),
            pltpu.VMEM((BLOCK, 2 * ROWS), F32), pltpu.VMEM((BLOCK, 2 * ROWS), F32),
            dma((RING,)),
        ] + [dma((MOST,))] * 16 + [dma, dma, dma((7,)), dma((7,)), dma((4,))],
        compiler_params=pltpu.CompilerParams(vmem_limit_bytes=TAIL_BYTES, collective_id=0, has_side_effects=True),
        name="tail",
    )(pltpu.with_memory_space_constraint(part, pltpu.VMEM), tok_hidden, g_mlp, g_final, next_tok.reshape(1, ROWS), w_gate.T, w_up.T, w_down, w_head)
    vec = jax.ShapeDtypeStruct((1, ROWS), F32)
    y_out, logp, lse = pl.pallas_call(
        emit_kernel,
        out_shape=(jax.ShapeDtypeStruct((ROWS, WIDTH), BF16), vec, vec),
        in_specs=[vm] * 3,
        out_specs=(hb, hb, hb),
        scratch_shapes=[dma((3,))],
        name="emit",
    )(*(pltpu.with_memory_space_constraint(v, pltpu.VMEM) for v in (y_out, logp, lse)))
    shape = (ROWS, SLOTS, 1, HEAD)
    return y_out, k_all.reshape(shape), v_all.reshape(shape), logp.reshape(ROWS), lse.reshape(ROWS)


def solution(mesh):
    row_spec = P('dp', None)
    vec_spec = P('dp')
    cache_spec = P('dp', None, 'tp', None)
    col_spec = P(None, 'tp')
    part_spec = P('tp')
    whole_spec = P(None)
    in_specs = (row_spec, vec_spec, cache_spec, cache_spec, vec_spec, whole_spec, col_spec, part_spec, col_spec, part_spec, col_spec, part_spec, P('tp', None), whole_spec, col_spec, col_spec, P('tp', None), whole_spec, P('tp', None))
    out_specs = (row_spec, cache_spec, cache_spec, vec_spec, vec_spec)
    return jax.shard_map(local_step, mesh=mesh, in_specs=in_specs, out_specs=out_specs, check_vma=False)
```

```python
import jax
import numpy as np
import jax.numpy as jnp
from jax import lax
from jax.experimental import pallas as pl
from jax.experimental.pallas import tpu as pltpu
from jax.sharding import PartitionSpec as P

THETA = 1000000.0
EPS = 1e-6
MESH = pl.DeviceIdType.MESH
F32 = jnp.float32
BF16 = jnp.bfloat16
ATTN_BYTES = 62 * 2 ** 20
TAIL_BYTES = 65500000

ROWS = 128
WIDTH = 2048
HEAD = 128
SLOTS = 512
GROUP = 32
CHUNK = 256
NCH = 8
HALF = 4
BLOCK = 256
SUM1 = ((0, 1), (1, 1), (2, 1), (3, 1))
SUM2 = ((0, 1), (1, 1), (2, 1), (3, 1))
TILE = 768
RING = 18
STEP = 4


def dot(a, b):
    return lax.dot_general(a, b, (((1,), (0,)), ((), ())), preferred_element_type=F32)


def dot_t(a, b):
    return lax.dot_general(a, b, (((1,), (1,)), ((), ())), preferred_element_type=F32)


def attn_kernel(lens_ref, lenv_hbm, freq_hbm, x_hbm, g_hbm, bq_hbm, bk_hbm, bv_hbm,
                wq_hbm, wk_hbm, wv_hbm, wo_hbm, k_hbm, v_hbm,
                part_ref, ko_hbm, vo_hbm,
                lenv_ref, freq_ref, x_ref, g_ref, bq_ref, bk_ref, bv_ref,
                kbuf, vbuf, wq, wk, wv, wo, q_s, k_s, v_s, qg_s, qt_s, sc_s, pt_s, o_s, at_s, ll_s,
                wsem, ksem, vsem, kosem, vosem, insem):
    groups = ROWS // GROUP
    part = GROUP // 4
    small = [pltpu.make_async_copy(src, dst, insem.at[i]) for i, (src, dst) in enumerate((
        (x_hbm, x_ref), (lenv_hbm, lenv_ref), (freq_hbm, freq_ref), (g_hbm, g_ref), (bq_hbm, bq_ref), (bk_hbm, bk_ref), (bv_hbm, bv_ref)))]
    for c in small:
        c.start()
    for i, (src, dst) in enumerate(((wq_hbm, wq), (wk_hbm, wk), (wv_hbm, wv))):
        pltpu.make_async_copy(src, dst, wsem.at[i]).start()

    def start_in(g, hbm, buf, sem, lo=0, hi=4):
        for i in range(lo, hi):
            rows = pl.ds(g * GROUP + i * part, part)
            pltpu.make_async_copy(hbm.at[rows], buf.at[rows], sem.at[g]).start()

    start_in(0, k_hbm, kbuf, ksem, 0, 2)
    for c in small:
        c.wait()
    start_in(0, k_hbm, kbuf, ksem, 2, 4)
    start_in(0, v_hbm, vbuf, vsem)
    len_rows = jnp.broadcast_to(lenv_ref[...].astype(F32), (ROWS, ROWS)).T
    angles = len_rows * freq_ref[...]
    cos = jnp.cos(angles)
    sin = jnp.sin(angles) * jnp.where(lax.broadcasted_iota(jnp.int32, (ROWS, HEAD), 1) < HEAD // 2, -1.0, 1.0)
    seq_of = lax.broadcasted_iota(jnp.int32, (GROUP, 128), 1) // 4
    pick = lax.broadcasted_iota(jnp.int32, (GROUP, 128), 0) == seq_of
    for g in range(groups):
        ll_s[g:g + 1, :] = jnp.sum(jnp.where(pick, len_rows[g * GROUP:(g + 1) * GROUP], 0.0), axis=0, keepdims=True).astype(jnp.int32)

    x = x_ref[...].astype(F32)
    inv = lax.rsqrt(jnp.mean(x * x, axis=-1, keepdims=True) + EPS)
    normed = (x * inv * g_ref[...].astype(F32).reshape(1, WIDTH)).astype(BF16)
    for i, (src, dst) in enumerate(((wq_hbm, wq), (wk_hbm, wk), (wv_hbm, wv))):
        pltpu.make_async_copy(src, dst, wsem.at[i]).wait()

    start_in(1, k_hbm, kbuf, ksem)

    def rope(u):
        return u * cos + pltpu.roll(u, HEAD // 2, 1) * sin

    k_s[...] = rope(dot(normed, wk[...]) + bk_ref[...].astype(F32).reshape(1, HEAD))
    v_s[...] = dot(normed, wv[...]) + bv_ref[...].astype(F32).reshape(1, HEAD)
    q_all = dot(normed, wq[...]) + bq_ref[...].astype(F32).reshape(1, 4 * HEAD)
    for h in range(4):
        q_s[h] = rope(q_all[:, h * HEAD:(h + 1) * HEAD])

    lane_seq = lax.broadcasted_iota(jnp.int32, (HEAD, 128), 1) // 4
    slot_id = lax.broadcasted_iota(jnp.int32, (SLOTS, 128), 0)
    row16 = lax.broadcasted_iota(jnp.int32, (16, HEAD), 0)
    row_seq = lax.broadcasted_iota(jnp.int32, (16, HEAD), 0) // 4

    def start_out(g):
        write(g, kbuf, ko_hbm, kosem)
        write(g, vbuf, vo_hbm, vosem)

    def write(g, buf, hbm, sem):
        for i in range(4):
            rows = pl.ds(g * GROUP + i * part, part)
            pltpu.make_async_copy(buf.at[rows], hbm.at[rows], sem.at[g]).start()

    def one_group(g, _):
        rows = pl.ds(pl.multiple_of(g * GROUP, GROUP), GROUP)
        pltpu.make_async_copy(k_hbm.at[rows], kbuf.at[rows], ksem.at[g]).wait()

        @pl.when(g + 1 < groups)
        def _():
            start_in(g + 1, v_hbm, vbuf, vsem)

        @pl.when(g + 1 == groups)
        def _():
            pltpu.make_async_copy(wo_hbm, wo, wsem.at[3]).start()

        def put(new_s, buf):
            def one(i, _):
                b = g * GROUP + i
                length = lens_ref[b]
                base = pl.multiple_of((length // 16) * 16, 16)
                old = buf[b, pl.ds(base, 16), :]
                new = jnp.broadcast_to(new_s[pl.ds(b, 1), :].astype(BF16), (16, HEAD))
                buf[b, pl.ds(base, 16), :] = jnp.where(row16 == length - base, new, old)
                return 0
            lax.fori_loop(0, GROUP, one, 0, unroll=8)

        put(k_s, kbuf)

        @pl.when(g + 1 == groups)
        def _():
            start_out(groups - 2)
            write(g, kbuf, ko_hbm, kosem)

        for h in range(4):
            qg_s[pl.ds(h, GROUP, stride=4), :] = q_s[h, rows, :]
        qt_s[...] = qg_s[...].T.astype(BF16)
        qt = qt_s[...]
        zero = jnp.zeros_like(qt)
        top_half, low_half = None, None
        for p in range(GROUP // 2):
            b = g * GROUP + 2 * p
            rhs = jnp.concatenate([jnp.where(lane_seq == 2 * p, qt, zero), jnp.where(lane_seq == 2 * p + 1, qt, zero)], axis=0)
            t0 = dot(jnp.concatenate([kbuf[b, :SLOTS // 2], kbuf[b + 1, :SLOTS // 2]], axis=1), rhs)
            t1 = dot(jnp.concatenate([kbuf[b, SLOTS // 2:], kbuf[b + 1, SLOTS // 2:]], axis=1), rhs)
            top_half = t0 if top_half is None else top_half + t0
            low_half = t1 if low_half is None else low_half + t1
        sc_s[:SLOTS // 2] = top_half
        sc_s[SLOTS // 2:] = low_half
        live = slot_id <= ll_s[pl.ds(g, 1), :]
        scores = jnp.where(live, sc_s[...] * (HEAD ** -0.5), -jnp.inf)
        top = jnp.max(scores, axis=0, keepdims=True)
        exps = jnp.exp(scores - top)
        sc_s[...] = exps
        recip = 1.0 / jnp.sum(exps, axis=0, keepdims=True)
        for i in range(4):
            blk = sc_s[i * 128:(i + 1) * 128, :] * recip
            pt_s[:, i * 128:(i + 1) * 128] = blk.T.astype(BF16)

        pltpu.make_async_copy(v_hbm.at[rows], vbuf.at[rows], vsem.at[g]).wait()

        @pl.when(g + 2 < groups)
        def _():
            start_in(g + 2, k_hbm, kbuf, ksem)

        @pl.when(g + 2 == groups)
        def _():
            for i in range(groups - 2):
                start_out(i)

        put(v_s, vbuf)

        @pl.when(g + 1 == groups)
        def _():
            write(g, vbuf, vo_hbm, vosem)

        for j in range(GROUP // 4):
            b = g * GROUP + 4 * j
            probs = pt_s[16 * j:16 * j + 16, :]
            o = jnp.zeros((16, HEAD), F32)
            for i in range(0, 4, 2):
                out = dot(probs, jnp.concatenate([vbuf[b + i], vbuf[b + i + 1]], axis=1))
                o = jnp.where(row_seq == i, out[:, :HEAD], o)
                o = jnp.where(row_seq == i + 1, out[:, HEAD:], o)
            o_s[16 * j:16 * j + 16, :] = o
        for h in range(4):
            at_s[rows, h * HEAD:(h + 1) * HEAD] = o_s[pl.ds(h, GROUP, stride=4), :].astype(BF16)
        return 0

    lax.fori_loop(0, groups, one_group, 0)

    pltpu.make_async_copy(wo_hbm, wo, wsem.at[3]).wait()
    attn = at_s[...]
    for c in range(WIDTH // BLOCK):
        part_ref[c] = dot(attn, wo[:, c * BLOCK:(c + 1) * BLOCK]).astype(BF16)
    for g in range(groups):
        rows = pl.ds(g * GROUP, GROUP)
        pltpu.make_async_copy(kbuf.at[rows], ko_hbm.at[rows], kosem.at[g]).wait()
        pltpu.make_async_copy(vbuf.at[rows], vo_hbm.at[rows], vosem.at[g]).wait()


def tail_kernel(ff, vocab_loc,
                part_ref, x_hbm, gm_hbm, gf_hbm, tok_hbm, wg_hbm, wu_hbm, wd_hbm, wh_hbm,
                y_ref, logp_ref, lse_ref,
                x_ref, gm_ref, gf_ref, tok_ref, wbuf, r1, s1, r2, a_s, m_s, hid, p2, r1b, s2, r2b, y_s, f_s, tok2, st_s, st_r, late0, late1,
                wsem, s_d1, r_d1, s_x1, r_x1, s_a, r_a, s_d2, r_d2, s_x2, r_x2,
                s_y, r_y, s_o, r_o, s_f, r_f, s_t, r_t, s_st, r_st, insem):
    dp = lax.axis_index('dp')
    tp = lax.axis_index('tp')
    core = lax.rem(tp, 2)
    dev = dp * 4 + tp
    partner = (dp, tp + 1 - 2 * core)
    xnext = (dp, lax.rem(tp + 2, 4))
    ynext = (1 - dp, tp)
    mine = core * HALF
    other = (1 - core) * HALF

    mlp_tiles = [(i * TILE, min(TILE, ff - i * TILE)) for i in range(-(-ff // TILE))]
    n_mlp = len(mlp_tiles)
    tail_pad = -(-mlp_tiles[-1][1] // BLOCK) * BLOCK
    vocab_half = vocab_loc // 2
    n_full = vocab_half // TILE
    n_tail = vocab_half - n_full * TILE
    n_head = n_full + (1 if n_tail else 0)
    assert n_full % STEP == 0 and n_tail
    head0 = 3 * n_mlp
    vbase = dp * vocab_half

    def mlp_copy(i):
        if i < 2 * n_mlp:
            src, (r, n) = (wg_hbm, wu_hbm)[i % 2], mlp_tiles[i // 2]
        else:
            src, (r, n) = wd_hbm, mlp_tiles[i - 2 * n_mlp]
        slot = i % RING
        return pltpu.make_async_copy(src.at[pl.ds(r, n)], wbuf.at[slot, pl.ds(0, n)], wsem.at[slot])

    def head_copy(i, n=TILE):
        slot = lax.rem(head0 + i, RING)
        start = pl.multiple_of(vbase + i * TILE, 16)
        return pltpu.make_async_copy(wh_hbm.at[pl.ds(start, n)], wbuf.at[slot, pl.ds(0, n)], wsem.at[slot])

    def start_item(i):
        if i < head0:
            mlp_copy(i).start()
        elif i - head0 < n_full:
            head_copy(i - head0).start()
        elif i - head0 < n_head:
            head_copy(i - head0, n_tail).start()

    small = [pltpu.make_async_copy(src, dst, insem.at[i]) for i, (src, dst) in enumerate((
        (x_hbm, x_ref), (gm_hbm, gm_ref), (gf_hbm, gf_ref), (tok_hbm, tok_ref)))]
    for c in small:
        c.start()
    issued = [0]

    def issue(n, freed=0):
        for _ in range(n):
            if issued[0] < RING + freed:
                start_item(issued[0])
                issued[0] += 1

    issue(2)

    barrier = pltpu.get_barrier_semaphore()
    for d in range(2):
        for t in range(4):
            @pl.when(d * 4 + t != dev)
            def _():
                pl.semaphore_signal(barrier, inc=1, device_id=(d, t), device_id_type=MESH)
    last_n = mlp_tiles[-1][1]
    if tail_pad > last_n:
        for i in (2 * n_mlp - 2, 2 * n_mlp - 1, 3 * n_mlp - 1):
            wbuf[i % RING, last_n:tail_pad, :] = jnp.zeros((tail_pad - last_n, WIDTH), BF16)
    pl.semaphore_wait(barrier, 7)
    issue(2)

    def remote(src, dst, ssem, rsem, who):
        return pltpu.make_async_remote_copy(src_ref=src, dst_ref=dst, send_sem=ssem, recv_sem=rsem, device_id=who, device_id_type=MESH)

    tok_copy = remote(tok_ref, tok2, s_t, r_t, ynext)
    def part_of(ref, base, grp):
        return ref.at[pl.ds(base + grp[0], grp[1])]

    d1 = [remote(part_of(part_ref, other, p), part_of(r1, 0, p), s_d1.at[i], r_d1.at[i], partner) for i, p in enumerate(SUM1)]
    x1 = [remote(part_of(s1, 0, p), part_of(r2, 0, p), s_x1.at[i], r_x1.at[i], xnext) for i, p in enumerate(SUM1)]
    ac = [remote(part_of(a_s, mine, p), part_of(a_s, mine, p), s_a.at[i], r_a.at[i], partner) for i, p in enumerate(SUM1)]
    d2 = [remote(part_of(p2, other, p), part_of(r1b, 0, p), s_d2.at[i], r_d2.at[i], partner) for i, p in enumerate(SUM2)]
    x2 = [remote(part_of(s2, 0, p), part_of(r2b, 0, p), s_x2.at[i], r_x2.at[i], xnext) for i, p in enumerate(SUM2)]
    yo = [remote(part_of(y_s.at[0], mine, p), part_of(y_s.at[0], mine, p), s_o.at[i], r_o.at[i], partner) for i, p in enumerate(SUM2)]
    yy = [remote(part_of(y_s.at[0], mine, p), part_of(y_s.at[1], mine, p), s_y.at[i], r_y.at[i], ynext) for i, p in enumerate(SUM2)]
    yf = [remote(part_of(y_s.at[1], mine, p), part_of(y_s.at[1], mine, p), s_f.at[i], r_f.at[i], partner) for i, p in enumerate(SUM2)]

    def cols_of(c):
        return pl.ds(pl.multiple_of(c * CHUNK, CHUNK), CHUNK)

    for c in d1:
        c.start()
    for c in small:
        c.wait()
    tok_copy.start()
    for i, (first, n) in enumerate(SUM1):
        d1[i].wait_recv()
        for j in range(first, first + n):
            s1[j] = (part_ref[mine + j].astype(F32) + r1[j].astype(F32)).astype(BF16)
        x1[i].start()
    issue(2)
    for i, (first, n) in enumerate(SUM1):
        x1[i].wait_recv()
        issue(1 if i % 2 else 2)
        for j in range(first, first + n):
            total = s1[j].astype(F32) + r2[j].astype(F32)
            a_s[mine + j] = (x_ref[:, cols_of(mine + j)].astype(F32) + total).astype(BF16)
        ac[i].start()
    for c in ac:
        c.wait_recv()
    issue(1)

    def inv_rms(src):
        total = jnp.zeros((ROWS, CHUNK), F32)
        for c in range(NCH):
            v = src[c].astype(F32)
            total = total + v * v
        return lax.rsqrt(jnp.sum(total, axis=-1, keepdims=True) * (1.0 / WIDTH) + EPS)

    inv = inv_rms(a_s)
    gm = gm_ref[...].astype(F32).reshape(1, WIDTH)
    for c in range(NCH):
        cols = slice(c * CHUNK, (c + 1) * CHUNK)
        m_s[:, cols] = (a_s[c].astype(F32) * inv * gm[:, cols]).astype(BF16)

    for i in range(2 * n_mlp):
        mlp_copy(i).wait()
    for i, (r, n) in enumerate(mlp_tiles):
        gslot, uslot = (2 * i) % RING, (2 * i + 1) % RING
        pad = -(-n // BLOCK) * BLOCK
        for b in range(0, pad, BLOCK):
            gate = dot_t(wbuf[gslot, b:b + BLOCK, :], m_s[...])
            up = dot_t(wbuf[uslot, b:b + BLOCK, :], m_s[...])
            hid[:, r + b:r + b + BLOCK] = (gate * jax.nn.sigmoid(gate) * up).T.astype(BF16)
            issue(1, 2 * i)

    for i in range(n_mlp):
        mlp_copy(2 * n_mlp + i).wait()

    def down(c):
        acc = None
        for i, (r, n) in enumerate(mlp_tiles):
            pad = -(-n // BLOCK) * BLOCK
            term = dot(hid[:, r:r + pad], wbuf[(2 * n_mlp + i) % RING, :pad, cols_of(c)])
            acc = term if acc is None else acc + term
        return acc.astype(BF16)

    def chip_sum(i):
        d2[i].wait_recv()
        first, n = SUM2[i]
        for j in range(first, first + n):
            s2[j] = (p2[mine + j].astype(F32) + r1b[j].astype(F32)).astype(BF16)
        x2[i].start()

    for i, (first, n) in enumerate(SUM2):
        for j in range(first, first + n):
            theirs, ours = down(other + j), down(mine + j)
            p2[other + j] = theirs
            p2[mine + j] = ours
            issue(1, 2 * n_mlp)
        d2[i].start()
        if i:
            chip_sum(i - 1)
    chip_sum(len(SUM2) - 1)
    issue(1, 3 * n_mlp)

    def forward(i):
        yy[i].wait_recv()
        yf[i].start()

    for i, (first, n) in enumerate(SUM2):
        x2[i].wait_recv()
        issue(2, 3 * n_mlp)
        for j in range(first, first + n):
            total = s2[j].astype(F32) + r2b[j].astype(F32)
            y_s[0, mine + j] = (a_s[mine + j].astype(F32) + total).astype(BF16)
        yy[i].start()
        yo[i].start()
    for i in range(len(SUM2)):
        forward(i)
    for c in yo:
        c.wait_recv()
    issue(RING, 3 * n_mlp)
    for c in range(NCH):
        y_ref[:, c * CHUNK:(c + 1) * CHUNK] = y_s[0, c]

    gf = gf_ref[...].astype(F32).reshape(1, WIDTH)

    def final_norm(grp):
        inv = inv_rms(y_s.at[grp])
        for c in range(NCH):
            cols = slice(c * CHUNK, (c + 1) * CHUNK)
            f_s[grp * ROWS:(grp + 1) * ROWS, cols] = (y_s[grp, c].astype(F32) * inv * gf[:, cols]).astype(BF16)

    final_norm(0)
    for c in yf:
        c.wait_recv()
    final_norm(1)
    tok_copy.wait()

    tok = jnp.concatenate([tok_ref[...], tok2[...]], axis=1) - (tp * vocab_loc + vbase)
    row_id = lax.broadcasted_iota(jnp.int32, (8, 2 * ROWS), 0)

    def tally(logits, first, state):
        top, tot, tgt = state
        blocks = [logits[8 * i:8 * i + 8] for i in range(logits.shape[0] // 8)]
        peak = blocks[0]
        for v in blocks[1:]:
            peak = jnp.maximum(peak, v)
        new = jnp.maximum(top, peak)
        part_sum = None
        for i, v in enumerate(blocks):
            e = jnp.exp(v - new)
            part_sum = e if part_sum is None else part_sum + e
            tgt = jnp.where(row_id + (first + 8 * i) == tok, v, tgt)
        tot = tot * jnp.exp(top - new) + part_sum
        return new, tot, tgt

    def late(k, state):
        end = (k + 1) * STEP * TILE
        for i, ref in enumerate((late0, late1)):
            state = tally(ref[...], jnp.where(k < 0, -(2 ** 30), end - (2 - i) * BLOCK), state)
        return state

    def some_tiles(k, state):
        for t in range(STEP):
            head_copy(k * STEP + t).wait()
        state = late(k - 1, state)
        todo = [(t, b) for t in range(STEP) for b in range(0, TILE, BLOCK)]
        for n, (t, b) in enumerate(todo):
            i = k * STEP + t
            logits = dot_t(wbuf[lax.rem(head0 + i, RING), pl.ds(b, BLOCK), :], f_s[...])
            if n < len(todo) - 2:
                state = tally(logits, i * TILE + b, state)
            elif n == len(todo) - 2:
                late0[...] = logits
            else:
                late1[...] = logits
        for t in range(STEP):
            i = k * STEP + t

            @pl.when(i + RING < n_full)
            def _():
                head_copy(i + RING).start()

            @pl.when(i + RING == n_full)
            def _():
                head_copy(n_full, n_tail).start()
        return state

    late0[...] = jnp.full(late0.shape, -1e30, F32)
    late1[...] = jnp.full(late1.shape, -1e30, F32)
    state = (jnp.full((8, 2 * ROWS), -1e30, F32), jnp.zeros((8, 2 * ROWS), F32), jnp.zeros((8, 2 * ROWS), F32))
    state = lax.fori_loop(0, n_full // STEP, some_tiles, state)
    head_copy(n_full, n_tail).wait()
    cut = -(-n_tail // 32) * 16
    state = late(n_full // STEP - 1, state)
    for b, size in ((0, cut), (cut, n_tail - cut)):
        logits = dot_t(wbuf[(head0 + n_full) % RING, pl.ds(b, size), :], f_s[...])
        state = tally(logits, n_full * TILE + b, state)
    top, tot, tgt = state
    peak = jnp.max(top, axis=0, keepdims=True)
    tot = jnp.sum(tot * jnp.exp(top - peak), axis=0, keepdims=True)
    tgt = jnp.sum(tgt, axis=0, keepdims=True)
    pad = jnp.zeros((5, ROWS), F32)
    for g in range(2):
        cols = slice(g * ROWS, (g + 1) * ROWS)
        st_s[g] = jnp.concatenate([peak[:, cols], tot[:, cols], tgt[:, cols], pad], axis=0)

    sends = []
    for k in range(1, 8):
        who = lax.rem(dev + k, 8)
        whod, whot = who // 4, lax.rem(who, 4)
        grp = lax.rem(whod + dp, 2)
        sends.append(remote(st_s.at[grp], st_r.at[dev], s_st.at[k - 1], r_st.at[k - 1], (whod, whot)))
    for c in sends:
        c.start()
    st_r[dev] = st_s[0]
    for c in sends:
        c.wait()
    stats = [st_r[i] for i in range(8)]
    peak = stats[0][0:1]
    for s in stats[1:]:
        peak = jnp.maximum(peak, s[0:1])
    tot = jnp.zeros_like(peak)
    tgt = jnp.zeros_like(peak)
    for s in stats:
        tot = tot + s[1:2] * jnp.exp(s[0:1] - peak)
        tgt = tgt + s[2:3]
    lse = peak + jnp.log(tot)
    lse_ref[...] = lse
    logp_ref[...] = tgt - lse

    for group in (d1, x1, ac, d2, x2, yo, yy, yf):
        for c in group:
            c.wait_send()


def emit_kernel(y_in, logp_in, lse_in, y_out, logp_out, lse_out, sem):
    copies = [pltpu.make_async_copy(src, dst, sem.at[i]) for i, (src, dst) in enumerate(((y_in, y_out), (logp_in, logp_out), (lse_in, lse_out)))]
    for c in copies:
        c.start()
    for c in copies:
        c.wait()


def local_step(tok_hidden, seq_lens, k_cache, v_cache, next_tok, g_attn, w_q, b_q, w_k, b_k, w_v, b_v, w_o, g_mlp, w_gate, w_up, w_down, g_final, w_head):
    steps = np.arange(HEAD // 2, dtype=np.float32) * np.float32(-2.0 / HEAD)
    freq = jnp.asarray(np.tile(np.power(np.float64(THETA), steps.astype(np.float64)).astype(np.float32), 2)[None])
    vm = pl.BlockSpec(memory_space=pltpu.VMEM)
    sm = pl.BlockSpec(memory_space=pltpu.SMEM)
    hb = pl.BlockSpec(memory_space=pltpu.HBM)
    dma = pltpu.SemaphoreType.DMA
    cache = jax.ShapeDtypeStruct((ROWS, SLOTS, HEAD), BF16)
    part, k_all, v_all = pl.pallas_call(
        attn_kernel,
        out_shape=(pltpu.VMEM((NCH, ROWS, CHUNK), BF16), cache, cache),
        in_specs=[sm] + [hb] * 13,
        out_specs=(vm, hb, hb),
        scratch_shapes=[
            pltpu.VMEM((1, ROWS), jnp.int32), pltpu.VMEM((1, HEAD), F32), pltpu.VMEM((ROWS, WIDTH), BF16), pltpu.VMEM((WIDTH,), BF16),
            pltpu.VMEM((4 * HEAD,), BF16), pltpu.VMEM((HEAD,), BF16), pltpu.VMEM((HEAD,), BF16),
            pltpu.VMEM((ROWS, SLOTS, HEAD), BF16), pltpu.VMEM((ROWS, SLOTS, HEAD), BF16),
            pltpu.VMEM((WIDTH, 512), BF16), pltpu.VMEM((WIDTH, HEAD), BF16), pltpu.VMEM((WIDTH, HEAD), BF16), pltpu.VMEM((512, WIDTH), BF16),
            pltpu.VMEM((4, ROWS, HEAD), F32), pltpu.VMEM((ROWS, HEAD), F32), pltpu.VMEM((ROWS, HEAD), F32),
            pltpu.VMEM((128, HEAD), F32), pltpu.VMEM((HEAD, 128), BF16), pltpu.VMEM((SLOTS, 128), F32), pltpu.VMEM((128, SLOTS), BF16),
            pltpu.VMEM((128, HEAD), F32), pltpu.VMEM((ROWS, 512), BF16), pltpu.VMEM((8, 128), jnp.int32),
            dma((4,)), dma((4,)), dma((4,)), dma((4,)), dma((4,)), dma((7,)),
        ],
        compiler_params=pltpu.CompilerParams(vmem_limit_bytes=ATTN_BYTES),
        name="attention",
    )(seq_lens, seq_lens.reshape(1, ROWS), freq, tok_hidden, g_attn, b_q, b_k, b_v,
      w_q, w_k, w_v, w_o, k_cache.reshape(ROWS, SLOTS, HEAD), v_cache.reshape(ROWS, SLOTS, HEAD))

    ff = w_gate.shape[1]
    vocab_loc = w_head.shape[0]
    ff_pad = -(-ff // BLOCK) * BLOCK
    chunk4 = pltpu.VMEM((HALF, ROWS, CHUNK), BF16)
    chunk8 = pltpu.VMEM((NCH, ROWS, CHUNK), BF16)

    def kernel(*refs):
        tail_kernel(ff, vocab_loc, *refs)

    y_out, logp, lse = pl.pallas_call(
        kernel,
        out_shape=(pltpu.VMEM((ROWS, WIDTH), BF16), pltpu.VMEM((1, ROWS), F32), pltpu.VMEM((1, ROWS), F32)),
        in_specs=[vm] + [hb] * 8,
        out_specs=(vm, vm, vm),
        scratch_shapes=[
            pltpu.VMEM((ROWS, WIDTH), BF16), pltpu.VMEM((WIDTH,), BF16), pltpu.VMEM((WIDTH,), BF16), pltpu.VMEM((1, ROWS), jnp.int32),
            pltpu.VMEM((RING, TILE, WIDTH), BF16),
            chunk4, chunk4, chunk4, chunk8, pltpu.VMEM((ROWS, WIDTH), BF16), pltpu.VMEM((ROWS, ff_pad), BF16),
            chunk8, chunk4, chunk4, chunk4, pltpu.VMEM((2, NCH, ROWS, CHUNK), BF16), pltpu.VMEM((2 * ROWS, WIDTH), BF16),
            pltpu.VMEM((1, ROWS), jnp.int32), pltpu.VMEM((2, 8, ROWS), F32), pltpu.VMEM((8, 8, ROWS), F32),
            pltpu.VMEM((BLOCK, 2 * ROWS), F32), pltpu.VMEM((BLOCK, 2 * ROWS), F32),
            dma((RING,)),
        ] + [dma((HALF,))] * 16 + [dma, dma, dma((7,)), dma((7,)), dma((4,))],
        compiler_params=pltpu.CompilerParams(vmem_limit_bytes=TAIL_BYTES, collective_id=0, has_side_effects=True),
        name="tail",
    )(pltpu.with_memory_space_constraint(part, pltpu.VMEM), tok_hidden, g_mlp, g_final, next_tok.reshape(1, ROWS), w_gate.T, w_up.T, w_down, w_head)
    vec = jax.ShapeDtypeStruct((1, ROWS), F32)
    y_out, logp, lse = pl.pallas_call(
        emit_kernel,
        out_shape=(jax.ShapeDtypeStruct((ROWS, WIDTH), BF16), vec, vec),
        in_specs=[vm] * 3,
        out_specs=(hb, hb, hb),
        scratch_shapes=[dma((3,))],
        name="emit",
    )(*(pltpu.with_memory_space_constraint(v, pltpu.VMEM) for v in (y_out, logp, lse)))
    shape = (ROWS, SLOTS, 1, HEAD)
    return y_out, k_all.reshape(shape), v_all.reshape(shape), logp.reshape(ROWS), lse.reshape(ROWS)


def solution(mesh):
    row_spec = P('dp', None)
    vec_spec = P('dp')
    cache_spec = P('dp', None, 'tp', None)
    col_spec = P(None, 'tp')
    part_spec = P('tp')
    whole_spec = P(None)
    in_specs = (row_spec, vec_spec, cache_spec, cache_spec, vec_spec, whole_spec, col_spec, part_spec, col_spec, part_spec, col_spec, part_spec, P('tp', None), whole_spec, col_spec, col_spec, P('tp', None), whole_spec, P('tp', None))
    out_specs = (row_spec, cache_spec, cache_spec, vec_spec, vec_spec)
    return jax.shard_map(local_step, mesh=mesh, in_specs=in_specs, out_specs=out_specs, check_vma=False)
```

```python
import jax
import numpy as np
import jax.numpy as jnp
from jax import lax
from jax.experimental import pallas as pl
from jax.experimental.pallas import tpu as pltpu
from jax.sharding import PartitionSpec as P

THETA = 1000000.0
EPS = 1e-6
MESH = pl.DeviceIdType.MESH
F32 = jnp.float32
BF16 = jnp.bfloat16
ATTN_BYTES = 62 * 2 ** 20
TAIL_BYTES = 65500000

ROWS = 128
WIDTH = 2048
HEAD = 128
SLOTS = 512
GROUP = 32
CHUNK = 256
NCH = 8
HALF = 4
BLOCK = 256
SUM1 = ((0, 1), (1, 1), (2, 1), (3, 1))
SUM2 = ((0, 1), (1, 1), (2, 1), (3, 1))
TILE = 768
RING = 18
STEP = 4


def dot(a, b):
    return lax.dot_general(a, b, (((1,), (0,)), ((), ())), preferred_element_type=F32)


def dot_t(a, b):
    return lax.dot_general(a, b, (((1,), (1,)), ((), ())), preferred_element_type=F32)


def attn_kernel(lens_ref, lenv_hbm, freq_hbm, x_hbm, g_hbm, bq_hbm, bk_hbm, bv_hbm,
                wq_hbm, wk_hbm, wv_hbm, wo_hbm, k_hbm, v_hbm,
                part_ref, ko_hbm, vo_hbm,
                lenv_ref, freq_ref, x_ref, g_ref, bq_ref, bk_ref, bv_ref,
                kbuf, vbuf, wq, wk, wv, wo, q_s, k_s, v_s, qg_s, qt_s, sc_s, pt_s, o_s, at_s, ll_s,
                wsem, ksem, vsem, kosem, vosem, insem):
    groups = ROWS // GROUP
    part = GROUP // 4
    small = [pltpu.make_async_copy(src, dst, insem.at[i]) for i, (src, dst) in enumerate((
        (x_hbm, x_ref), (lenv_hbm, lenv_ref), (freq_hbm, freq_ref), (g_hbm, g_ref), (bq_hbm, bq_ref), (bk_hbm, bk_ref), (bv_hbm, bv_ref)))]
    for c in small:
        c.start()
    for i, (src, dst) in enumerate(((wq_hbm, wq), (wk_hbm, wk), (wv_hbm, wv))):
        pltpu.make_async_copy(src, dst, wsem.at[i]).start()

    def start_in(g, hbm, buf, sem, lo=0, hi=4):
        for i in range(lo, hi):
            rows = pl.ds(g * GROUP + i * part, part)
            pltpu.make_async_copy(hbm.at[rows], buf.at[rows], sem.at[g]).start()

    start_in(0, k_hbm, kbuf, ksem, 0, 2)
    for c in small:
        c.wait()
    start_in(0, k_hbm, kbuf, ksem, 2, 4)
    start_in(0, v_hbm, vbuf, vsem)
    len_rows = jnp.broadcast_to(lenv_ref[...].astype(F32), (ROWS, ROWS)).T
    angles = len_rows * freq_ref[...]
    cos = jnp.cos(angles)
    sin = jnp.sin(angles) * jnp.where(lax.broadcasted_iota(jnp.int32, (ROWS, HEAD), 1) < HEAD // 2, -1.0, 1.0)
    seq_of = lax.broadcasted_iota(jnp.int32, (GROUP, 128), 1) // 4
    pick = lax.broadcasted_iota(jnp.int32, (GROUP, 128), 0) == seq_of
    for g in range(groups):
        ll_s[g:g + 1, :] = jnp.sum(jnp.where(pick, len_rows[g * GROUP:(g + 1) * GROUP], 0.0), axis=0, keepdims=True).astype(jnp.int32)

    x = x_ref[...].astype(F32)
    inv = lax.rsqrt(jnp.mean(x * x, axis=-1, keepdims=True) + EPS)
    normed = (x * inv * g_ref[...].astype(F32).reshape(1, WIDTH)).astype(BF16)
    for i, (src, dst) in enumerate(((wq_hbm, wq), (wk_hbm, wk), (wv_hbm, wv))):
        pltpu.make_async_copy(src, dst, wsem.at[i]).wait()

    start_in(1, k_hbm, kbuf, ksem)

    def rope(u):
        return u * cos + pltpu.roll(u, HEAD // 2, 1) * sin

    k_s[...] = rope(dot(normed, wk[...]) + bk_ref[...].astype(F32).reshape(1, HEAD))
    v_s[...] = dot(normed, wv[...]) + bv_ref[...].astype(F32).reshape(1, HEAD)
    q_all = dot(normed, wq[...]) + bq_ref[...].astype(F32).reshape(1, 4 * HEAD)
    for h in range(4):
        q_s[h] = rope(q_all[:, h * HEAD:(h + 1) * HEAD])

    lane_seq = lax.broadcasted_iota(jnp.int32, (HEAD, 128), 1) // 4
    slot_id = lax.broadcasted_iota(jnp.int32, (SLOTS, 128), 0)
    row16 = lax.broadcasted_iota(jnp.int32, (16, HEAD), 0)
    row_seq = lax.broadcasted_iota(jnp.int32, (16, HEAD), 0) // 4

    def start_out(g):
        write(g, kbuf, ko_hbm, kosem)
        write(g, vbuf, vo_hbm, vosem)

    def write(g, buf, hbm, sem):
        for i in range(4):
            rows = pl.ds(g * GROUP + i * part, part)
            pltpu.make_async_copy(buf.at[rows], hbm.at[rows], sem.at[g]).start()

    def one_group(g, _):
        rows = pl.ds(pl.multiple_of(g * GROUP, GROUP), GROUP)
        pltpu.make_async_copy(k_hbm.at[rows], kbuf.at[rows], ksem.at[g]).wait()

        @pl.when(g + 1 < groups)
        def _():
            start_in(g + 1, v_hbm, vbuf, vsem)

        @pl.when(g + 1 == groups)
        def _():
            pltpu.make_async_copy(wo_hbm, wo, wsem.at[3]).start()

        def put(new_s, buf):
            def one(i, _):
                b = g * GROUP + i
                length = lens_ref[b]
                base = pl.multiple_of((length // 16) * 16, 16)
                old = buf[b, pl.ds(base, 16), :]
                new = jnp.broadcast_to(new_s[pl.ds(b, 1), :].astype(BF16), (16, HEAD))
                buf[b, pl.ds(base, 16), :] = jnp.where(row16 == length - base, new, old)
                return 0
            lax.fori_loop(0, GROUP, one, 0, unroll=8)

        put(k_s, kbuf)

        @pl.when(g + 1 == groups)
        def _():
            start_out(groups - 2)
            write(g, kbuf, ko_hbm, kosem)

        for h in range(4):
            qg_s[pl.ds(h, GROUP, stride=4), :] = q_s[h, rows, :]
        qt_s[...] = qg_s[...].T.astype(BF16)
        qt = qt_s[...]
        zero = jnp.zeros_like(qt)
        top_half, low_half = None, None
        for p in range(GROUP // 2):
            b = g * GROUP + 2 * p
            rhs = jnp.concatenate([jnp.where(lane_seq == 2 * p, qt, zero), jnp.where(lane_seq == 2 * p + 1, qt, zero)], axis=0)
            t0 = dot(jnp.concatenate([kbuf[b, :SLOTS // 2], kbuf[b + 1, :SLOTS // 2]], axis=1), rhs)
            t1 = dot(jnp.concatenate([kbuf[b, SLOTS // 2:], kbuf[b + 1, SLOTS // 2:]], axis=1), rhs)
            top_half = t0 if top_half is None else top_half + t0
            low_half = t1 if low_half is None else low_half + t1
        sc_s[:SLOTS // 2] = top_half
        sc_s[SLOTS // 2:] = low_half
        live = slot_id <= ll_s[pl.ds(g, 1), :]
        scores = jnp.where(live, sc_s[...] * (HEAD ** -0.5), -jnp.inf)
        top = jnp.max(scores, axis=0, keepdims=True)
        exps = jnp.exp(scores - top)
        sc_s[...] = exps
        recip = 1.0 / jnp.sum(exps, axis=0, keepdims=True)
        for i in range(4):
            blk = sc_s[i * 128:(i + 1) * 128, :] * recip
            pt_s[:, i * 128:(i + 1) * 128] = blk.T.astype(BF16)

        pltpu.make_async_copy(v_hbm.at[rows], vbuf.at[rows], vsem.at[g]).wait()

        @pl.when(g + 2 < groups)
        def _():
            start_in(g + 2, k_hbm, kbuf, ksem)

        @pl.when(g + 2 == groups)
        def _():
            for i in range(groups - 2):
                start_out(i)

        put(v_s, vbuf)

        @pl.when(g + 1 == groups)
        def _():
            write(g, vbuf, vo_hbm, vosem)

        for j in range(GROUP // 4):
            b = g * GROUP + 4 * j
            probs = pt_s[16 * j:16 * j + 16, :]
            o = jnp.zeros((16, HEAD), F32)
            for i in range(0, 4, 2):
                out = dot(probs, jnp.concatenate([vbuf[b + i], vbuf[b + i + 1]], axis=1))
                o = jnp.where(row_seq == i, out[:, :HEAD], o)
                o = jnp.where(row_seq == i + 1, out[:, HEAD:], o)
            o_s[16 * j:16 * j + 16, :] = o
        for h in range(4):
            at_s[rows, h * HEAD:(h + 1) * HEAD] = o_s[pl.ds(h, GROUP, stride=4), :].astype(BF16)
        return 0

    lax.fori_loop(0, groups, one_group, 0)

    pltpu.make_async_copy(wo_hbm, wo, wsem.at[3]).wait()
    attn = at_s[...]
    for c in range(WIDTH // BLOCK):
        part_ref[c] = dot(attn, wo[:, c * BLOCK:(c + 1) * BLOCK]).astype(BF16)
    for g in range(groups):
        rows = pl.ds(g * GROUP, GROUP)
        pltpu.make_async_copy(kbuf.at[rows], ko_hbm.at[rows], kosem.at[g]).wait()
        pltpu.make_async_copy(vbuf.at[rows], vo_hbm.at[rows], vosem.at[g]).wait()


def tail_kernel(ff, vocab_loc,
                part_ref, x_hbm, gm_hbm, gf_hbm, tok_hbm, wg_hbm, wu_hbm, wd_hbm, wh_hbm,
                y_ref, logp_ref, lse_ref,
                x_ref, gm_ref, gf_ref, tok_ref, wbuf, r1, s1, r2, a_s, m_s, hid, p2, r1b, s2, r2b, y_s, f_s, tok2, st_s, st_r, late0, late1,
                wsem, s_d1, r_d1, s_x1, r_x1, s_a, r_a, s_d2, r_d2, s_x2, r_x2,
                s_y, r_y, s_o, r_o, s_f, r_f, s_t, r_t, s_st, r_st, insem):
    dp = lax.axis_index('dp')
    tp = lax.axis_index('tp')
    core = lax.rem(tp, 2)
    dev = dp * 4 + tp
    partner = (dp, tp + 1 - 2 * core)
    xnext = (dp, lax.rem(tp + 2, 4))
    ynext = (1 - dp, tp)
    mine = core * HALF
    other = (1 - core) * HALF

    mlp_tiles = [(i * TILE, min(TILE, ff - i * TILE)) for i in range(-(-ff // TILE))]
    n_mlp = len(mlp_tiles)
    tail_pad = -(-mlp_tiles[-1][1] // BLOCK) * BLOCK
    vocab_half = vocab_loc // 2
    n_full = vocab_half // TILE
    n_tail = vocab_half - n_full * TILE
    n_head = n_full + (1 if n_tail else 0)
    assert n_full % STEP == 0 and n_tail
    head0 = 3 * n_mlp
    vbase = dp * vocab_half

    def mlp_copy(i):
        if i < 2 * n_mlp:
            src, (r, n) = (wg_hbm, wu_hbm)[i % 2], mlp_tiles[i // 2]
        else:
            src, (r, n) = wd_hbm, mlp_tiles[i - 2 * n_mlp]
        slot = i % RING
        return pltpu.make_async_copy(src.at[pl.ds(r, n)], wbuf.at[slot, pl.ds(0, n)], wsem.at[slot])

    def head_copy(i, n=TILE):
        slot = lax.rem(head0 + i, RING)
        start = pl.multiple_of(vbase + i * TILE, 16)
        return pltpu.make_async_copy(wh_hbm.at[pl.ds(start, n)], wbuf.at[slot, pl.ds(0, n)], wsem.at[slot])

    def start_item(i):
        if i < head0:
            mlp_copy(i).start()
        elif i - head0 < n_full:
            head_copy(i - head0).start()
        elif i - head0 < n_head:
            head_copy(i - head0, n_tail).start()

    small = [pltpu.make_async_copy(src, dst, insem.at[i]) for i, (src, dst) in enumerate((
        (x_hbm, x_ref), (gm_hbm, gm_ref), (gf_hbm, gf_ref), (tok_hbm, tok_ref)))]
    for c in small:
        c.start()
    issued = [0]

    def issue(n, freed=0):
        for _ in range(n):
            if issued[0] < RING + freed:
                start_item(issued[0])
                issued[0] += 1

    issue(2)

    barrier = pltpu.get_barrier_semaphore()
    for d in range(2):
        for t in range(4):
            @pl.when(d * 4 + t != dev)
            def _():
                pl.semaphore_signal(barrier, inc=1, device_id=(d, t), device_id_type=MESH)
    last_n = mlp_tiles[-1][1]
    if tail_pad > last_n:
        for i in (2 * n_mlp - 2, 2 * n_mlp - 1, 3 * n_mlp - 1):
            wbuf[i % RING, last_n:tail_pad, :] = jnp.zeros((tail_pad - last_n, WIDTH), BF16)
    pl.semaphore_wait(barrier, 7)
    issue(2)

    def remote(src, dst, ssem, rsem, who):
        return pltpu.make_async_remote_copy(src_ref=src, dst_ref=dst, send_sem=ssem, recv_sem=rsem, device_id=who, device_id_type=MESH)

    tok_copy = remote(tok_ref, tok2, s_t, r_t, ynext)
    def part_of(ref, base, grp):
        return ref.at[pl.ds(base + grp[0], grp[1])]

    d1 = [remote(part_of(part_ref, other, p), part_of(r1, 0, p), s_d1.at[i], r_d1.at[i], partner) for i, p in enumerate(SUM1)]
    x1 = [remote(part_of(s1, 0, p), part_of(r2, 0, p), s_x1.at[i], r_x1.at[i], xnext) for i, p in enumerate(SUM1)]
    ac = [remote(part_of(a_s, mine, p), part_of(a_s, mine, p), s_a.at[i], r_a.at[i], partner) for i, p in enumerate(SUM1)]
    d2 = [remote(part_of(p2, other, p), part_of(r1b, 0, p), s_d2.at[i], r_d2.at[i], partner) for i, p in enumerate(SUM2)]
    x2 = [remote(part_of(s2, 0, p), part_of(r2b, 0, p), s_x2.at[i], r_x2.at[i], xnext) for i, p in enumerate(SUM2)]
    yo = [remote(part_of(y_s.at[0], mine, p), part_of(y_s.at[0], mine, p), s_o.at[i], r_o.at[i], partner) for i, p in enumerate(SUM2)]
    yy = [remote(part_of(y_s.at[0], mine, p), part_of(y_s.at[1], mine, p), s_y.at[i], r_y.at[i], ynext) for i, p in enumerate(SUM2)]
    yf = [remote(part_of(y_s.at[1], mine, p), part_of(y_s.at[1], mine, p), s_f.at[i], r_f.at[i], partner) for i, p in enumerate(SUM2)]

    def cols_of(c):
        return pl.ds(pl.multiple_of(c * CHUNK, CHUNK), CHUNK)

    for c in d1:
        c.start()
    for c in small:
        c.wait()
    tok_copy.start()
    for i, (first, n) in enumerate(SUM1):
        d1[i].wait_recv()
        for j in range(first, first + n):
            s1[j] = (part_ref[mine + j].astype(F32) + r1[j].astype(F32)).astype(BF16)
        x1[i].start()
    issue(2)
    for i, (first, n) in enumerate(SUM1):
        x1[i].wait_recv()
        issue(1 if i % 2 else 2)
        for j in range(first, first + n):
            total = s1[j].astype(F32) + r2[j].astype(F32)
            a_s[mine + j] = (x_ref[:, cols_of(mine + j)].astype(F32) + total).astype(BF16)
        ac[i].start()
    for c in ac:
        c.wait_recv()
    issue(1)

    def inv_rms(src):
        total = jnp.zeros((ROWS, CHUNK), F32)
        for c in range(NCH):
            v = src[c].astype(F32)
            total = total + v * v
        return lax.rsqrt(jnp.sum(total, axis=-1, keepdims=True) * (1.0 / WIDTH) + EPS)

    inv = inv_rms(a_s)
    gm = gm_ref[...].astype(F32).reshape(1, WIDTH)
    for c in range(NCH):
        cols = slice(c * CHUNK, (c + 1) * CHUNK)
        m_s[:, cols] = (a_s[c].astype(F32) * inv * gm[:, cols]).astype(BF16)

    for i in range(2 * n_mlp):
        mlp_copy(i).wait()
    for i, (r, n) in enumerate(mlp_tiles):
        gslot, uslot = (2 * i) % RING, (2 * i + 1) % RING
        pad = -(-n // BLOCK) * BLOCK
        for b in range(0, pad, BLOCK):
            gate = dot_t(wbuf[gslot, b:b + BLOCK, :], m_s[...])
            up = dot_t(wbuf[uslot, b:b + BLOCK, :], m_s[...])
            hid[:, r + b:r + b + BLOCK] = (gate * jax.nn.sigmoid(gate) * up).T.astype(BF16)
            issue(1, 2 * i)

    for i in range(n_mlp):
        mlp_copy(2 * n_mlp + i).wait()

    def down(c):
        acc = None
        for i, (r, n) in enumerate(mlp_tiles):
            pad = -(-n // BLOCK) * BLOCK
            term = dot(hid[:, r:r + pad], wbuf[(2 * n_mlp + i) % RING, :pad, cols_of(c)])
            acc = term if acc is None else acc + term
        return acc.astype(BF16)

    def chip_sum(i):
        d2[i].wait_recv()
        first, n = SUM2[i]
        for j in range(first, first + n):
            s2[j] = (p2[mine + j].astype(F32) + r1b[j].astype(F32)).astype(BF16)
        x2[i].start()

    for i, (first, n) in enumerate(SUM2):
        for j in range(first, first + n):
            theirs, ours = down(other + j), down(mine + j)
            p2[other + j] = theirs
            p2[mine + j] = ours
            issue(1, 2 * n_mlp)
        d2[i].start()
        if i:
            chip_sum(i - 1)
    chip_sum(len(SUM2) - 1)
    issue(1, 3 * n_mlp)

    last = len(SUM2) - 1
    straight = remote(part_of(y_s.at[0], mine, SUM2[last]), part_of(y_s.at[1], mine, SUM2[last]), s_f.at[last], r_f.at[last], (1 - dp, tp + 1 - 2 * core))

    def forward(i):
        yy[i].wait_recv()
        if i < last:
            yf[i].start()
        else:
            @pl.when(core == 1)
            def _():
                yf[i].start()

    for i, (first, n) in enumerate(SUM2):
        x2[i].wait_recv()
        issue(2, 3 * n_mlp)
        for j in range(first, first + n):
            total = s2[j].astype(F32) + r2b[j].astype(F32)
            y_s[0, mine + j] = (a_s[mine + j].astype(F32) + total).astype(BF16)
        yy[i].start()
        if i == last:
            @pl.when(core == 0)
            def _():
                straight.start()
        yo[i].start()
    for i in range(len(SUM2)):
        forward(i)
    for c in yo:
        c.wait_recv()
    issue(RING, 3 * n_mlp)
    for c in range(NCH):
        y_ref[:, c * CHUNK:(c + 1) * CHUNK] = y_s[0, c]

    gf = gf_ref[...].astype(F32).reshape(1, WIDTH)

    def final_norm(grp):
        inv = inv_rms(y_s.at[grp])
        for c in range(NCH):
            cols = slice(c * CHUNK, (c + 1) * CHUNK)
            f_s[grp * ROWS:(grp + 1) * ROWS, cols] = (y_s[grp, c].astype(F32) * inv * gf[:, cols]).astype(BF16)

    final_norm(0)
    for c in yf:
        c.wait_recv()
    final_norm(1)
    tok_copy.wait()

    tok = jnp.concatenate([tok_ref[...], tok2[...]], axis=1) - (tp * vocab_loc + vbase)
    row_id = lax.broadcasted_iota(jnp.int32, (8, 2 * ROWS), 0)

    def tally(logits, first, state):
        top, tot, tgt = state
        blocks = [logits[8 * i:8 * i + 8] for i in range(logits.shape[0] // 8)]
        peak = blocks[0]
        for v in blocks[1:]:
            peak = jnp.maximum(peak, v)
        new = jnp.maximum(top, peak)
        part_sum = None
        for i, v in enumerate(blocks):
            e = jnp.exp(v - new)
            part_sum = e if part_sum is None else part_sum + e
            tgt = jnp.where(row_id + (first + 8 * i) == tok, v, tgt)
        tot = tot * jnp.exp(top - new) + part_sum
        return new, tot, tgt

    def late(k, state):
        end = (k + 1) * STEP * TILE
        for i, ref in enumerate((late0, late1)):
            state = tally(ref[...], jnp.where(k < 0, -(2 ** 30), end - (2 - i) * BLOCK), state)
        return state

    def some_tiles(k, state):
        for t in range(STEP):
            head_copy(k * STEP + t).wait()
        state = late(k - 1, state)
        todo = [(t, b) for t in range(STEP) for b in range(0, TILE, BLOCK)]
        for n, (t, b) in enumerate(todo):
            i = k * STEP + t
            logits = dot_t(wbuf[lax.rem(head0 + i, RING), pl.ds(b, BLOCK), :], f_s[...])
            if n < len(todo) - 2:
                state = tally(logits, i * TILE + b, state)
            elif n == len(todo) - 2:
                late0[...] = logits
            else:
                late1[...] = logits
        for t in range(STEP):
            i = k * STEP + t

            @pl.when(i + RING < n_full)
            def _():
                head_copy(i + RING).start()

            @pl.when(i + RING == n_full)
            def _():
                head_copy(n_full, n_tail).start()
        return state

    late0[...] = jnp.full(late0.shape, -1e30, F32)
    late1[...] = jnp.full(late1.shape, -1e30, F32)
    state = (jnp.full((8, 2 * ROWS), -1e30, F32), jnp.zeros((8, 2 * ROWS), F32), jnp.zeros((8, 2 * ROWS), F32))
    state = lax.fori_loop(0, n_full // STEP, some_tiles, state)
    head_copy(n_full, n_tail).wait()
    cut = -(-n_tail // 32) * 16
    state = late(n_full // STEP - 1, state)
    for b, size in ((0, cut), (cut, n_tail - cut)):
        logits = dot_t(wbuf[(head0 + n_full) % RING, pl.ds(b, size), :], f_s[...])
        state = tally(logits, n_full * TILE + b, state)
    top, tot, tgt = state
    peak = jnp.max(top, axis=0, keepdims=True)
    tot = jnp.sum(tot * jnp.exp(top - peak), axis=0, keepdims=True)
    tgt = jnp.sum(tgt, axis=0, keepdims=True)
    pad = jnp.zeros((5, ROWS), F32)
    for g in range(2):
        cols = slice(g * ROWS, (g + 1) * ROWS)
        st_s[g] = jnp.concatenate([peak[:, cols], tot[:, cols], tgt[:, cols], pad], axis=0)

    sends = []
    for k in range(1, 8):
        who = lax.rem(dev + k, 8)
        whod, whot = who // 4, lax.rem(who, 4)
        grp = lax.rem(whod + dp, 2)
        sends.append(remote(st_s.at[grp], st_r.at[dev], s_st.at[k - 1], r_st.at[k - 1], (whod, whot)))
    for c in sends:
        c.start()
    st_r[dev] = st_s[0]
    for c in sends:
        c.wait()
    stats = [st_r[i] for i in range(8)]
    peak = stats[0][0:1]
    for s in stats[1:]:
        peak = jnp.maximum(peak, s[0:1])
    tot = jnp.zeros_like(peak)
    tgt = jnp.zeros_like(peak)
    for s in stats:
        tot = tot + s[1:2] * jnp.exp(s[0:1] - peak)
        tgt = tgt + s[2:3]
    lse = peak + jnp.log(tot)
    lse_ref[...] = lse
    logp_ref[...] = tgt - lse

    for group in (d1, x1, ac, d2, x2, yo, yy, yf):
        for c in group:
            c.wait_send()


def emit_kernel(y_in, logp_in, lse_in, y_out, logp_out, lse_out, sem):
    copies = [pltpu.make_async_copy(src, dst, sem.at[i]) for i, (src, dst) in enumerate(((y_in, y_out), (logp_in, logp_out), (lse_in, lse_out)))]
    for c in copies:
        c.start()
    for c in copies:
        c.wait()


def local_step(tok_hidden, seq_lens, k_cache, v_cache, next_tok, g_attn, w_q, b_q, w_k, b_k, w_v, b_v, w_o, g_mlp, w_gate, w_up, w_down, g_final, w_head):
    steps = np.arange(HEAD // 2, dtype=np.float32) * np.float32(-2.0 / HEAD)
    freq = jnp.asarray(np.tile(np.power(np.float64(THETA), steps.astype(np.float64)).astype(np.float32), 2)[None])
    vm = pl.BlockSpec(memory_space=pltpu.VMEM)
    sm = pl.BlockSpec(memory_space=pltpu.SMEM)
    hb = pl.BlockSpec(memory_space=pltpu.HBM)
    dma = pltpu.SemaphoreType.DMA
    cache = jax.ShapeDtypeStruct((ROWS, SLOTS, HEAD), BF16)
    part, k_all, v_all = pl.pallas_call(
        attn_kernel,
        out_shape=(pltpu.VMEM((NCH, ROWS, CHUNK), BF16), cache, cache),
        in_specs=[sm] + [hb] * 13,
        out_specs=(vm, hb, hb),
        scratch_shapes=[
            pltpu.VMEM((1, ROWS), jnp.int32), pltpu.VMEM((1, HEAD), F32), pltpu.VMEM((ROWS, WIDTH), BF16), pltpu.VMEM((WIDTH,), BF16),
            pltpu.VMEM((4 * HEAD,), BF16), pltpu.VMEM((HEAD,), BF16), pltpu.VMEM((HEAD,), BF16),
            pltpu.VMEM((ROWS, SLOTS, HEAD), BF16), pltpu.VMEM((ROWS, SLOTS, HEAD), BF16),
            pltpu.VMEM((WIDTH, 512), BF16), pltpu.VMEM((WIDTH, HEAD), BF16), pltpu.VMEM((WIDTH, HEAD), BF16), pltpu.VMEM((512, WIDTH), BF16),
            pltpu.VMEM((4, ROWS, HEAD), F32), pltpu.VMEM((ROWS, HEAD), F32), pltpu.VMEM((ROWS, HEAD), F32),
            pltpu.VMEM((128, HEAD), F32), pltpu.VMEM((HEAD, 128), BF16), pltpu.VMEM((SLOTS, 128), F32), pltpu.VMEM((128, SLOTS), BF16),
            pltpu.VMEM((128, HEAD), F32), pltpu.VMEM((ROWS, 512), BF16), pltpu.VMEM((8, 128), jnp.int32),
            dma((4,)), dma((4,)), dma((4,)), dma((4,)), dma((4,)), dma((7,)),
        ],
        compiler_params=pltpu.CompilerParams(vmem_limit_bytes=ATTN_BYTES),
        name="attention",
    )(seq_lens, seq_lens.reshape(1, ROWS), freq, tok_hidden, g_attn, b_q, b_k, b_v,
      w_q, w_k, w_v, w_o, k_cache.reshape(ROWS, SLOTS, HEAD), v_cache.reshape(ROWS, SLOTS, HEAD))

    ff = w_gate.shape[1]
    vocab_loc = w_head.shape[0]
    ff_pad = -(-ff // BLOCK) * BLOCK
    chunk4 = pltpu.VMEM((HALF, ROWS, CHUNK), BF16)
    chunk8 = pltpu.VMEM((NCH, ROWS, CHUNK), BF16)

    def kernel(*refs):
        tail_kernel(ff, vocab_loc, *refs)

    y_out, logp, lse = pl.pallas_call(
        kernel,
        out_shape=(pltpu.VMEM((ROWS, WIDTH), BF16), pltpu.VMEM((1, ROWS), F32), pltpu.VMEM((1, ROWS), F32)),
        in_specs=[vm] + [hb] * 8,
        out_specs=(vm, vm, vm),
        scratch_shapes=[
            pltpu.VMEM((ROWS, WIDTH), BF16), pltpu.VMEM((WIDTH,), BF16), pltpu.VMEM((WIDTH,), BF16), pltpu.VMEM((1, ROWS), jnp.int32),
            pltpu.VMEM((RING, TILE, WIDTH), BF16),
            chunk4, chunk4, chunk4, chunk8, pltpu.VMEM((ROWS, WIDTH), BF16), pltpu.VMEM((ROWS, ff_pad), BF16),
            chunk8, chunk4, chunk4, chunk4, pltpu.VMEM((2, NCH, ROWS, CHUNK), BF16), pltpu.VMEM((2 * ROWS, WIDTH), BF16),
            pltpu.VMEM((1, ROWS), jnp.int32), pltpu.VMEM((2, 8, ROWS), F32), pltpu.VMEM((8, 8, ROWS), F32),
            pltpu.VMEM((BLOCK, 2 * ROWS), F32), pltpu.VMEM((BLOCK, 2 * ROWS), F32),
            dma((RING,)),
        ] + [dma((HALF,))] * 16 + [dma, dma, dma((7,)), dma((7,)), dma((4,))],
        compiler_params=pltpu.CompilerParams(vmem_limit_bytes=TAIL_BYTES, collective_id=0, has_side_effects=True),
        name="tail",
    )(pltpu.with_memory_space_constraint(part, pltpu.VMEM), tok_hidden, g_mlp, g_final, next_tok.reshape(1, ROWS), w_gate.T, w_up.T, w_down, w_head)
    vec = jax.ShapeDtypeStruct((1, ROWS), F32)
    y_out, logp, lse = pl.pallas_call(
        emit_kernel,
        out_shape=(jax.ShapeDtypeStruct((ROWS, WIDTH), BF16), vec, vec),
        in_specs=[vm] * 3,
        out_specs=(hb, hb, hb),
        scratch_shapes=[dma((3,))],
        name="emit",
    )(*(pltpu.with_memory_space_constraint(v, pltpu.VMEM) for v in (y_out, logp, lse)))
    shape = (ROWS, SLOTS, 1, HEAD)
    return y_out, k_all.reshape(shape), v_all.reshape(shape), logp.reshape(ROWS), lse.reshape(ROWS)


def solution(mesh):
    row_spec = P('dp', None)
    vec_spec = P('dp')
    cache_spec = P('dp', None, 'tp', None)
    col_spec = P(None, 'tp')
    part_spec = P('tp')
    whole_spec = P(None)
    in_specs = (row_spec, vec_spec, cache_spec, cache_spec, vec_spec, whole_spec, col_spec, part_spec, col_spec, part_spec, col_spec, part_spec, P('tp', None), whole_spec, col_spec, col_spec, P('tp', None), whole_spec, P('tp', None))
    out_specs = (row_spec, cache_spec, cache_spec, vec_spec, vec_spec)
    return jax.shard_map(local_step, mesh=mesh, in_specs=in_specs, out_specs=out_specs, check_vma=False)
```
